32 devices in a mesh: task: 4 (over y, x), tok: 8 (over z, core).
Axes of the slice: x: 2, y: 2, z: 4, core: 2. Of those that a mesh axis runs over, the one named last changes fastest.
Arguments:
- hidden: bfloat16 [4, 256, 3584], P('task', 'tok'), may hold values from -6 to 6
- attn_out: bfloat16 [4, 256, 3584], P('task', 'tok'), may hold values from -6 to 6
- gain_attn: bfloat16 [3584], replicated, may hold values from 0.5 to 1.5
- gain_mlp: bfloat16 [3584], replicated, may hold values from 0.5 to 1.5
- lengths: int32 [4, 2], P('task'), may hold values from 32 to 128
Outputs:
- gram_attn: float32 [8, 896, 1792], P('tok', 'task')
- gram_mlp: float32 [8, 896, 1792], P('tok', 'task')
The draws below stay inside these ranges and needn't reach their ends.
All inputs are finite; a program needn't handle non-finite values.
Results may differ from the reference program's by a relative error of at most 0.0044.
Values may be sent and summed in bfloat16 or wider, within the bound.
A program may use at most 64 MiB of HBM per device.

```python
import jax
import jax.numpy as jnp
from jax import lax

D = 3584
SEQS = 2
BSIDE = 2
BW = 1792
PR = 896
TOKENS = 256
SEQ_LEN = 128
N_TASK = 4
N_TOK = 8


def with_ends(result, stream_key, smallest, largest):
    longest = result.shape.index(max(result.shape))
    spots = []
    for shift in (0, 1):
        where = [jax.random.randint(jax.random.fold_in(stream_key, axis), (), 0, length) for axis, length in enumerate(result.shape)]
        where[longest] = (where[longest] + shift) % result.shape[longest]
        spots.append(tuple(where))
    return result.at[spots[0]].set(smallest).at[spots[1]].set(largest)


def block_levels(stream_key, shape, shards, least, high):
    loudness = 1.0
    for position, blocks in shards:
        steps = jax.random.uniform(jax.random.fold_in(jax.random.fold_in(stream_key, 6), position), (blocks,), jnp.float32, least / len(shards), high / len(shards))
        loudness = loudness * jnp.repeat(jnp.exp(steps), shape[position] // blocks).reshape((-1,) + (1,) * (len(shape) - 1 - position))
    return loudness


def scatter_about(rng, dims, scale, most, split=(), kind=jnp.bfloat16):
    drawn = scale * jax.random.normal(rng, dims, jnp.float32)
    if split:
        drawn = drawn * block_levels(rng, dims, split, -0.22, 0.18)
    return jnp.clip(drawn, -most, most).astype(kind)


def setup_inputs(seed: int = 0) -> dict:
    key_list = jax.random.split(jax.random.key(seed), 6)
    return {
        "hidden": scatter_about(key_list[0], (N_TASK, TOKENS, D), 1.0, 6.0, ((0, 4), (1, 8))),
        "attn_out": scatter_about(key_list[1], (N_TASK, TOKENS, D), 1.0, 6.0, ((0, 4), (1, 8))),
        "gain_attn": jnp.clip(1.0 + 0.1 * jax.random.normal(key_list[2], (D,), jnp.float32), 0.5, 1.5).astype(jnp.bfloat16),
        "gain_mlp": jnp.clip(1.0 + 0.1 * jax.random.normal(key_list[3], (D,), jnp.float32), 0.5, 1.5).astype(jnp.bfloat16),
        "lengths": with_ends(jax.random.randint(key_list[4], (N_TASK, SEQS), SEQ_LEN // 4, SEQ_LEN + 1), jax.random.fold_in(key_list[4], 1), SEQ_LEN // 4, SEQ_LEN).astype(jnp.int32),
    }


def normed(values, gain):
    scale = lax.rsqrt(lax.optimization_barrier(jnp.mean(values * values, axis=-1, keepdims=True)) + 1e-06)
    return values * scale * gain.astype(jnp.float32)

def reference(hidden, attn_out, gain_attn, gain_mlp, lengths):
    place = jnp.arange(TOKENS, dtype=jnp.int32)
    which = place // SEQ_LEN
    offset = place % SEQ_LEN
    total_attn = jnp.zeros((D, D), jnp.float32)
    total_mlp = jnp.zeros((D, D), jnp.float32)
    for group in range(N_TASK):
        limit = lengths[group][which]
        live = (offset < limit).astype(jnp.float32)[:, None]
        first = hidden[group].astype(jnp.float32)
        x_attn = (normed(first, gain_attn) * live).astype(jnp.bfloat16)
        mixed = first + attn_out[group].astype(jnp.float32)
        x_mlp = (normed(mixed, gain_mlp) * live).astype(jnp.bfloat16)
        total_attn = total_attn + jnp.dot(x_attn.T, x_attn, preferred_element_type=jnp.float32)
        total_mlp = total_mlp + jnp.dot(x_mlp.T, x_mlp, preferred_element_type=jnp.float32)

    def tiled(total):
        gram = total / TOKENS
        blocks = gram.reshape(BSIDE, BW, BSIDE, BW).transpose(0, 2, 1, 3)
        return blocks.reshape(N_TOK, PR, BW)
    return (tiled(total_attn), tiled(total_mlp))
```

```python
import functools

import jax
import jax.numpy as jnp
from jax import lax
from jax.experimental import pallas as pl
from jax.experimental.pallas import tpu as pltpu
from jax.sharding import PartitionSpec as P

LANES = 128
LENT = (2, 3)


def planes_in_product_order():
    plane = lax.axis_index("tok") // 2
    inner = jnp.logical_or(plane == 1, plane == 2)
    plane_1 = plane + 1 - 2 * (plane % 2)
    plane_2 = jnp.where(plane // 2 == 1, plane - 2, plane + 2)
    plane_3 = 3 - plane
    return (
        jnp.where(inner, plane_1, plane), jnp.where(inner, plane, plane_1),
        jnp.where(inner, plane_3, plane_2), jnp.where(inner, plane_2, plane_3),
    )


def product(rows, held, plane, which, columns=slice(None)):
    n_task = lax.axis_size("task")
    left = rows[pl.ds(plane * n_task, n_task), which]
    right = held[which, pl.ds(plane * 2 * n_task, 2 * n_task), :, columns]
    depth = left.shape[0] * left.shape[1]
    return lax.dot_general(
        left.reshape(depth, left.shape[2]), right.reshape(depth, right.shape[2]),
        (((0,), (0,)), ((), ())), preferred_element_type=jnp.float32,
    )


def last_kernel(held, rows, total, out_attn, out_mlp, staged, sent):
    row_count, column_band = out_attn.shape[1], out_attn.shape[2]
    plane = planes_in_product_order()[3]
    factor = 1.0 / (lax.axis_size("tok") * held.shape[2])
    n_bands = sent.shape[1]
    width = column_band // n_bands
    writes = []
    for which, out in ((0, out_attn), (1, out_mlp)):
        for band in range(n_bands):
            span = slice(band * width, (band + 1) * width)
            piece = total[which, :, span] + product(rows, held, plane, which, span)
            staged[which, 0, :, span] = piece[:row_count] * factor
            write = pltpu.make_async_copy(
                staged.at[which, :, :, span], out.at[:, :, span], sent.at[which, band]
            )
            write.start()
            writes.append(write)
    for write in writes:
        write.wait()


def gather_kernel(
    hidden_hbm, attn_hbm, gain_attn_hbm, gain_mlp_hbm, lengths_hbm, held, rows, total,
    hidden, attn_out, gain_attn, gain_mlp, lengths, mine, lent, passing, rising,
    loaded, ready, z_got, pass_got, rise_got, first_got, second_got, diagonal_got, pair_got, row_got, sent, row_sent,
):
    task, tok = lax.axis_index("task"), lax.axis_index("tok")
    n_task = lax.axis_size("task")
    plane, core = tok // 2, tok % 2
    band = plane % 2
    tok_dev, column_band = held.shape[2], held.shape[3]
    n_planes = held.shape[1] // (2 * n_task)
    inner = jnp.logical_or(plane == 1, plane == 2)
    outer = jnp.logical_not(inner)

    def flip(value, bit):
        return value + bit - 2 * bit * (value // bit % 2)

    task_x, task_y = flip(task, 1), flip(task, 2)
    task_d = flip(task_x, 2)
    plane_1, plane_2 = flip(plane, 1), flip(plane, 2)
    plane_3 = flip(plane_1, 2)
    near, far = jnp.where(inner, plane_3, plane_2), jnp.where(inner, plane_2, plane_3)
    order = (plane, plane_1, near, far)
    product_order = planes_in_product_order()

    def at(tasks, planes, cores):
        return {"task": tasks, "tok": planes * 2 + cores}

    def chunk(planes, tasks, cores):
        return planes * (2 * n_task) + tasks * 2 + cores

    own = chunk(plane, task, core)
    to_x, to_y, to_pair = at(task_x, plane, core), at(task_y, plane, core), at(task, plane, 1 - core)
    to_1, to_2, to_3 = at(task, plane_1, core), at(task, plane_2, core), at(task, plane_3, core)

    loads = [
        pltpu.make_async_copy(source, target, loaded.at[spot])
        for spot, (source, target) in enumerate((
            (hidden_hbm, hidden), (attn_hbm, attn_out), (gain_attn_hbm, gain_attn),
            (gain_mlp_hbm, gain_mlp), (lengths_hbm, lengths),
        ))
    ]
    for load in loads:
        load.start()

    barrier = pltpu.get_barrier_semaphore()
    always, odd = plane >= 0, plane % 2 == 1
    z_peers = (
        (to_1, plane_1, always, always), (to_2, plane_2, always, odd),
        (to_3, plane_3, inner, inner),
    )

    def signal(semaphore, peer):
        pl.semaphore_signal(
            semaphore, inc=1, device_id=peer, device_id_type=pl.DeviceIdType.MESH
        )

    for peer in (to_x, to_y, to_pair):
        signal(barrier, peer)
    for peer, planes, met, _ in z_peers:
        @pl.when(jnp.logical_and(met, planes > plane))
        def _(peer=peer):
            signal(barrier, peer)

    for load in loads:
        load.wait()
    pl.semaphore_wait(barrier, 3 + jnp.minimum(plane, 2))
    for reach, (peer, planes, _, answer) in enumerate(z_peers):
        @pl.when(jnp.logical_and(answer, planes < plane))
        def _(reach=reach, peer=peer):
            signal(ready.at[reach], peer)

    slab = 16
    seq_count = lengths.shape[1]
    seq_slots = tok_dev * lax.axis_size("tok") // seq_count
    for low in range(0, tok_dev, slab):
        part = pl.ds(low, slab)
        place = tok * tok_dev + low + lax.broadcasted_iota(jnp.int32, (slab, 1), 0)
        live = jnp.zeros((slab, 1), jnp.float32)
        for seq in range(seq_count):
            offset = place - seq * seq_slots
            inside = (offset >= 0) & (offset < seq_slots) & (offset < lengths[0, seq])
            live = jnp.where(inside, 1.0, live)
        first = hidden[0, part, :].astype(jnp.float32)
        mixed = first + attn_out[0, part, :].astype(jnp.float32)
        for which, values, gain in ((0, first, gain_attn), (1, mixed, gain_mlp)):
            done = (normed(values, gain[...].reshape(1, -1)) * live).astype(jnp.bfloat16)
            for side in range(2):
                mine[which, side, part, :] = done[:, side * column_band : (side + 1) * column_band]
    for which in range(2):
        held[which, own] = mine[which, band]

    def copy(source, which, q, got, peer):
        return pltpu.make_async_remote_copy(
            src_ref=source, dst_ref=held.at[which, q], send_sem=sent.at[0],
            recv_sem=got, device_id=peer, device_id_type=pl.DeviceIdType.MESH,
        )

    def send(*arguments):
        copy(*arguments).start()

    def arrived(span, got):
        pltpu.make_async_remote_copy(
            src_ref=span, dst_ref=span, send_sem=sent.at[0], recv_sem=got,
            device_id=to_pair, device_id_type=pl.DeviceIdType.MESH,
        ).wait_recv()

    def pair_copy(step, member, which, q, source):
        spot = step if step < n_planes - 1 else n_planes - 1 + member // 3
        send(source, which, q, pair_got.at[spot], to_pair)

    def own_step(step):
        q = chunk(order[step], task, core)

        def source(which):
            return held.at[which, q] if step else mine.at[which, band]

        def landed(which):
            if step:
                arrived(held.at[which, q], z_got.at[which, step - 1])

        landed(0)
        send(source(0), 0, q, first_got.at[0, step], to_x)
        pair_copy(step, 0, 0, q, source(0))
        landed(1)
        send(source(1), 1, q, first_got.at[1, step], to_y)
        send(source(1), 1, q, second_got.at[step], to_x)
        send(source(0), 0, q, second_got.at[step], to_y)
        pair_copy(step, 0, 1, q, source(1))

    def answered(reach):
        _, planes, met, answer = z_peers[reach]

        @pl.when(jnp.logical_and(answer, planes > plane))
        def _():
            pl.semaphore_wait(ready.at[reach], 1)

    def inward(planes):
        @pl.when(plane == planes)
        def _():
            for which in range(2):
                send(mine.at[which, 1 - band], which, own, z_got.at[which, 1], to_3)

    def z_sends():
        inward(2)
        answered(0)
        for which in range(2):
            send(mine.at[which, 1 - band], which, own, z_got.at[which, 0], to_1)

        @pl.when(outer)
        def _():
            for which in range(2):
                outward(
                    mine.at[which, band], passing.at[which], sent.at[0], pass_got.at[which], to_1
                ).start()

        answered(2)

        @pl.when(plane == 1)
        def _():
            for which in range(2):
                outward(
                    mine.at[which, band], rising.at[which], sent.at[0], rise_got.at[which], to_3
                ).start()

        @pl.when(plane == 2)
        def _():
            for which in range(2):
                send(mine.at[which, band], which, own, z_got.at[which, 1], to_2)

    def outward(source, target, semaphore, got, peer):
        return pltpu.make_async_remote_copy(
            src_ref=source, dst_ref=target, send_sem=semaphore, recv_sem=got, device_id=peer,
            device_id_type=pl.DeviceIdType.MESH,
        )

    def rise_on():
        @pl.when(plane == 2)
        def _():
            q = chunk(plane_3, task, core)
            for which in range(2):
                arrived(rising.at[which], rise_got.at[which])
                outward(
                    rising.at[which], held.at[which, q], sent.at[2], z_got.at[which, 1], to_1
                ).start()

    def relay(planes):
        @pl.when(plane == planes)
        def _():
            answered(1)
            q = chunk(plane_1, task, core)
            for which in range(2):
                send(held.at[which, q], which, q, z_got.at[which, 2], to_2)

    def pass_on():
        @pl.when(inner)
        def _():
            q = chunk(plane_1, task, core)
            for which in range(2):
                arrived(passing.at[which], pass_got.at[which])
                outward(
                    passing.at[which], held.at[which, q], sent.at[1], z_got.at[which, 2], to_3
                ).start()

    def first_side(step):
        for which, tasks, member, axis, peer in ((0, task_x, 1, 0, to_y), (1, task_y, 2, 1, to_x)):
            q = chunk(order[step], tasks, core)
            arrived(held.at[which, q], first_got.at[axis, step])
            send(held.at[which, q], which, q, diagonal_got.at[step], peer)
            pair_copy(step, member, which, q, held.at[which, q])

    def second_side(step):
        both = held.at[:, pl.ds(chunk(order[step], task_x, core), 1)]
        arrived(both, second_got.at[step])
        for which, tasks, member in ((1, task_x, 1), (0, task_y, 2)):
            q = chunk(order[step], tasks, core)
            pair_copy(step, member, which, q, held.at[which, q])

    def diagonal_step(step):
        q = chunk(order[step], task_d, core)
        arrived(held.at[:, pl.ds(q, 1)], diagonal_got.at[step])
        for which in range(2):
            pair_copy(step, 3, which, q, held.at[which, q])

    row_count = column_band // 2 // n_task
    padded = rows.shape[3]
    window = min(padded + LANES, column_band)
    row_start = core * (column_band // 2) + task * row_count
    base = jnp.minimum(row_start // LANES * LANES, column_band - window)
    shift = window - (row_start - base)

    everyone = (task, task_x, task_y, task_d)
    lends = [(1, member) for member in range(4)] + [(0, member) for member in LENT]
    gives = [
        (step, member) for step in range(n_planes - 1) for member in range(4)
        if step < 2 or (0, member) not in lends
    ]

    def row_copy(source, group, peer):
        return pltpu.make_async_remote_copy(
            src_ref=source, dst_ref=rows.at[group], send_sem=row_sent.at[0],
            recv_sem=row_got.at[group // n_task], device_id=peer,
            device_id_type=pl.DeviceIdType.MESH,
        )

    def cut(step, members):
        low = chunk(order[step], 0, 0)
        span = held.at[:, pl.ds(low, len(members))]
        arrived(span, pair_got.at[step if step < n_planes - 1 else n_planes - 1 + members[0] // 3])
        for member in members:
            tasks = everyone[member]
            group = order[step] * n_task + tasks

            def cut_into(target, group=group):
                for which in range(2):
                    span = held[
                        which, pl.ds(group * 2, 2), :, pl.ds(pl.multiple_of(base, LANES), window)
                    ]
                    span = span.reshape(2 * tok_dev, window).astype(jnp.float32)
                    span = pltpu.roll(span, shift, 1)
                    target[which] = span[:, :padded].astype(jnp.bfloat16)

            @pl.when(outer)
            def _():
                cut_into(rows.at[group])

            if (step, member) in lends:
                @pl.when(inner)
                def _():
                    cut_into(lent.at[step, tasks])

    def give_rows(step, members):
        @pl.when(outer)
        def _():
            for member in members:
                if (step, member) in gives:
                    group = order[step] * n_task + everyone[member]
                    row_copy(rows.at[group], group, to_1).start()

    def lend_rows(step, members):
        @pl.when(inner)
        def _():
            for member in members:
                if (step, member) in lends:
                    tasks = everyone[member]
                    group = order[step] * n_task + tasks
                    row_copy(lent.at[step, tasks], group, to_3).start()

    def rows_arrive(step):
        @pl.when(inner)
        def _():
            planes = product_order[step]
            span = rows.at[pl.ds(planes * n_task, n_task)]
            pltpu.make_async_remote_copy(
                src_ref=span, dst_ref=span, send_sem=row_sent.at[0], recv_sem=row_got.at[planes],
                device_id=to_1, device_id_type=pl.DeviceIdType.MESH,
            ).wait_recv()

    def multiply(step):
        rows_arrive(step)

        @pl.loop(0, 2)
        def _(which):
            piece = product(rows, held, product_order[step], which)
            if step == 0:
                total[which] = piece
            else:
                total[which] += piece

    every = (0, 1, 2, 3)
    own_step(0)
    z_sends()
    first_side(0)
    own_step(1)
    inward(1)
    rise_on()
    second_side(0)
    diagonal_step(0)
    relay(2)
    first_side(1)
    cut(0, every)
    pass_on()
    give_rows(0, every)
    own_step(2)
    second_side(1)
    relay(1)
    diagonal_step(1)
    first_side(2)
    own_step(3)
    cut(1, every)
    give_rows(1, every)
    lend_rows(0, every)
    second_side(2)
    multiply(0)
    diagonal_step(2)
    lend_rows(1, every)
    first_side(3)
    cut(2, every)
    give_rows(2, every)
    multiply(1)
    second_side(3)
    multiply(2)
    diagonal_step(3)
    cut(3, (0, 1, 2))
    cut(3, (3,))
    rows_arrive(3)

    def all_sent(span, semaphore):
        pltpu.make_async_remote_copy(
            src_ref=span, dst_ref=span, send_sem=semaphore, recv_sem=row_got.at[0],
            device_id=to_pair, device_id_type=pl.DeviceIdType.MESH,
        ).wait_send()

    @pl.when(inner)
    def _():
        all_sent(held, sent.at[0])
        all_sent(passing, sent.at[1])

        @pl.when(plane == 2)
        def _():
            all_sent(rising, sent.at[2])

        all_sent(rows.at[pl.ds(0, len(lends))], row_sent.at[0])

    @pl.when(outer)
    def _():
        all_sent(held.at[:, pl.ds(0, held.shape[1] - 2)], sent.at[0])
        all_sent(rows.at[pl.ds(0, len(gives))], row_sent.at[0])


def gathered(hidden, attn_out, gain_attn, gain_mlp, lengths):
    _, tok_dev, width = hidden.shape
    n_tok, n_task = lax.axis_size("tok"), lax.axis_size("task")
    column_band = width // 2
    row_count = column_band // 2 // n_task
    padded = -(-row_count // LANES) * LANES
    devices = n_tok * n_task
    groups = devices // 2
    vmem, hbm = (pl.BlockSpec(memory_space=space) for space in (pltpu.VMEM, pltpu.HBM))
    semaphores = pltpu.SemaphoreType.DMA
    held, rows, total = pl.pallas_call(
        gather_kernel,
        out_shape=(
            jax.ShapeDtypeStruct((2, devices, tok_dev, column_band), jnp.bfloat16),
            jax.ShapeDtypeStruct((groups, 2, 2 * tok_dev, padded), jnp.bfloat16),
            jax.ShapeDtypeStruct((2, padded, column_band), jnp.float32),
        ),
        in_specs=[hbm] * 5,
        out_specs=(vmem,) * 3,
        scratch_shapes=[
            pltpu.VMEM(hidden.shape, jnp.bfloat16),
            pltpu.VMEM(attn_out.shape, jnp.bfloat16),
            pltpu.VMEM(gain_attn.shape, jnp.bfloat16),
            pltpu.VMEM(gain_mlp.shape, jnp.bfloat16),
            pltpu.SMEM(lengths.shape, jnp.int32),
            pltpu.VMEM((2, 2, tok_dev, column_band), jnp.bfloat16),
            pltpu.VMEM((2, n_task, 2, 2 * tok_dev, padded), jnp.bfloat16),
            pltpu.VMEM((2, tok_dev, column_band), jnp.bfloat16),
            pltpu.VMEM((2, tok_dev, column_band), jnp.bfloat16),
            semaphores((5,)),
            pltpu.SemaphoreType.REGULAR((3,)),
            semaphores((2, 3)),
            semaphores((2,)),
            semaphores((2,)),
            semaphores((2, 4)),
            semaphores((4,)),
            semaphores((4,)),
            semaphores((5,)),
            semaphores((4,)),
            semaphores((3,)),
            semaphores((1,)),
        ],
        compiler_params=pltpu.CompilerParams(
            collective_id=0, has_side_effects=True, vmem_limit_bytes=24 * 2**20
        ),
    )(*(
        pltpu.with_memory_space_constraint(array, pltpu.HBM)
        for array in (hidden, attn_out, gain_attn, gain_mlp, lengths)
    ))
    shape = (1, row_count, column_band)
    n_bands = 2
    return pl.pallas_call(
        last_kernel,
        out_shape=(jax.ShapeDtypeStruct(shape, jnp.float32),) * 2,
        in_specs=[vmem] * 3,
        out_specs=(hbm, hbm),
        scratch_shapes=[
            pltpu.VMEM((2,) + shape, jnp.float32),
            semaphores((2, n_bands)),
        ],
        compiler_params=pltpu.CompilerParams(vmem_limit_bytes=12 * 2**20),
    )(held, rows, total)


def from_partner(block, axis, distance):
    count = lax.axis_size(axis)
    route = []
    for low in range(count):
        high = low | 1 << distance
        if high != low and high < count:
            route += [(low, high), (high, low)]
    return lax.ppermute(block, axis, route)


def normed(values, gain):
    scale = lax.rsqrt(jnp.mean(values * values, axis=-1, keepdims=True) + 1e-06)
    return values * scale * gain.astype(jnp.float32)


def per_device(hidden, attn_out, gain_attn, gain_mlp, lengths):
    tok_dev = hidden.shape[1]
    width = hidden.shape[2]
    n_tok = lax.axis_size("tok")
    n_task = lax.axis_size("task")
    block_side = min(4, max(2, n_tok // 16))
    token_parts = n_tok // (block_side * block_side)
    if (n_task, n_tok, block_side) == (4, 8, 2) and width % (4 * LANES) == 0 and tok_dev % 16 == 0:
        return gathered(hidden, attn_out, gain_attn, gain_mlp, lengths)
    column_band = width // block_side
    tile_rows = column_band // token_parts
    slice_rows = tok_dev // token_parts
    seq_count = lengths.shape[1]
    seq_slots = tok_dev * n_tok // seq_count
    place = lax.axis_index("tok") * tok_dev + jnp.arange(tok_dev, dtype=jnp.int32)
    which = place // seq_slots
    offset = place % seq_slots
    owner = which[:, None] == jnp.arange(seq_count, dtype=jnp.int32)[None, :]
    limit = jnp.sum(jnp.where(owner, lengths[0][None, :], 0), axis=1)
    live = (offset < limit).astype(jnp.float32)[:, None]
    first = hidden[0].astype(jnp.float32)
    x_attn = (normed(first, gain_attn) * live).astype(jnp.bfloat16)
    mixed = first + attn_out[0].astype(jnp.float32)
    x_mlp = (normed(mixed, gain_mlp) * live).astype(jnp.bfloat16)

    def bands(values):
        split = values.reshape(token_parts, slice_rows, block_side, column_band).transpose(
            2, 0, 1, 3
        )
        shape = (block_side, block_side, token_parts, slice_rows, column_band)
        left_side = jnp.broadcast_to(split[:, None], shape).reshape(n_tok, slice_rows, column_band)
        right_side = jnp.broadcast_to(split[None], shape).reshape(n_tok, slice_rows, column_band)
        return (left_side, right_side)

    left_attn, right_attn = bands(x_attn)
    left_mlp, right_mlp = bands(x_mlp)
    arrived = (
        lax.all_to_all(left_attn, "tok", split_axis=0, concat_axis=0, tiled=True),
        lax.all_to_all(right_attn, "tok", split_axis=0, concat_axis=0, tiled=True),
        lax.all_to_all(left_mlp, "tok", split_axis=0, concat_axis=0, tiled=True),
        lax.all_to_all(right_mlp, "tok", split_axis=0, concat_axis=0, tiled=True),
    )
    contract = (((0, 1), (0, 1)), ((), ()))
    tile_attn = lax.dot_general(
        arrived[0], arrived[1], contract, preferred_element_type=jnp.float32
    )
    tile_mlp = lax.dot_general(arrived[2], arrived[3], contract, preferred_element_type=jnp.float32)
    grams = (
        tile_attn.reshape(token_parts, tile_rows, column_band),
        tile_mlp.reshape(token_parts, tile_rows, column_band),
    )
    part_index = lax.axis_index("tok") % token_parts
    depth_bits = token_parts.bit_length() - 1

    def halve(current, bit):
        upper_bit = part_index // (1 << bit) % 2 == 1
        middle = current[0].shape[0] // 2
        outgoing = tuple(
            (jnp.where(upper_bit, piece[:middle], piece[middle:]) for piece in current)
        )
        kept = tuple((jnp.where(upper_bit, piece[middle:], piece[:middle]) for piece in current))
        incoming = from_partner(outgoing, "tok", bit)
        return tuple((mine + theirs for mine, theirs in zip(kept, incoming)))

    for bit in range(depth_bits - 1, -1, -1):
        grams = halve(grams, bit)
    shaped = tuple((piece.reshape(n_task, tile_rows // n_task, column_band) for piece in grams))
    grams = lax.psum_scatter(shaped, "task", scatter_dimension=0, tiled=True)
    factor = 1.0 / (tok_dev * n_tok)
    final_attn = grams[0] * factor
    final_mlp = grams[1] * factor
    return (final_attn, final_mlp)


def solution(mesh):
    return jax.shard_map(
        per_device,
        mesh=mesh,
        in_specs=(P("task", "tok", None), P("task", "tok", None), P(), P(), P("task", None)),
        out_specs=(P("tok", "task", None), P("tok", "task", None)),
        check_vma=False,
    )
```

```python
import functools

import jax
import jax.numpy as jnp
from jax import lax
from jax.experimental import pallas as pl
from jax.experimental.pallas import tpu as pltpu
from jax.sharding import PartitionSpec as P

LANES = 128
LENT = (2, 3)


def planes_in_product_order():
    plane = lax.axis_index("tok") // 2
    inner = jnp.logical_or(plane == 1, plane == 2)
    plane_1 = plane + 1 - 2 * (plane % 2)
    plane_2 = jnp.where(plane // 2 == 1, plane - 2, plane + 2)
    plane_3 = 3 - plane
    return (
        jnp.where(inner, plane_1, plane), jnp.where(inner, plane, plane_1),
        jnp.where(inner, plane_3, plane_2), jnp.where(inner, plane_2, plane_3),
    )


def product(rows, held, plane, which, columns=slice(None)):
    n_task = lax.axis_size("task")
    left = rows[pl.ds(plane * n_task, n_task), which]
    right = held[which, pl.ds(plane * 2 * n_task, 2 * n_task), :, columns]
    depth = left.shape[0] * left.shape[1]
    return lax.dot_general(
        left.reshape(depth, left.shape[2]), right.reshape(depth, right.shape[2]),
        (((0,), (0,)), ((), ())), preferred_element_type=jnp.float32,
    )


def last_kernel(held, rows, total, out_attn, out_mlp, staged, sent):
    row_count, column_band = out_attn.shape[1], out_attn.shape[2]
    plane = planes_in_product_order()[3]
    factor = 1.0 / (lax.axis_size("tok") * held.shape[2])
    n_bands = sent.shape[1]
    width = column_band // n_bands
    writes = []
    for which, out in ((0, out_attn), (1, out_mlp)):
        for band in range(n_bands):
            span = slice(band * width, (band + 1) * width)
            piece = total[which, :, span] + product(rows, held, plane, which, span)
            staged[which, 0, :, span] = piece[:row_count] * factor
            write = pltpu.make_async_copy(
                staged.at[which, :, :, span], out.at[:, :, span], sent.at[which, band]
            )
            write.start()
            writes.append(write)
    for write in writes:
        write.wait()


def gather_kernel(
    hidden_hbm, attn_hbm, gain_attn_hbm, gain_mlp_hbm, lengths_hbm, held, rows, total,
    hidden, attn_out, gain_attn, gain_mlp, lengths, mine, lent, passing, rising,
    loaded, ready, z_got, pass_got, rise_got, first_got, second_got, diagonal_got, pair_got, row_got, sent, row_sent,
):
    task, tok = lax.axis_index("task"), lax.axis_index("tok")
    n_task = lax.axis_size("task")
    plane, core = tok // 2, tok % 2
    band = plane % 2
    tok_dev, column_band = held.shape[2], held.shape[3]
    n_planes = held.shape[1] // (2 * n_task)
    inner = jnp.logical_or(plane == 1, plane == 2)
    outer = jnp.logical_not(inner)

    def flip(value, bit):
        return value + bit - 2 * bit * (value // bit % 2)

    task_x, task_y = flip(task, 1), flip(task, 2)
    task_d = flip(task_x, 2)
    plane_1, plane_2 = flip(plane, 1), flip(plane, 2)
    plane_3 = flip(plane_1, 2)
    near, far = jnp.where(inner, plane_3, plane_2), jnp.where(inner, plane_2, plane_3)
    order = (plane, plane_1, near, far)
    product_order = planes_in_product_order()

    def at(tasks, planes, cores):
        return {"task": tasks, "tok": planes * 2 + cores}

    def chunk(planes, tasks, cores):
        return planes * (2 * n_task) + tasks * 2 + cores

    own = chunk(plane, task, core)
    to_x, to_y, to_pair = at(task_x, plane, core), at(task_y, plane, core), at(task, plane, 1 - core)
    to_1, to_2, to_3 = at(task, plane_1, core), at(task, plane_2, core), at(task, plane_3, core)

    loads = [
        pltpu.make_async_copy(source, target, loaded.at[spot])
        for spot, (source, target) in enumerate((
            (hidden_hbm, hidden), (attn_hbm, attn_out), (gain_attn_hbm, gain_attn),
            (gain_mlp_hbm, gain_mlp), (lengths_hbm, lengths),
        ))
    ]
    for load in loads:
        load.start()

    barrier = pltpu.get_barrier_semaphore()
    always, odd = plane >= 0, plane % 2 == 1
    z_peers = (
        (to_1, plane_1, always, always), (to_2, plane_2, always, odd),
        (to_3, plane_3, inner, inner),
    )

    def signal(semaphore, peer):
        pl.semaphore_signal(
            semaphore, inc=1, device_id=peer, device_id_type=pl.DeviceIdType.MESH
        )

    for peer in (to_x, to_y, to_pair):
        signal(barrier, peer)
    for peer, planes, met, _ in z_peers:
        @pl.when(jnp.logical_and(met, planes > plane))
        def _(peer=peer):
            signal(barrier, peer)

    for load in loads:
        load.wait()
    pl.semaphore_wait(barrier, 3 + jnp.minimum(plane, 2))
    for reach, (peer, planes, _, answer) in enumerate(z_peers):
        @pl.when(jnp.logical_and(answer, planes < plane))
        def _(reach=reach, peer=peer):
            signal(ready.at[reach], peer)

    slab = 16
    seq_count = lengths.shape[1]
    seq_slots = tok_dev * lax.axis_size("tok") // seq_count
    for low in range(0, tok_dev, slab):
        part = pl.ds(low, slab)
        place = tok * tok_dev + low + lax.broadcasted_iota(jnp.int32, (slab, 1), 0)
        live = jnp.zeros((slab, 1), jnp.float32)
        for seq in range(seq_count):
            offset = place - seq * seq_slots
            inside = (offset >= 0) & (offset < seq_slots) & (offset < lengths[0, seq])
            live = jnp.where(inside, 1.0, live)
        first = hidden[0, part, :].astype(jnp.float32)
        mixed = first + attn_out[0, part, :].astype(jnp.float32)
        for which, values, gain in ((0, first, gain_attn), (1, mixed, gain_mlp)):
            done = (normed(values, gain[...].reshape(1, -1)) * live).astype(jnp.bfloat16)
            for side in range(2):
                mine[which, side, part, :] = done[:, side * column_band : (side + 1) * column_band]
    for which in range(2):
        held[which, own] = mine[which, band]

    def copy(source, which, q, got, peer):
        return pltpu.make_async_remote_copy(
            src_ref=source, dst_ref=held.at[which, q], send_sem=sent.at[0],
            recv_sem=got, device_id=peer, device_id_type=pl.DeviceIdType.MESH,
        )

    def send(*arguments):
        copy(*arguments).start()

    def arrived(span, got):
        pltpu.make_async_remote_copy(
            src_ref=span, dst_ref=span, send_sem=sent.at[0], recv_sem=got,
            device_id=to_pair, device_id_type=pl.DeviceIdType.MESH,
        ).wait_recv()

    def pair_copy(step, member, which, q, source):
        spot = step if step < n_planes - 1 else n_planes - 1 + member // 3
        send(source, which, q, pair_got.at[spot], to_pair)

    def own_step(step):
        q = chunk(order[step], task, core)

        def source(which):
            return held.at[which, q] if step else mine.at[which, band]

        def landed(which):
            if step:
                arrived(held.at[which, q], z_got.at[which, step - 1])

        landed(0)
        send(source(0), 0, q, first_got.at[0, step], to_x)
        pair_copy(step, 0, 0, q, source(0))
        landed(1)
        send(source(1), 1, q, first_got.at[1, step], to_y)
        send(source(1), 1, q, second_got.at[step], to_x)
        send(source(0), 0, q, second_got.at[step], to_y)
        pair_copy(step, 0, 1, q, source(1))

    def answered(reach):
        _, planes, met, answer = z_peers[reach]

        @pl.when(jnp.logical_and(answer, planes > plane))
        def _():
            pl.semaphore_wait(ready.at[reach], 1)

    def inward(planes):
        @pl.when(plane == planes)
        def _():
            for which in range(2):
                send(mine.at[which, 1 - band], which, own, z_got.at[which, 1], to_3)

    def z_sends():
        inward(2)
        answered(0)
        for which in range(2):
            send(mine.at[which, 1 - band], which, own, z_got.at[which, 0], to_1)

        @pl.when(outer)
        def _():
            for which in range(2):
                outward(
                    mine.at[which, band], passing.at[which], sent.at[0], pass_got.at[which], to_1
                ).start()

        answered(2)

        @pl.when(plane == 1)
        def _():
            for which in range(2):
                outward(
                    mine.at[which, band], rising.at[which], sent.at[0], rise_got.at[which], to_3
                ).start()

        @pl.when(plane == 2)
        def _():
            for which in range(2):
                send(mine.at[which, band], which, own, z_got.at[which, 1], to_2)

    def outward(source, target, semaphore, got, peer):
        return pltpu.make_async_remote_copy(
            src_ref=source, dst_ref=target, send_sem=semaphore, recv_sem=got, device_id=peer,
            device_id_type=pl.DeviceIdType.MESH,
        )

    def rise_on():
        @pl.when(plane == 2)
        def _():
            q = chunk(plane_3, task, core)
            for which in range(2):
                arrived(rising.at[which], rise_got.at[which])
                outward(
                    rising.at[which], held.at[which, q], sent.at[2], z_got.at[which, 1], to_1
                ).start()

    def relay(planes):
        @pl.when(plane == planes)
        def _():
            answered(1)
            q = chunk(plane_1, task, core)
            for which in range(2):
                send(held.at[which, q], which, q, z_got.at[which, 2], to_2)

    def pass_on():
        @pl.when(inner)
        def _():
            q = chunk(plane_1, task, core)
            for which in range(2):
                arrived(passing.at[which], pass_got.at[which])
                outward(
                    passing.at[which], held.at[which, q], sent.at[1], z_got.at[which, 2], to_3
                ).start()

    def first_side(step):
        for which, tasks, member, axis, peer in ((0, task_x, 1, 0, to_y), (1, task_y, 2, 1, to_x)):
            q = chunk(order[step], tasks, core)
            arrived(held.at[which, q], first_got.at[axis, step])
            send(held.at[which, q], which, q, diagonal_got.at[step], peer)
            pair_copy(step, member, which, q, held.at[which, q])

    def second_side(step):
        both = held.at[:, pl.ds(chunk(order[step], task_x, core), 1)]
        arrived(both, second_got.at[step])
        for which, tasks, member in ((1, task_x, 1), (0, task_y, 2)):
            q = chunk(order[step], tasks, core)
            pair_copy(step, member, which, q, held.at[which, q])

    def diagonal_step(step):
        q = chunk(order[step], task_d, core)
        arrived(held.at[:, pl.ds(q, 1)], diagonal_got.at[step])
        for which in range(2):
            pair_copy(step, 3, which, q, held.at[which, q])

    def diagonal_last(now):
        @pl.when(now)
        def _():
            diagonal_step(n_planes - 1)

    row_count = column_band // 2 // n_task
    padded = rows.shape[3]
    window = min(padded + LANES, column_band)
    row_start = core * (column_band // 2) + task * row_count
    base = jnp.minimum(row_start // LANES * LANES, column_band - window)
    shift = window - (row_start - base)

    everyone = (task, task_x, task_y, task_d)
    lends = [(1, member) for member in range(4)] + [(0, member) for member in LENT]
    gives = [
        (step, member) for step in range(n_planes - 1) for member in range(4)
        if step < 2 or (0, member) not in lends
    ]

    def row_copy(source, group, peer):
        return pltpu.make_async_remote_copy(
            src_ref=source, dst_ref=rows.at[group], send_sem=row_sent.at[0],
            recv_sem=row_got.at[group // n_task], device_id=peer,
            device_id_type=pl.DeviceIdType.MESH,
        )

    def cut(step, members):
        low = chunk(order[step], 0, 0)
        span = held.at[:, pl.ds(low, len(members))]
        arrived(span, pair_got.at[step if step < n_planes - 1 else n_planes - 1 + members[0] // 3])
        for member in members:
            tasks = everyone[member]
            group = order[step] * n_task + tasks

            def cut_into(target, group=group):
                for which in range(2):
                    span = held[
                        which, pl.ds(group * 2, 2), :, pl.ds(pl.multiple_of(base, LANES), window)
                    ]
                    span = span.reshape(2 * tok_dev, window).astype(jnp.float32)
                    span = pltpu.roll(span, shift, 1)
                    target[which] = span[:, :padded].astype(jnp.bfloat16)

            @pl.when(outer)
            def _():
                cut_into(rows.at[group])

            if (step, member) in lends:
                @pl.when(inner)
                def _():
                    cut_into(lent.at[step, tasks])

    def give_rows(step, members):
        @pl.when(outer)
        def _():
            for member in members:
                if (step, member) in gives:
                    group = order[step] * n_task + everyone[member]
                    row_copy(rows.at[group], group, to_1).start()

    def lend_rows(step, members):
        @pl.when(inner)
        def _():
            for member in members:
                if (step, member) in lends:
                    tasks = everyone[member]
                    group = order[step] * n_task + tasks
                    row_copy(lent.at[step, tasks], group, to_3).start()

    def rows_arrive(step):
        @pl.when(inner)
        def _():
            planes = product_order[step]
            span = rows.at[pl.ds(planes * n_task, n_task)]
            pltpu.make_async_remote_copy(
                src_ref=span, dst_ref=span, send_sem=row_sent.at[0], recv_sem=row_got.at[planes],
                device_id=to_1, device_id_type=pl.DeviceIdType.MESH,
            ).wait_recv()

    def multiply(step):
        rows_arrive(step)

        @pl.loop(0, 2)
        def _(which):
            piece = product(rows, held, product_order[step], which)
            if step == 0:
                total[which] = piece
            else:
                total[which] += piece

    every = (0, 1, 2, 3)
    own_step(0)
    z_sends()
    first_side(0)
    own_step(1)
    inward(1)
    rise_on()
    second_side(0)
    diagonal_step(0)
    relay(2)
    first_side(1)
    pass_on()
    cut(0, every)
    give_rows(0, every)
    own_step(2)
    second_side(1)
    relay(1)
    diagonal_step(1)
    first_side(2)
    cut(1, every)
    give_rows(1, every)
    own_step(3)
    lend_rows(0, every)
    second_side(2)
    multiply(0)
    diagonal_step(2)
    lend_rows(1, every)
    first_side(3)
    cut(2, every)
    give_rows(2, every)
    multiply(1)
    second_side(3)
    diagonal_last(inner)
    multiply(2)
    diagonal_last(outer)
    cut(3, (0, 1, 2))
    cut(3, (3,))
    rows_arrive(3)

    def all_sent(span, semaphore):
        pltpu.make_async_remote_copy(
            src_ref=span, dst_ref=span, send_sem=semaphore, recv_sem=row_got.at[0],
            device_id=to_pair, device_id_type=pl.DeviceIdType.MESH,
        ).wait_send()

    @pl.when(inner)
    def _():
        all_sent(held, sent.at[0])
        all_sent(passing, sent.at[1])

        @pl.when(plane == 2)
        def _():
            all_sent(rising, sent.at[2])

        all_sent(rows.at[pl.ds(0, len(lends))], row_sent.at[0])

    @pl.when(outer)
    def _():
        all_sent(held.at[:, pl.ds(0, held.shape[1] - 2)], sent.at[0])
        all_sent(rows.at[pl.ds(0, len(gives))], row_sent.at[0])


def gathered(hidden, attn_out, gain_attn, gain_mlp, lengths):
    _, tok_dev, width = hidden.shape
    n_tok, n_task = lax.axis_size("tok"), lax.axis_size("task")
    column_band = width // 2
    row_count = column_band // 2 // n_task
    padded = -(-row_count // LANES) * LANES
    devices = n_tok * n_task
    groups = devices // 2
    vmem, hbm = (pl.BlockSpec(memory_space=space) for space in (pltpu.VMEM, pltpu.HBM))
    semaphores = pltpu.SemaphoreType.DMA
    held, rows, total = pl.pallas_call(
        gather_kernel,
        out_shape=(
            jax.ShapeDtypeStruct((2, devices, tok_dev, column_band), jnp.bfloat16),
            jax.ShapeDtypeStruct((groups, 2, 2 * tok_dev, padded), jnp.bfloat16),
            jax.ShapeDtypeStruct((2, padded, column_band), jnp.float32),
        ),
        in_specs=[hbm] * 5,
        out_specs=(vmem,) * 3,
        scratch_shapes=[
            pltpu.VMEM(hidden.shape, jnp.bfloat16),
            pltpu.VMEM(attn_out.shape, jnp.bfloat16),
            pltpu.VMEM(gain_attn.shape, jnp.bfloat16),
            pltpu.VMEM(gain_mlp.shape, jnp.bfloat16),
            pltpu.SMEM(lengths.shape, jnp.int32),
            pltpu.VMEM((2, 2, tok_dev, column_band), jnp.bfloat16),
            pltpu.VMEM((2, n_task, 2, 2 * tok_dev, padded), jnp.bfloat16),
            pltpu.VMEM((2, tok_dev, column_band), jnp.bfloat16),
            pltpu.VMEM((2, tok_dev, column_band), jnp.bfloat16),
            semaphores((5,)),
            pltpu.SemaphoreType.REGULAR((3,)),
            semaphores((2, 3)),
            semaphores((2,)),
            semaphores((2,)),
            semaphores((2, 4)),
            semaphores((4,)),
            semaphores((4,)),
            semaphores((5,)),
            semaphores((4,)),
            semaphores((3,)),
            semaphores((1,)),
        ],
        compiler_params=pltpu.CompilerParams(
            collective_id=0, has_side_effects=True, vmem_limit_bytes=24 * 2**20
        ),
    )(*(
        pltpu.with_memory_space_constraint(array, pltpu.HBM)
        for array in (hidden, attn_out, gain_attn, gain_mlp, lengths)
    ))
    shape = (1, row_count, column_band)
    n_bands = column_band // (2 * LANES)
    return pl.pallas_call(
        last_kernel,
        out_shape=(jax.ShapeDtypeStruct(shape, jnp.float32),) * 2,
        in_specs=[vmem] * 3,
        out_specs=(hbm, hbm),
        scratch_shapes=[
            pltpu.VMEM((2,) + shape, jnp.float32),
            semaphores((2, n_bands)),
        ],
        compiler_params=pltpu.CompilerParams(vmem_limit_bytes=12 * 2**20),
    )(held, rows, total)


def from_partner(block, axis, distance):
    count = lax.axis_size(axis)
    route = []
    for low in range(count):
        high = low | 1 << distance
        if high != low and high < count:
            route += [(low, high), (high, low)]
    return lax.ppermute(block, axis, route)


def normed(values, gain):
    scale = lax.rsqrt(jnp.mean(values * values, axis=-1, keepdims=True) + 1e-06)
    return values * scale * gain.astype(jnp.float32)


def per_device(hidden, attn_out, gain_attn, gain_mlp, lengths):
    tok_dev = hidden.shape[1]
    width = hidden.shape[2]
    n_tok = lax.axis_size("tok")
    n_task = lax.axis_size("task")
    block_side = min(4, max(2, n_tok // 16))
    token_parts = n_tok // (block_side * block_side)
    if (n_task, n_tok, block_side) == (4, 8, 2) and width % (4 * LANES) == 0 and tok_dev % 16 == 0:
        return gathered(hidden, attn_out, gain_attn, gain_mlp, lengths)
    column_band = width // block_side
    tile_rows = column_band // token_parts
    slice_rows = tok_dev // token_parts
    seq_count = lengths.shape[1]
    seq_slots = tok_dev * n_tok // seq_count
    place = lax.axis_index("tok") * tok_dev + jnp.arange(tok_dev, dtype=jnp.int32)
    which = place // seq_slots
    offset = place % seq_slots
    owner = which[:, None] == jnp.arange(seq_count, dtype=jnp.int32)[None, :]
    limit = jnp.sum(jnp.where(owner, lengths[0][None, :], 0), axis=1)
    live = (offset < limit).astype(jnp.float32)[:, None]
    first = hidden[0].astype(jnp.float32)
    x_attn = (normed(first, gain_attn) * live).astype(jnp.bfloat16)
    mixed = first + attn_out[0].astype(jnp.float32)
    x_mlp = (normed(mixed, gain_mlp) * live).astype(jnp.bfloat16)

    def bands(values):
        split = values.reshape(token_parts, slice_rows, block_side, column_band).transpose(
            2, 0, 1, 3
        )
        shape = (block_side, block_side, token_parts, slice_rows, column_band)
        left_side = jnp.broadcast_to(split[:, None], shape).reshape(n_tok, slice_rows, column_band)
        right_side = jnp.broadcast_to(split[None], shape).reshape(n_tok, slice_rows, column_band)
        return (left_side, right_side)

    left_attn, right_attn = bands(x_attn)
    left_mlp, right_mlp = bands(x_mlp)
    arrived = (
        lax.all_to_all(left_attn, "tok", split_axis=0, concat_axis=0, tiled=True),
        lax.all_to_all(right_attn, "tok", split_axis=0, concat_axis=0, tiled=True),
        lax.all_to_all(left_mlp, "tok", split_axis=0, concat_axis=0, tiled=True),
        lax.all_to_all(right_mlp, "tok", split_axis=0, concat_axis=0, tiled=True),
    )
    contract = (((0, 1), (0, 1)), ((), ()))
    tile_attn = lax.dot_general(
        arrived[0], arrived[1], contract, preferred_element_type=jnp.float32
    )
    tile_mlp = lax.dot_general(arrived[2], arrived[3], contract, preferred_element_type=jnp.float32)
    grams = (
        tile_attn.reshape(token_parts, tile_rows, column_band),
        tile_mlp.reshape(token_parts, tile_rows, column_band),
    )
    part_index = lax.axis_index("tok") % token_parts
    depth_bits = token_parts.bit_length() - 1

    def halve(current, bit):
        upper_bit = part_index // (1 << bit) % 2 == 1
        middle = current[0].shape[0] // 2
        outgoing = tuple(
            (jnp.where(upper_bit, piece[:middle], piece[middle:]) for piece in current)
        )
        kept = tuple((jnp.where(upper_bit, piece[middle:], piece[:middle]) for piece in current))
        incoming = from_partner(outgoing, "tok", bit)
        return tuple((mine + theirs for mine, theirs in zip(kept, incoming)))

    for bit in range(depth_bits - 1, -1, -1):
        grams = halve(grams, bit)
    shaped = tuple((piece.reshape(n_task, tile_rows // n_task, column_band) for piece in grams))
    grams = lax.psum_scatter(shaped, "task", scatter_dimension=0, tiled=True)
    factor = 1.0 / (tok_dev * n_tok)
    final_attn = grams[0] * factor
    final_mlp = grams[1] * factor
    return (final_attn, final_mlp)


def solution(mesh):
    return jax.shard_map(
        per_device,
        mesh=mesh,
        in_specs=(P("task", "tok", None), P("task", "tok", None), P(), P(), P("task", None)),
        out_specs=(P("tok", "task", None), P("tok", "task", None)),
        check_vma=False,
    )
```

```python
import functools

import jax
import jax.numpy as jnp
from jax import lax
from jax.experimental import pallas as pl
from jax.experimental.pallas import tpu as pltpu
from jax.sharding import PartitionSpec as P

LANES = 128
LENT = (2, 3)


def planes_in_product_order():
    plane = lax.axis_index("tok") // 2
    inner = jnp.logical_or(plane == 1, plane == 2)
    plane_1 = plane + 1 - 2 * (plane % 2)
    plane_2 = jnp.where(plane // 2 == 1, plane - 2, plane + 2)
    plane_3 = 3 - plane
    return (
        jnp.where(inner, plane_1, plane), jnp.where(inner, plane, plane_1),
        jnp.where(inner, plane_3, plane_2), jnp.where(inner, plane_2, plane_3),
    )


def product(rows, held, plane, which):
    n_task = lax.axis_size("task")
    left = rows[pl.ds(plane * n_task, n_task), which]
    right = held[which, pl.ds(plane * 2 * n_task, 2 * n_task)]
    depth = left.shape[0] * left.shape[1]
    return lax.dot_general(
        left.reshape(depth, left.shape[2]), right.reshape(depth, right.shape[2]),
        (((0,), (0,)), ((), ())), preferred_element_type=jnp.float32,
    )


def band_edges(width):
    unit = 2 * LANES
    half = width // 2 // unit * unit
    return (0, unit, half, width), (0, width - half, width - unit, width)


def last_kernel(held, rows, total, out_attn, out_mlp, staged, sent):
    row_count, column_band = out_attn.shape[1], out_attn.shape[2]
    plane = planes_in_product_order()[3]
    factor = 1.0 / (lax.axis_size("tok") * held.shape[2])
    n_task = lax.axis_size("task")
    edges = band_edges(column_band)
    writes = []
    for which, out in ((0, out_attn), (1, out_mlp)):
        left = rows[pl.ds(plane * n_task, n_task), which]
        left = left.reshape(-1, left.shape[2]).T
        for low, high in zip(edges[which], edges[which][1:]):
            span = slice(low, high)
            right = held[which, pl.ds(plane * 2 * n_task, 2 * n_task), :, span]
            piece = total[which, :, span] + jnp.dot(
                left, right.reshape(-1, high - low), preferred_element_type=jnp.float32
            )
            staged[which, 0, :, span] = piece[:row_count] * factor
            write = pltpu.make_async_copy(
                staged.at[which, :, :, span], out.at[:, :, span], sent.at[len(writes)]
            )
            write.start()
            writes.append(write)
    for write in writes:
        write.wait()


def gather_kernel(
    hidden_hbm, attn_hbm, gain_attn_hbm, gain_mlp_hbm, lengths_hbm, held, rows, total,
    hidden, attn_out, gain_attn, gain_mlp, lengths, mine, lent, passing, rising,
    loaded, ready, z_got, pass_got, rise_got, first_got, second_got, diagonal_got, late_got, pair_got,
    row_got, sent, row_sent,
):
    task, tok = lax.axis_index("task"), lax.axis_index("tok")
    n_task = lax.axis_size("task")
    plane, core = tok // 2, tok % 2
    band = plane % 2
    tok_dev, column_band = held.shape[2], held.shape[3]
    n_planes = held.shape[1] // (2 * n_task)
    inner = jnp.logical_or(plane == 1, plane == 2)
    outer = jnp.logical_not(inner)

    def flip(value, bit):
        return value + bit - 2 * bit * (value // bit % 2)

    task_x, task_y = flip(task, 1), flip(task, 2)
    task_d = flip(task_x, 2)
    plane_1, plane_2 = flip(plane, 1), flip(plane, 2)
    plane_3 = flip(plane_1, 2)
    near, far = jnp.where(inner, plane_3, plane_2), jnp.where(inner, plane_2, plane_3)
    order = (plane, plane_1, near, far)
    product_order = planes_in_product_order()

    def at(tasks, planes, cores):
        return {"task": tasks, "tok": planes * 2 + cores}

    def chunk(planes, tasks, cores):
        return planes * (2 * n_task) + tasks * 2 + cores

    own = chunk(plane, task, core)
    to_x, to_y, to_pair = at(task_x, plane, core), at(task_y, plane, core), at(task, plane, 1 - core)
    to_1, to_2, to_3 = at(task, plane_1, core), at(task, plane_2, core), at(task, plane_3, core)

    loads = [
        pltpu.make_async_copy(source, target, loaded.at[spot])
        for spot, (source, target) in enumerate((
            (hidden_hbm, hidden), (attn_hbm, attn_out), (gain_attn_hbm, gain_attn),
            (gain_mlp_hbm, gain_mlp), (lengths_hbm, lengths),
        ))
    ]
    for load in loads:
        load.start()

    barrier = pltpu.get_barrier_semaphore()
    always, odd = plane >= 0, plane % 2 == 1
    z_peers = (
        (to_1, plane_1, always, always), (to_2, plane_2, always, odd),
        (to_3, plane_3, inner, inner),
    )

    def signal(semaphore, peer):
        pl.semaphore_signal(
            semaphore, inc=1, device_id=peer, device_id_type=pl.DeviceIdType.MESH
        )

    for peer in (to_x, to_y, to_pair):
        signal(barrier, peer)

    @pl.when(core == 1)
    def _():
        for tasks in (task_x, task_y):
            signal(barrier, at(tasks, plane, 0))

    for peer, planes, met, _ in z_peers:
        @pl.when(jnp.logical_and(met, planes > plane))
        def _(peer=peer):
            signal(barrier, peer)

    for load in loads:
        load.wait()
    slab = 16
    seq_count = lengths.shape[1]
    seq_slots = tok_dev * lax.axis_size("tok") // seq_count
    for low in range(0, tok_dev, slab):
        part = pl.ds(low, slab)
        place = tok * tok_dev + low + lax.broadcasted_iota(jnp.int32, (slab, 1), 0)
        live = jnp.zeros((slab, 1), jnp.float32)
        for seq in range(seq_count):
            offset = place - seq * seq_slots
            inside = (offset >= 0) & (offset < seq_slots) & (offset < lengths[0, seq])
            live = jnp.where(inside, 1.0, live)
        first = hidden[0, part, :].astype(jnp.float32)
        mixed = first + attn_out[0, part, :].astype(jnp.float32)
        for which, values, gain in ((0, first, gain_attn), (1, mixed, gain_mlp)):
            done = (normed(values, gain[...].reshape(1, -1)) * live).astype(jnp.bfloat16)
            for side in range(2):
                mine[which, side, part, :] = done[:, side * column_band : (side + 1) * column_band]
    for which in range(2):
        held[which, own] = mine[which, band]
    pl.semaphore_wait(barrier, 5 - 2 * core + jnp.minimum(plane, 2))
    for reach, (peer, planes, _, answer) in enumerate(z_peers):
        @pl.when(jnp.logical_and(answer, planes < plane))
        def _(reach=reach, peer=peer):
            signal(ready.at[reach], peer)

    def copy(source, which, q, got, peer):
        return pltpu.make_async_remote_copy(
            src_ref=source, dst_ref=held.at[which, q], send_sem=sent.at[0],
            recv_sem=got, device_id=peer, device_id_type=pl.DeviceIdType.MESH,
        )

    def send(*arguments):
        copy(*arguments).start()

    def arrived(span, got):
        pltpu.make_async_remote_copy(
            src_ref=span, dst_ref=span, send_sem=sent.at[0], recv_sem=got,
            device_id=to_pair, device_id_type=pl.DeviceIdType.MESH,
        ).wait_recv()

    def pair_copy(step, member, which, q, source):
        spot = step if step < n_planes - 1 else n_planes - 1 + member // 3
        send(source, which, q, pair_got.at[spot], to_pair)

    def own_step(step):
        q = chunk(order[step], task, core)

        def source(which):
            return held.at[which, q] if step else mine.at[which, band]

        def landed(which):
            if step:
                arrived(held.at[which, q], z_got.at[which, step - 1])

        landed(0)
        send(source(0), 0, q, first_got.at[0, step], to_x)
        pair_copy(step, 0, 0, q, source(0))
        landed(1)
        send(source(1), 1, q, first_got.at[1, step], to_y)
        send(source(1), 1, q, second_got.at[step], to_x)
        send(source(0), 0, q, second_got.at[step], to_y)
        pair_copy(step, 0, 1, q, source(1))

    def answered(reach):
        _, planes, met, answer = z_peers[reach]

        @pl.when(jnp.logical_and(answer, planes > plane))
        def _():
            pl.semaphore_wait(ready.at[reach], 1)

    def inward(planes):
        @pl.when(plane == planes)
        def _():
            for which in range(2):
                send(mine.at[which, 1 - band], which, own, z_got.at[which, 1], to_3)

    def z_sends():
        inward(2)
        answered(0)
        for which in range(2):
            send(mine.at[which, 1 - band], which, own, z_got.at[which, 0], to_1)

        @pl.when(outer)
        def _():
            for which in range(2):
                outward(
                    mine.at[which, band], passing.at[which], sent.at[0], pass_got.at[which], to_1
                ).start()

        answered(2)

        @pl.when(plane == 1)
        def _():
            for which in range(2):
                outward(
                    mine.at[which, band], rising.at[which], sent.at[0], rise_got.at[which], to_3
                ).start()

        @pl.when(plane == 2)
        def _():
            for which in range(2):
                send(mine.at[which, band], which, own, z_got.at[which, 1], to_2)

    def outward(source, target, semaphore, got, peer):
        return pltpu.make_async_remote_copy(
            src_ref=source, dst_ref=target, send_sem=semaphore, recv_sem=got, device_id=peer,
            device_id_type=pl.DeviceIdType.MESH,
        )

    def rise_on():
        @pl.when(plane == 2)
        def _():
            q = chunk(plane_3, task, core)
            for which in range(2):
                arrived(rising.at[which], rise_got.at[which])
                outward(
                    rising.at[which], held.at[which, q], sent.at[2], z_got.at[which, 1], to_1
                ).start()

    def relay(planes):
        @pl.when(plane == planes)
        def _():
            answered(1)
            q = chunk(plane_1, task, core)
            for which in range(2):
                send(held.at[which, q], which, q, z_got.at[which, 2], to_2)

    def pass_on():
        @pl.when(inner)
        def _():
            q = chunk(plane_1, task, core)
            for which in range(2):
                arrived(passing.at[which], pass_got.at[which])
                outward(
                    passing.at[which], held.at[which, q], sent.at[1], z_got.at[which, 2], to_3
                ).start()

    early_rows, late_rows = pl.ds(0, tok_dev // 2), pl.ds(tok_dev // 2, tok_dev // 2)

    def part_copy(which, q, part, got, peer):
        span = held.at[which, q, part]
        pltpu.make_async_remote_copy(
            src_ref=span, dst_ref=span, send_sem=sent.at[0], recv_sem=got, device_id=peer,
            device_id_type=pl.DeviceIdType.MESH,
        ).start()

    def first_side(step):
        def relay_whole(which, q, peer):
            send(held.at[which, q], which, q, diagonal_got.at[step], peer)

        for which, tasks, member, axis, towards in ((0, task_x, 1, 0, task_y), (1, task_y, 2, 1, task_x)):
            q = chunk(order[step], tasks, core)
            peer = at(towards, plane, core)
            arrived(held.at[which, q], first_got.at[axis, step])
            if step < n_planes - 1:
                relay_whole(which, q, peer)
            else:
                @pl.when(core == 1)
                def _(which=which, q=q, peer=peer):
                    relay_whole(which, q, peer)

                @pl.when(core == 0)
                def _(which=which, q=q, peer=peer, towards=towards):
                    part_copy(which, q, early_rows, diagonal_got.at[step], peer)
                    part_copy(which, q, late_rows, late_got.at[0], peer)
                    part_copy(which, q, late_rows, late_got.at[0], at(towards, plane, 1))
            pair_copy(step, member, which, q, held.at[which, q])

    def second_side(step):
        both = held.at[:, pl.ds(chunk(order[step], task_x, core), 1)]
        arrived(both, second_got.at[step])
        for which, tasks, member in ((1, task_x, 1), (0, task_y, 2)):
            q = chunk(order[step], tasks, core)
            pair_copy(step, member, which, q, held.at[which, q])

    def diagonal_step(step):
        q = chunk(order[step], task_d, core)
        arrived(held.at[:, pl.ds(q, 1)], diagonal_got.at[step])
        for which in range(2):
            pair_copy(step, 3, which, q, held.at[which, q])

    def diagonal_last(now):
        last = n_planes - 1

        @pl.when(jnp.logical_and(now, core == 1))
        def _():
            diagonal_step(last)

        @pl.when(jnp.logical_and(now, core == 0))
        def _():
            q = chunk(order[last], task_d, 0)
            arrived(held.at[:, pl.ds(q, 1), early_rows], diagonal_got.at[last])
            for which in range(2):
                part_copy(which, q, early_rows, pair_got.at[last + 1], to_pair)

    row_count = column_band // 2 // n_task
    padded = rows.shape[3]
    window = min(padded + LANES, column_band)
    row_start = core * (column_band // 2) + task * row_count
    base = jnp.minimum(row_start // LANES * LANES, column_band - window)
    shift = window - (row_start - base)

    everyone = (task, task_x, task_y, task_d)
    lends = [(1, member) for member in range(4)] + [(0, member) for member in LENT]
    gives = [
        (step, member) for step in range(n_planes - 1) for member in range(4)
        if step < 2 or (0, member) not in lends
    ]

    def row_copy(source, group, peer):
        return pltpu.make_async_remote_copy(
            src_ref=source, dst_ref=rows.at[group], send_sem=row_sent.at[0],
            recv_sem=row_got.at[group // n_task], device_id=peer,
            device_id_type=pl.DeviceIdType.MESH,
        )

    def cut(step, members):
        low = chunk(order[step], 0, 0)
        span = held.at[:, pl.ds(low, len(members))]
        if (step, members) != (n_planes - 1, (3,)):
            arrived(span, pair_got.at[min(step, n_planes - 1)])
        else:
            half = held.at[:, pl.ds(low, 1), late_rows]
            arrived(half, late_got.at[0])

            @pl.when(core == 0)
            def _():
                arrived(span, pair_got.at[n_planes])

            @pl.when(core == 1)
            def _():
                arrived(half, pair_got.at[n_planes])

        for member in members:
            tasks = everyone[member]
            group = order[step] * n_task + tasks

            def cut_into(target, group=group):
                for which in range(2):
                    span = held[
                        which, pl.ds(group * 2, 2), :, pl.ds(pl.multiple_of(base, LANES), window)
                    ]
                    span = span.reshape(2 * tok_dev, window).astype(jnp.float32)
                    span = pltpu.roll(span, shift, 1)
                    target[which] = span[:, :padded].astype(jnp.bfloat16)

            @pl.when(outer)
            def _():
                cut_into(rows.at[group])

            if (step, member) in lends:
                @pl.when(inner)
                def _():
                    cut_into(lent.at[step, tasks])

    def give_rows(step, members):
        @pl.when(outer)
        def _():
            for member in members:
                if (step, member) in gives:
                    group = order[step] * n_task + everyone[member]
                    row_copy(rows.at[group], group, to_1).start()

    def lend_rows(step, members):
        @pl.when(inner)
        def _():
            for member in members:
                if (step, member) in lends:
                    tasks = everyone[member]
                    group = order[step] * n_task + tasks
                    row_copy(lent.at[step, tasks], group, to_3).start()

    def rows_arrive(step):
        @pl.when(inner)
        def _():
            planes = product_order[step]
            span = rows.at[pl.ds(planes * n_task, n_task)]
            pltpu.make_async_remote_copy(
                src_ref=span, dst_ref=span, send_sem=row_sent.at[0], recv_sem=row_got.at[planes],
                device_id=to_1, device_id_type=pl.DeviceIdType.MESH,
            ).wait_recv()

    def multiply(step):
        rows_arrive(step)

        @pl.loop(0, 2)
        def _(which):
            piece = product(rows, held, product_order[step], which)
            if step == 0:
                total[which] = piece
            else:
                total[which] += piece

    def cut_and_give(step, cores):
        @pl.when(core == cores)
        def _():
            cut(step, every)
            give_rows(step, every)

    every = (0, 1, 2, 3)
    own_step(0)
    z_sends()
    first_side(0)
    own_step(1)
    inward(1)
    rise_on()
    second_side(0)
    diagonal_step(0)
    relay(2)
    first_side(1)
    pass_on()
    cut(0, every)
    give_rows(0, every)
    own_step(2)
    second_side(1)
    relay(1)
    diagonal_step(1)
    first_side(2)
    cut(1, every)
    give_rows(1, every)
    own_step(3)
    lend_rows(0, every)
    second_side(2)
    multiply(0)
    diagonal_step(2)
    lend_rows(1, every)
    cut_and_give(2, 0)
    first_side(3)
    cut_and_give(2, 1)
    multiply(1)
    second_side(3)
    diagonal_last(inner)
    multiply(2)
    diagonal_last(outer)
    cut(3, (0, 1, 2))
    cut(3, (3,))
    rows_arrive(3)

    def all_sent(span, semaphore):
        pltpu.make_async_remote_copy(
            src_ref=span, dst_ref=span, send_sem=semaphore, recv_sem=row_got.at[0],
            device_id=to_pair, device_id_type=pl.DeviceIdType.MESH,
        ).wait_send()

    @pl.when(inner)
    def _():
        all_sent(held, sent.at[0])
        all_sent(passing, sent.at[1])

        @pl.when(plane == 2)
        def _():
            all_sent(rising, sent.at[2])

        all_sent(rows.at[pl.ds(0, len(lends))], row_sent.at[0])

    @pl.when(outer)
    def _():
        all_sent(held.at[:, pl.ds(0, held.shape[1] - 2)], sent.at[0])
        all_sent(rows.at[pl.ds(0, len(gives))], row_sent.at[0])


def gathered(hidden, attn_out, gain_attn, gain_mlp, lengths):
    _, tok_dev, width = hidden.shape
    n_tok, n_task = lax.axis_size("tok"), lax.axis_size("task")
    column_band = width // 2
    row_count = column_band // 2 // n_task
    padded = -(-row_count // LANES) * LANES
    devices = n_tok * n_task
    groups = devices // 2
    vmem, hbm = (pl.BlockSpec(memory_space=space) for space in (pltpu.VMEM, pltpu.HBM))
    semaphores = pltpu.SemaphoreType.DMA
    held, rows, total = pl.pallas_call(
        gather_kernel,
        out_shape=(
            jax.ShapeDtypeStruct((2, devices, tok_dev, column_band), jnp.bfloat16),
            jax.ShapeDtypeStruct((groups, 2, 2 * tok_dev, padded), jnp.bfloat16),
            jax.ShapeDtypeStruct((2, padded, column_band), jnp.float32),
        ),
        in_specs=[hbm] * 5,
        out_specs=(vmem,) * 3,
        scratch_shapes=[
            pltpu.VMEM(hidden.shape, jnp.bfloat16),
            pltpu.VMEM(attn_out.shape, jnp.bfloat16),
            pltpu.VMEM(gain_attn.shape, jnp.bfloat16),
            pltpu.VMEM(gain_mlp.shape, jnp.bfloat16),
            pltpu.SMEM(lengths.shape, jnp.int32),
            pltpu.VMEM((2, 2, tok_dev, column_band), jnp.bfloat16),
            pltpu.VMEM((2, n_task, 2, 2 * tok_dev, padded), jnp.bfloat16),
            pltpu.VMEM((2, tok_dev, column_band), jnp.bfloat16),
            pltpu.VMEM((2, tok_dev, column_band), jnp.bfloat16),
            semaphores((5,)),
            pltpu.SemaphoreType.REGULAR((3,)),
            semaphores((2, 3)),
            semaphores((2,)),
            semaphores((2,)),
            semaphores((2, 4)),
            semaphores((4,)),
            semaphores((4,)),
            semaphores((1,)),
            semaphores((5,)),
            semaphores((4,)),
            semaphores((3,)),
            semaphores((1,)),
        ],
        compiler_params=pltpu.CompilerParams(
            collective_id=0, has_side_effects=True, vmem_limit_bytes=24 * 2**20
        ),
    )(*(
        pltpu.with_memory_space_constraint(array, pltpu.HBM)
        for array in (hidden, attn_out, gain_attn, gain_mlp, lengths)
    ))
    shape = (1, row_count, column_band)
    return pl.pallas_call(
        last_kernel,
        out_shape=(jax.ShapeDtypeStruct(shape, jnp.float32),) * 2,
        in_specs=[vmem] * 3,
        out_specs=(hbm, hbm),
        scratch_shapes=[
            pltpu.VMEM((2,) + shape, jnp.float32),
            semaphores((6,)),
        ],
        compiler_params=pltpu.CompilerParams(vmem_limit_bytes=12 * 2**20),
    )(held, rows, total)


def from_partner(block, axis, distance):
    count = lax.axis_size(axis)
    route = []
    for low in range(count):
        high = low | 1 << distance
        if high != low and high < count:
            route += [(low, high), (high, low)]
    return lax.ppermute(block, axis, route)


def normed(values, gain):
    scale = lax.rsqrt(jnp.mean(values * values, axis=-1, keepdims=True) + 1e-06)
    return values * scale * gain.astype(jnp.float32)


def per_device(hidden, attn_out, gain_attn, gain_mlp, lengths):
    tok_dev = hidden.shape[1]
    width = hidden.shape[2]
    n_tok = lax.axis_size("tok")
    n_task = lax.axis_size("task")
    block_side = min(4, max(2, n_tok // 16))
    token_parts = n_tok // (block_side * block_side)
    if (n_task, n_tok, block_side) == (4, 8, 2) and width % (4 * LANES) == 0 and tok_dev % 32 == 0:
        return gathered(hidden, attn_out, gain_attn, gain_mlp, lengths)
    column_band = width // block_side
    tile_rows = column_band // token_parts
    slice_rows = tok_dev // token_parts
    seq_count = lengths.shape[1]
    seq_slots = tok_dev * n_tok // seq_count
    place = lax.axis_index("tok") * tok_dev + jnp.arange(tok_dev, dtype=jnp.int32)
    which = place // seq_slots
    offset = place % seq_slots
    owner = which[:, None] == jnp.arange(seq_count, dtype=jnp.int32)[None, :]
    limit = jnp.sum(jnp.where(owner, lengths[0][None, :], 0), axis=1)
    live = (offset < limit).astype(jnp.float32)[:, None]
    first = hidden[0].astype(jnp.float32)
    x_attn = (normed(first, gain_attn) * live).astype(jnp.bfloat16)
    mixed = first + attn_out[0].astype(jnp.float32)
    x_mlp = (normed(mixed, gain_mlp) * live).astype(jnp.bfloat16)

    def bands(values):
        split = values.reshape(token_parts, slice_rows, block_side, column_band).transpose(
            2, 0, 1, 3
        )
        shape = (block_side, block_side, token_parts, slice_rows, column_band)
        left_side = jnp.broadcast_to(split[:, None], shape).reshape(n_tok, slice_rows, column_band)
        right_side = jnp.broadcast_to(split[None], shape).reshape(n_tok, slice_rows, column_band)
        return (left_side, right_side)

    left_attn, right_attn = bands(x_attn)
    left_mlp, right_mlp = bands(x_mlp)
    arrived = (
        lax.all_to_all(left_attn, "tok", split_axis=0, concat_axis=0, tiled=True),
        lax.all_to_all(right_attn, "tok", split_axis=0, concat_axis=0, tiled=True),
        lax.all_to_all(left_mlp, "tok", split_axis=0, concat_axis=0, tiled=True),
        lax.all_to_all(right_mlp, "tok", split_axis=0, concat_axis=0, tiled=True),
    )
    contract = (((0, 1), (0, 1)), ((), ()))
    tile_attn = lax.dot_general(
        arrived[0], arrived[1], contract, preferred_element_type=jnp.float32
    )
    tile_mlp = lax.dot_general(arrived[2], arrived[3], contract, preferred_element_type=jnp.float32)
    grams = (
        tile_attn.reshape(token_parts, tile_rows, column_band),
        tile_mlp.reshape(token_parts, tile_rows, column_band),
    )
    part_index = lax.axis_index("tok") % token_parts
    depth_bits = token_parts.bit_length() - 1

    def halve(current, bit):
        upper_bit = part_index // (1 << bit) % 2 == 1
        middle = current[0].shape[0] // 2
        outgoing = tuple(
            (jnp.where(upper_bit, piece[:middle], piece[middle:]) for piece in current)
        )
        kept = tuple((jnp.where(upper_bit, piece[middle:], piece[:middle]) for piece in current))
        incoming = from_partner(outgoing, "tok", bit)
        return tuple((mine + theirs for mine, theirs in zip(kept, incoming)))

    for bit in range(depth_bits - 1, -1, -1):
        grams = halve(grams, bit)
    shaped = tuple((piece.reshape(n_task, tile_rows // n_task, column_band) for piece in grams))
    grams = lax.psum_scatter(shaped, "task", scatter_dimension=0, tiled=True)
    factor = 1.0 / (tok_dev * n_tok)
    final_attn = grams[0] * factor
    final_mlp = grams[1] * factor
    return (final_attn, final_mlp)


def solution(mesh):
    return jax.shard_map(
        per_device,
        mesh=mesh,
        in_specs=(P("task", "tok", None), P("task", "tok", None), P(), P(), P("task", None)),
        out_specs=(P("tok", "task", None), P("tok", "task", None)),
        check_vma=False,
    )
```

```python
import functools

import jax
import jax.numpy as jnp
from jax import lax
from jax.experimental import pallas as pl
from jax.experimental.pallas import tpu as pltpu
from jax.sharding import PartitionSpec as P

LANES = 128
LENT = (2, 3)


def planes_in_product_order():
    plane = lax.axis_index("tok") // 2
    inner = jnp.logical_or(plane == 1, plane == 2)
    plane_1 = plane + 1 - 2 * (plane % 2)
    plane_2 = jnp.where(plane // 2 == 1, plane - 2, plane + 2)
    plane_3 = 3 - plane
    return (
        jnp.where(inner, plane_1, plane), jnp.where(inner, plane, plane_1),
        jnp.where(inner, plane_3, plane_2), jnp.where(inner, plane_2, plane_3),
    )


def product(rows, held, plane, which):
    n_task = lax.axis_size("task")
    left = rows[pl.ds(plane * n_task, n_task), which]
    right = held[which, pl.ds(plane * 2 * n_task, 2 * n_task)]
    depth = left.shape[0] * left.shape[1]
    return lax.dot_general(
        left.reshape(depth, left.shape[2]), right.reshape(depth, right.shape[2]),
        (((0,), (0,)), ((), ())), preferred_element_type=jnp.float32,
    )


def band_edges(width):
    unit = 2 * LANES
    half = width // 2 // unit * unit
    return (0, unit, half, width), (0, width - half, width - unit, width)


def last_kernel(held, rows, total, out_attn, out_mlp, staged, sent):
    row_count, column_band = out_attn.shape[1], out_attn.shape[2]
    plane = planes_in_product_order()[3]
    factor = 1.0 / (lax.axis_size("tok") * held.shape[2])
    n_task = lax.axis_size("task")
    edges = band_edges(column_band)
    for which, out in ((0, out_attn), (1, out_mlp)):
        left = rows[pl.ds(plane * n_task, n_task), which]
        left = left.reshape(-1, left.shape[2]).T
        for low, high in zip(edges[which], edges[which][1:]):
            span = slice(low, high)
            right = held[which, pl.ds(plane * 2 * n_task, 2 * n_task), :, span]
            piece = total[which, :, span] + jnp.dot(
                left, right.reshape(-1, high - low), preferred_element_type=jnp.float32
            )
            staged[which, 0, :, span] = piece[:row_count] * factor
            pltpu.make_async_copy(
                staged.at[which, :, :, span], out.at[:, :, span], sent.at[which]
            ).start()
    for which, out in ((0, out_attn), (1, out_mlp)):
        pltpu.make_async_copy(staged.at[which], out, sent.at[which]).wait()


def gather_kernel(
    hidden_hbm, attn_hbm, gain_attn_hbm, gain_mlp_hbm, lengths_hbm, held, rows, total,
    inputs, gain_attn, gain_mlp, lengths, mine, lent, passing, rising,
    loaded, ready, z_got, pass_got, rise_got, first_got, second_got, diagonal_got, early_got, late_got, pair_got,
    row_got, sent, row_sent,
):
    task, tok = lax.axis_index("task"), lax.axis_index("tok")
    n_task = lax.axis_size("task")
    plane, core = tok // 2, tok % 2
    band = plane % 2
    tok_dev, column_band = held.shape[2], held.shape[3]
    n_planes = held.shape[1] // (2 * n_task)
    inner = jnp.logical_or(plane == 1, plane == 2)
    outer = jnp.logical_not(inner)

    def flip(value, bit):
        return value + bit - 2 * bit * (value // bit % 2)

    task_x, task_y = flip(task, 1), flip(task, 2)
    task_d = flip(task_x, 2)
    plane_1, plane_2 = flip(plane, 1), flip(plane, 2)
    plane_3 = flip(plane_1, 2)
    near, far = jnp.where(inner, plane_3, plane_2), jnp.where(inner, plane_2, plane_3)
    order = (plane, plane_1, near, far)
    product_order = planes_in_product_order()

    def at(tasks, planes, cores):
        return {"task": tasks, "tok": planes * 2 + cores}

    def chunk(planes, tasks, cores):
        return planes * (2 * n_task) + tasks * 2 + cores

    own = chunk(plane, task, core)
    to_x, to_y, to_pair = at(task_x, plane, core), at(task_y, plane, core), at(task, plane, 1 - core)
    to_1, to_2, to_3 = at(task, plane_1, core), at(task, plane_2, core), at(task, plane_3, core)

    barrier = pltpu.get_barrier_semaphore()
    always, odd = plane >= 0, plane % 2 == 1
    z_peers = (
        (to_1, plane_1, always, always), (to_2, plane_2, always, odd),
        (to_3, plane_3, inner, inner),
    )

    def signal(semaphore, peer):
        pl.semaphore_signal(
            semaphore, inc=1, device_id=peer, device_id_type=pl.DeviceIdType.MESH
        )

    for spot, source, target in (
        (0, hidden_hbm, inputs.at[pl.ds(0, 1)]), (0, attn_hbm, inputs.at[pl.ds(1, 1)]),
        (1, gain_attn_hbm, gain_attn), (2, gain_mlp_hbm, gain_mlp),
        (3, lengths_hbm, lengths),
    ):
        pltpu.make_async_copy(source, target, loaded.at[spot]).start()
    for peer in (to_x, to_y, to_pair):
        signal(barrier, peer)

    @pl.when(core == 1)
    def _():
        for tasks in (task_x, task_y):
            signal(barrier, at(tasks, plane, 0))

    for peer, planes, met, _ in z_peers:
        @pl.when(jnp.logical_and(met, planes > plane))
        def _(peer=peer):
            signal(barrier, peer)

    pltpu.make_async_copy(inputs, inputs, loaded.at[0]).wait()
    pltpu.make_async_copy(gain_attn_hbm, gain_attn, loaded.at[1]).wait()
    pltpu.make_async_copy(gain_mlp_hbm, gain_mlp, loaded.at[2]).wait()
    pltpu.make_async_copy(lengths_hbm, lengths, loaded.at[3]).wait()
    slab = 16
    seq_count = lengths.shape[1]
    seq_slots = tok_dev * lax.axis_size("tok") // seq_count
    for low in range(0, tok_dev, slab):
        part = pl.ds(low, slab)
        place = tok * tok_dev + low + lax.broadcasted_iota(jnp.int32, (slab, 1), 0)
        live = jnp.zeros((slab, 1), jnp.float32)
        for seq in range(seq_count):
            offset = place - seq * seq_slots
            inside = (offset >= 0) & (offset < seq_slots) & (offset < lengths[0, seq])
            live = jnp.where(inside, 1.0, live)
        first = inputs[0, part, :].astype(jnp.float32)
        mixed = first + inputs[1, part, :].astype(jnp.float32)
        for which, values, gain in ((0, first, gain_attn), (1, mixed, gain_mlp)):
            done = (normed(values, gain[...].reshape(1, -1)) * live).astype(jnp.bfloat16)
            for side in range(2):
                mine[which, side, part, :] = done[:, side * column_band : (side + 1) * column_band]
    for which in range(2):
        held[which, own] = mine[which, band]
    pl.semaphore_wait(barrier, 5 - 2 * core + jnp.minimum(plane, 2))
    for reach, (peer, planes, _, answer) in enumerate(z_peers):
        @pl.when(jnp.logical_and(answer, planes < plane))
        def _(reach=reach, peer=peer):
            signal(ready.at[reach % 2], peer)

    def copy(source, which, q, got, peer):
        return pltpu.make_async_remote_copy(
            src_ref=source, dst_ref=held.at[which, q], send_sem=sent.at[0],
            recv_sem=got, device_id=peer, device_id_type=pl.DeviceIdType.MESH,
        )

    def send(*arguments):
        copy(*arguments).start()

    def arrived(span, got):
        pltpu.make_async_remote_copy(
            src_ref=span, dst_ref=span, send_sem=sent.at[0], recv_sem=got,
            device_id=to_pair, device_id_type=pl.DeviceIdType.MESH,
        ).wait_recv()

    def pair_copy(step, member, which, q, source):
        spot = step if step < n_planes - 1 else n_planes - 1 + member // 3
        send(source, which, q, pair_got.at[spot], to_pair)

    def own_step(step):
        q = chunk(order[step], task, core)

        def source(which):
            return held.at[which, q] if step else mine.at[which, band]

        def landed(which):
            if step == 1:
                arrived(held.at[which, q], z_got.at[which])
            elif step and which == 0:
                arrived(held.at[:, pl.ds(q, 1)], z_got.at[step])

        landed(0)
        send(source(0), 0, q, first_got.at[0, step], to_x)
        pair_copy(step, 0, 0, q, source(0))
        landed(1)
        send(source(1), 1, q, first_got.at[1, step], to_y)
        send(source(1), 1, q, second_got.at[step], to_x)
        send(source(0), 0, q, second_got.at[step], to_y)
        pair_copy(step, 0, 1, q, source(1))

    def answered(reach):
        _, planes, met, answer = z_peers[reach]

        @pl.when(jnp.logical_and(answer, planes > plane))
        def _():
            pl.semaphore_wait(ready.at[reach % 2], 1)

    def inward(planes):
        @pl.when(plane == planes)
        def _():
            for which in range(2):
                send(mine.at[which, 1 - band], which, own, z_got.at[2], to_3)

    def z_sends():
        inward(2)
        answered(0)
        for which in range(2):
            send(mine.at[which, 1 - band], which, own, z_got.at[which], to_1)

        @pl.when(outer)
        def _():
            for which in range(2):
                outward(
                    mine.at[which, band], passing.at[which], sent.at[0], pass_got.at[0], to_1
                ).start()

        answered(2)

        @pl.when(plane == 1)
        def _():
            for which in range(2):
                outward(
                    mine.at[which, band], rising.at[which], sent.at[0], rise_got.at[0], to_3
                ).start()

        @pl.when(plane == 2)
        def _():
            for which in range(2):
                send(mine.at[which, band], which, own, z_got.at[2], to_2)

    def outward(source, target, semaphore, got, peer):
        return pltpu.make_async_remote_copy(
            src_ref=source, dst_ref=target, send_sem=semaphore, recv_sem=got, device_id=peer,
            device_id_type=pl.DeviceIdType.MESH,
        )

    def rise_on():
        @pl.when(plane == 2)
        def _():
            q = chunk(plane_3, task, core)
            arrived(rising, rise_got.at[0])
            for which in range(2):
                outward(
                    rising.at[which], held.at[which, q], sent.at[1], z_got.at[2], to_1
                ).start()

    def relay(planes):
        @pl.when(plane == planes)
        def _():
            answered(1)
            q = chunk(plane_1, task, core)
            for which in range(2):
                send(held.at[which, q], which, q, z_got.at[3], to_2)

    def pass_on():
        @pl.when(inner)
        def _():
            q = chunk(plane_1, task, core)
            arrived(passing, pass_got.at[0])
            for which in range(2):
                outward(
                    passing.at[which], held.at[which, q], sent.at[1], z_got.at[3], to_3
                ).start()

    early_rows, late_rows = pl.ds(0, tok_dev // 2), pl.ds(tok_dev // 2, tok_dev // 2)

    def part_copy(which, q, part, spot, got, peer):
        span = held.at[which, q, part]
        pltpu.make_async_remote_copy(
            src_ref=span, dst_ref=span, send_sem=sent.at[spot], recv_sem=got, device_id=peer,
            device_id_type=pl.DeviceIdType.MESH,
        ).start()

    def first_side(step):
        def relay_whole(which, q, peer):
            send(held.at[which, q], which, q, diagonal_got.at[step], peer)

        for which, tasks, member, axis, towards in ((0, task_x, 1, 0, task_y), (1, task_y, 2, 1, task_x)):
            q = chunk(order[step], tasks, core)
            peer = at(towards, plane, core)
            arrived(held.at[which, q], first_got.at[axis, step])
            if step < n_planes - 1:
                relay_whole(which, q, peer)
            else:
                @pl.when(core == 1)
                def _(which=which, q=q, peer=peer):
                    relay_whole(which, q, peer)

                @pl.when(core == 0)
                def _(which=which, q=q, peer=peer, towards=towards):
                    twin = at(towards, plane, 1)
                    part_copy(which, q, early_rows, 0, early_got.at[0], twin)
                    part_copy(which, q, late_rows, 0, late_got.at[0], peer)
                    part_copy(which, q, late_rows, 2, late_got.at[0], twin)
            pair_copy(step, member, which, q, held.at[which, q])

    def second_side(step):
        both = held.at[:, pl.ds(chunk(order[step], task_x, core), 1)]
        arrived(both, second_got.at[step])
        for which, tasks, member in ((1, task_x, 1), (0, task_y, 2)):
            q = chunk(order[step], tasks, core)
            pair_copy(step, member, which, q, held.at[which, q])

    def diagonal_step(step):
        q = chunk(order[step], task_d, core)
        arrived(held.at[:, pl.ds(q, 1)], diagonal_got.at[step])
        for which in range(2):
            pair_copy(step, 3, which, q, held.at[which, q])

    def diagonal_last():
        last = n_planes - 1

        @pl.when(core == 1)
        def _():
            diagonal_step(last)
            q = chunk(order[last], task_d, 0)
            arrived(held.at[:, pl.ds(q, 1), early_rows], early_got.at[0])
            for which in range(2):
                part_copy(which, q, early_rows, 2, pair_got.at[last + 1], to_pair)

    row_count = column_band // 2 // n_task
    padded = rows.shape[3]
    window = min(padded + LANES, column_band)
    row_start = core * (column_band // 2) + task * row_count
    base = jnp.minimum(row_start // LANES * LANES, column_band - window)
    shift = window - (row_start - base)

    everyone = (task, task_x, task_y, task_d)
    lends = [(1, member) for member in range(4)] + [(0, member) for member in LENT]
    gives = [
        (step, member) for step in range(n_planes - 1) for member in range(4)
        if step < 2 or (0, member) not in lends
    ]

    def row_copy(source, group, peer):
        return pltpu.make_async_remote_copy(
            src_ref=source, dst_ref=rows.at[group], send_sem=row_sent.at[0],
            recv_sem=row_got.at[group // n_task], device_id=peer,
            device_id_type=pl.DeviceIdType.MESH,
        )

    def cut(step, members):
        low = chunk(order[step], 0, 0)
        span = held.at[:, pl.ds(low, len(members))]
        if (step, members) != (n_planes - 1, (3,)):
            arrived(span, pair_got.at[min(step, n_planes - 1)])
        else:
            half = held.at[:, pl.ds(low, 1), late_rows]
            arrived(half, late_got.at[0])

            @pl.when(core == 0)
            def _():
                arrived(held.at[0, pl.ds(0, 3)], pair_got.at[n_planes])

        for member in members:
            tasks = everyone[member]
            group = order[step] * n_task + tasks

            def cut_into(target, group=group):
                for which in range(2):
                    span = held[
                        which, pl.ds(group * 2, 2), :, pl.ds(pl.multiple_of(base, LANES), window)
                    ]
                    span = span.reshape(2 * tok_dev, window).astype(jnp.float32)
                    span = pltpu.roll(span, shift, 1)
                    target[which] = span[:, :padded].astype(jnp.bfloat16)

            @pl.when(outer)
            def _():
                cut_into(rows.at[group])

            if (step, member) in lends:
                @pl.when(inner)
                def _():
                    cut_into(lent.at[step, tasks])

    def give_rows(step, members):
        @pl.when(outer)
        def _():
            for member in members:
                if (step, member) in gives:
                    group = order[step] * n_task + everyone[member]
                    row_copy(rows.at[group], group, to_1).start()

    def lend_rows(step, members):
        @pl.when(inner)
        def _():
            for member in members:
                if (step, member) in lends:
                    tasks = everyone[member]
                    group = order[step] * n_task + tasks
                    row_copy(lent.at[step, tasks], group, to_3).start()

    def rows_arrive(step):
        @pl.when(inner)
        def _():
            planes = product_order[step]
            span = rows.at[pl.ds(planes * n_task, n_task)]
            pltpu.make_async_remote_copy(
                src_ref=span, dst_ref=span, send_sem=row_sent.at[0], recv_sem=row_got.at[planes],
                device_id=to_1, device_id_type=pl.DeviceIdType.MESH,
            ).wait_recv()

    def multiply(step):
        rows_arrive(step)

        @pl.loop(0, 2)
        def _(which):
            piece = product(rows, held, product_order[step], which)
            if step == 0:
                total[which] = piece
            else:
                total[which] += piece

    def cut_and_give(step, cores):
        @pl.when(core == cores)
        def _():
            cut(step, every)
            give_rows(step, every)

    def multiply_when(now, step):
        @pl.when(now)
        def _():
            multiply(step)

    def cut_when(now, step, members):
        @pl.when(now)
        def _():
            cut(step, members)

    every = (0, 1, 2, 3)
    own_step(0)
    z_sends()
    first_side(0)
    own_step(1)
    inward(1)
    rise_on()
    second_side(0)
    diagonal_step(0)
    relay(2)
    first_side(1)
    pass_on()
    cut(0, every)
    give_rows(0, every)
    own_step(2)
    second_side(1)
    relay(1)
    diagonal_step(1)
    first_side(2)
    cut(1, every)
    give_rows(1, every)
    own_step(3)
    lend_rows(0, every)
    second_side(2)
    multiply(0)
    diagonal_step(2)
    lend_rows(1, every)
    cut_and_give(2, 0)
    first_side(3)
    cut_and_give(2, 1)
    multiply(1)
    multiply_when(outer, 2)
    second_side(3)
    cut_when(jnp.logical_and(outer, core == 0), 3, (0, 1, 2))
    diagonal_last()
    multiply_when(inner, 2)
    cut_when(jnp.logical_or(inner, core == 1), 3, (0, 1, 2))
    cut(3, (3,))
    rows_arrive(3)

    def all_sent(span, semaphore):
        pltpu.make_async_remote_copy(
            src_ref=span, dst_ref=span, send_sem=semaphore, recv_sem=row_got.at[0],
            device_id=to_pair, device_id_type=pl.DeviceIdType.MESH,
        ).wait_send()

    chunks = held.shape[1]
    for cores in range(2):
        for place, least in ((outer, chunks - 3), (inner, chunks - 1)):
            @pl.when(jnp.logical_and(place, core == cores))
            def _(count=least + cores):
                all_sent(held.at[:, pl.ds(0, count)], sent.at[0])

    all_sent(held.at[0, pl.ds(0, 1)], sent.at[2])

    @pl.when(plane == 1)
    def _():
        all_sent(passing, sent.at[1])

    @pl.when(plane == 2)
    def _():
        all_sent(mine, sent.at[1])

    @pl.when(inner)
    def _():
        all_sent(rows.at[pl.ds(0, len(lends))], row_sent.at[0])

    @pl.when(outer)
    def _():
        all_sent(rows.at[pl.ds(0, len(gives))], row_sent.at[0])


def gathered(hidden, attn_out, gain_attn, gain_mlp, lengths):
    _, tok_dev, width = hidden.shape
    n_tok, n_task = lax.axis_size("tok"), lax.axis_size("task")
    column_band = width // 2
    row_count = column_band // 2 // n_task
    padded = -(-row_count // LANES) * LANES
    devices = n_tok * n_task
    groups = devices // 2
    vmem, hbm = (pl.BlockSpec(memory_space=space) for space in (pltpu.VMEM, pltpu.HBM))
    semaphores = pltpu.SemaphoreType.DMA
    held, rows, total = pl.pallas_call(
        gather_kernel,
        out_shape=(
            jax.ShapeDtypeStruct((2, devices, tok_dev, column_band), jnp.bfloat16),
            jax.ShapeDtypeStruct((groups, 2, 2 * tok_dev, padded), jnp.bfloat16),
            jax.ShapeDtypeStruct((2, padded, column_band), jnp.float32),
        ),
        in_specs=[hbm] * 5,
        out_specs=(vmem,) * 3,
        scratch_shapes=[
            pltpu.VMEM((2,) + hidden.shape[1:], jnp.bfloat16),
            pltpu.VMEM(gain_attn.shape, jnp.bfloat16),
            pltpu.VMEM(gain_mlp.shape, jnp.bfloat16),
            pltpu.SMEM(lengths.shape, jnp.int32),
            pltpu.VMEM((2, 2, tok_dev, column_band), jnp.bfloat16),
            pltpu.VMEM((2, n_task, 2, 2 * tok_dev, padded), jnp.bfloat16),
            pltpu.VMEM((2, tok_dev, column_band), jnp.bfloat16),
            pltpu.VMEM((2, tok_dev, column_band), jnp.bfloat16),
            semaphores((4,)),
            pltpu.SemaphoreType.REGULAR((2,)),
            semaphores((4,)),
            semaphores((1,)),
            semaphores((1,)),
            semaphores((2, 4)),
            semaphores((4,)),
            semaphores((4,)),
            semaphores((1,)),
            semaphores((1,)),
            semaphores((5,)),
            semaphores((4,)),
            semaphores((3,)),
            semaphores((1,)),
        ],
        compiler_params=pltpu.CompilerParams(
            collective_id=0, has_side_effects=True, vmem_limit_bytes=24 * 2**20
        ),
    )(*(
        pltpu.with_memory_space_constraint(array, pltpu.HBM)
        for array in (hidden, attn_out, gain_attn, gain_mlp, lengths)
    ))
    shape = (1, row_count, column_band)
    return pl.pallas_call(
        last_kernel,
        out_shape=(jax.ShapeDtypeStruct(shape, jnp.float32),) * 2,
        in_specs=[vmem] * 3,
        out_specs=(hbm, hbm),
        scratch_shapes=[
            pltpu.VMEM((2,) + shape, jnp.float32),
            semaphores((2,)),
        ],
        compiler_params=pltpu.CompilerParams(vmem_limit_bytes=12 * 2**20),
    )(held, rows, total)


def from_partner(block, axis, distance):
    count = lax.axis_size(axis)
    route = []
    for low in range(count):
        high = low | 1 << distance
        if high != low and high < count:
            route += [(low, high), (high, low)]
    return lax.ppermute(block, axis, route)


def normed(values, gain):
    scale = lax.rsqrt(jnp.mean(values * values, axis=-1, keepdims=True) + 1e-06)
    return values * scale * gain.astype(jnp.float32)


def per_device(hidden, attn_out, gain_attn, gain_mlp, lengths):
    tok_dev = hidden.shape[1]
    width = hidden.shape[2]
    n_tok = lax.axis_size("tok")
    n_task = lax.axis_size("task")
    block_side = min(4, max(2, n_tok // 16))
    token_parts = n_tok // (block_side * block_side)
    if (n_task, n_tok, block_side) == (4, 8, 2) and width % (4 * LANES) == 0 and tok_dev % 32 == 0:
        return gathered(hidden, attn_out, gain_attn, gain_mlp, lengths)
    column_band = width // block_side
    tile_rows = column_band // token_parts
    slice_rows = tok_dev // token_parts
    seq_count = lengths.shape[1]
    seq_slots = tok_dev * n_tok // seq_count
    place = lax.axis_index("tok") * tok_dev + jnp.arange(tok_dev, dtype=jnp.int32)
    which = place // seq_slots
    offset = place % seq_slots
    owner = which[:, None] == jnp.arange(seq_count, dtype=jnp.int32)[None, :]
    limit = jnp.sum(jnp.where(owner, lengths[0][None, :], 0), axis=1)
    live = (offset < limit).astype(jnp.float32)[:, None]
    first = hidden[0].astype(jnp.float32)
    x_attn = (normed(first, gain_attn) * live).astype(jnp.bfloat16)
    mixed = first + attn_out[0].astype(jnp.float32)
    x_mlp = (normed(mixed, gain_mlp) * live).astype(jnp.bfloat16)

    def bands(values):
        split = values.reshape(token_parts, slice_rows, block_side, column_band).transpose(
            2, 0, 1, 3
        )
        shape = (block_side, block_side, token_parts, slice_rows, column_band)
        left_side = jnp.broadcast_to(split[:, None], shape).reshape(n_tok, slice_rows, column_band)
        right_side = jnp.broadcast_to(split[None], shape).reshape(n_tok, slice_rows, column_band)
        return (left_side, right_side)

    left_attn, right_attn = bands(x_attn)
    left_mlp, right_mlp = bands(x_mlp)
    arrived = (
        lax.all_to_all(left_attn, "tok", split_axis=0, concat_axis=0, tiled=True),
        lax.all_to_all(right_attn, "tok", split_axis=0, concat_axis=0, tiled=True),
        lax.all_to_all(left_mlp, "tok", split_axis=0, concat_axis=0, tiled=True),
        lax.all_to_all(right_mlp, "tok", split_axis=0, concat_axis=0, tiled=True),
    )
    contract = (((0, 1), (0, 1)), ((), ()))
    tile_attn = lax.dot_general(
        arrived[0], arrived[1], contract, preferred_element_type=jnp.float32
    )
    tile_mlp = lax.dot_general(arrived[2], arrived[3], contract, preferred_element_type=jnp.float32)
    grams = (
        tile_attn.reshape(token_parts, tile_rows, column_band),
        tile_mlp.reshape(token_parts, tile_rows, column_band),
    )
    part_index = lax.axis_index("tok") % token_parts
    depth_bits = token_parts.bit_length() - 1

    def halve(current, bit):
        upper_bit = part_index // (1 << bit) % 2 == 1
        middle = current[0].shape[0] // 2
        outgoing = tuple(
            (jnp.where(upper_bit, piece[:middle], piece[middle:]) for piece in current)
        )
        kept = tuple((jnp.where(upper_bit, piece[middle:], piece[:middle]) for piece in current))
        incoming = from_partner(outgoing, "tok", bit)
        return tuple((mine + theirs for mine, theirs in zip(kept, incoming)))

    for bit in range(depth_bits - 1, -1, -1):
        grams = halve(grams, bit)
    shaped = tuple((piece.reshape(n_task, tile_rows // n_task, column_band) for piece in grams))
    grams = lax.psum_scatter(shaped, "task", scatter_dimension=0, tiled=True)
    factor = 1.0 / (tok_dev * n_tok)
    final_attn = grams[0] * factor
    final_mlp = grams[1] * factor
    return (final_attn, final_mlp)


def solution(mesh):
    return jax.shard_map(
        per_device,
        mesh=mesh,
        in_specs=(P("task", "tok", None), P("task", "tok", None), P(), P(), P("task", None)),
        out_specs=(P("tok", "task", None), P("tok", "task", None)),
        check_vma=False,
    )
```

```python
import functools

import jax
import jax.numpy as jnp
from jax import lax
from jax.experimental import pallas as pl
from jax.experimental.pallas import tpu as pltpu
from jax.sharding import PartitionSpec as P

LANES = 128
LENT = (2, 3)


def planes_in_product_order():
    plane = lax.axis_index("tok") // 2
    inner = jnp.logical_or(plane == 1, plane == 2)
    plane_1 = plane + 1 - 2 * (plane % 2)
    plane_2 = jnp.where(plane // 2 == 1, plane - 2, plane + 2)
    plane_3 = 3 - plane
    return (
        jnp.where(inner, plane_1, plane), jnp.where(inner, plane, plane_1),
        jnp.where(inner, plane_3, plane_2), jnp.where(inner, plane_2, plane_3),
    )


def product(rows, held, plane, which):
    n_task = lax.axis_size("task")
    left = rows[pl.ds(plane * n_task, n_task), which]
    right = held[which, pl.ds(plane * 2 * n_task, 2 * n_task)]
    depth = left.shape[0] * left.shape[1]
    return lax.dot_general(
        left.reshape(depth, left.shape[2]), right.reshape(depth, right.shape[2]),
        (((0,), (0,)), ((), ())), preferred_element_type=jnp.float32,
    )


def band_edges(width):
    unit = 2 * LANES
    half = width // 2 // unit * unit
    return (0, unit, half, width), (0, width - half, width - unit, width)


def last_kernel(held, rows, total, out_attn, out_mlp, staged, sent):
    row_count, column_band = out_attn.shape[1], out_attn.shape[2]
    plane = planes_in_product_order()[3]
    factor = 1.0 / (lax.axis_size("tok") * held.shape[2])
    n_task = lax.axis_size("task")
    outs = (out_attn, out_mlp)
    lefts = []
    for which in range(2):
        left = rows[pl.ds(plane * n_task, n_task), which]
        lefts.append(left.reshape(-1, left.shape[2]).T[:row_count])
    bands = [
        (which, low, high)
        for which, edges in enumerate(band_edges(column_band))
        for low, high in zip(edges, edges[1:])
    ]

    def multiplied(which, low, high):
        right = held[which, pl.ds(plane * 2 * n_task, 2 * n_task), :, low:high]
        return jnp.dot(
            lefts[which], right.reshape(-1, high - low), preferred_element_type=jnp.float32
        )

    def put(piece, which, low, high):
        span = slice(low, high)
        staged[which, 0, :, span] = (total[which, :row_count, span] + piece) * factor
        pltpu.make_async_copy(
            staged.at[which, :, :, span], outs[which].at[:, :, span], sent.at[which]
        ).start()

    ahead = multiplied(*bands[0])
    for band, later in zip(bands, bands[1:]):
        piece, ahead = ahead, multiplied(*later)
        put(piece, *band)
    put(ahead, *bands[-1])
    for which, out in ((0, out_attn), (1, out_mlp)):
        pltpu.make_async_copy(staged.at[which], out, sent.at[which]).wait()


def gather_kernel(
    hidden_hbm, attn_hbm, gain_attn_hbm, gain_mlp_hbm, lengths_hbm, held, rows, total,
    inputs, gain_attn, gain_mlp, lengths, mine, lent, passing, rising,
    loaded, ready, z_got, pass_got, rise_got, first_got, second_got, diagonal_got, early_got, late_got, pair_got,
    row_got, sent, row_sent,
):
    task, tok = lax.axis_index("task"), lax.axis_index("tok")
    n_task = lax.axis_size("task")
    plane, core = tok // 2, tok % 2
    band = plane % 2
    tok_dev, column_band = held.shape[2], held.shape[3]
    n_planes = held.shape[1] // (2 * n_task)
    inner = jnp.logical_or(plane == 1, plane == 2)
    outer = jnp.logical_not(inner)

    def flip(value, bit):
        return value + bit - 2 * bit * (value // bit % 2)

    task_x, task_y = flip(task, 1), flip(task, 2)
    task_d = flip(task_x, 2)
    plane_1, plane_2 = flip(plane, 1), flip(plane, 2)
    plane_3 = flip(plane_1, 2)
    near, far = jnp.where(inner, plane_3, plane_2), jnp.where(inner, plane_2, plane_3)
    order = (plane, plane_1, near, far)
    product_order = planes_in_product_order()

    def at(tasks, planes, cores):
        return {"task": tasks, "tok": planes * 2 + cores}

    def chunk(planes, tasks, cores):
        return planes * (2 * n_task) + tasks * 2 + cores

    own = chunk(plane, task, core)
    to_x, to_y, to_pair = at(task_x, plane, core), at(task_y, plane, core), at(task, plane, 1 - core)
    to_1, to_2, to_3 = at(task, plane_1, core), at(task, plane_2, core), at(task, plane_3, core)

    barrier = pltpu.get_barrier_semaphore()
    always, odd = plane >= 0, plane % 2 == 1
    z_peers = (
        (to_1, plane_1, always, always), (to_2, plane_2, always, odd),
        (to_3, plane_3, inner, inner),
    )

    def signal(semaphore, peer):
        pl.semaphore_signal(
            semaphore, inc=1, device_id=peer, device_id_type=pl.DeviceIdType.MESH
        )

    for spot, source, target in (
        (0, hidden_hbm, inputs.at[pl.ds(0, 1)]), (0, attn_hbm, inputs.at[pl.ds(1, 1)]),
        (1, gain_attn_hbm, gain_attn), (2, gain_mlp_hbm, gain_mlp),
        (3, lengths_hbm, lengths),
    ):
        pltpu.make_async_copy(source, target, loaded.at[spot]).start()
    for peer in (to_x, to_y, to_pair):
        signal(barrier, peer)

    @pl.when(core == 1)
    def _():
        for tasks in (task_x, task_y):
            signal(barrier, at(tasks, plane, 0))

    for peer, planes, met, _ in z_peers:
        @pl.when(jnp.logical_and(met, planes > plane))
        def _(peer=peer):
            signal(barrier, peer)

    pltpu.make_async_copy(inputs, inputs, loaded.at[0]).wait()
    pltpu.make_async_copy(gain_attn_hbm, gain_attn, loaded.at[1]).wait()
    pltpu.make_async_copy(gain_mlp_hbm, gain_mlp, loaded.at[2]).wait()
    pltpu.make_async_copy(lengths_hbm, lengths, loaded.at[3]).wait()
    slab = 8
    seq_count = lengths.shape[1]
    seq_slots = tok_dev * lax.axis_size("tok") // seq_count
    for low in range(0, tok_dev, slab):
        part = pl.ds(low, slab)
        place = tok * tok_dev + low + lax.broadcasted_iota(jnp.int32, (slab, 1), 0)
        live = jnp.zeros((slab, 1), jnp.float32)
        for seq in range(seq_count):
            offset = place - seq * seq_slots
            inside = (offset >= 0) & (offset < seq_slots) & (offset < lengths[0, seq])
            live = jnp.where(inside, 1.0, live)
        first = inputs[0, part, :].astype(jnp.float32)
        mixed = first + inputs[1, part, :].astype(jnp.float32)
        for which, values, gain in ((0, first, gain_attn), (1, mixed, gain_mlp)):
            scale = lax.rsqrt(jnp.mean(values * values, axis=-1, keepdims=True) + 1e-06) * live
            weight = gain[...].reshape(1, -1).astype(jnp.float32)
            done = (values * scale * weight).astype(jnp.bfloat16)
            for side in range(2):
                mine[which, side, part, :] = done[:, side * column_band : (side + 1) * column_band]
    for which in range(2):
        held[which, own] = mine[which, band]
    pl.semaphore_wait(barrier, 5 - 2 * core + jnp.minimum(plane, 2))
    for reach, (peer, planes, _, answer) in enumerate(z_peers):
        @pl.when(jnp.logical_and(answer, planes < plane))
        def _(reach=reach, peer=peer):
            signal(ready.at[reach % 2], peer)

    def copy(source, which, q, got, peer):
        return pltpu.make_async_remote_copy(
            src_ref=source, dst_ref=held.at[which, q], send_sem=sent.at[0],
            recv_sem=got, device_id=peer, device_id_type=pl.DeviceIdType.MESH,
        )

    def send(*arguments):
        copy(*arguments).start()

    def arrived(span, got):
        pltpu.make_async_remote_copy(
            src_ref=span, dst_ref=span, send_sem=sent.at[0], recv_sem=got,
            device_id=to_pair, device_id_type=pl.DeviceIdType.MESH,
        ).wait_recv()

    def pair_copy(step, member, which, q, source):
        spot = step if step < n_planes - 1 else n_planes - 1 + member // 3
        send(source, which, q, pair_got.at[spot], to_pair)

    def own_step(step):
        q = chunk(order[step], task, core)

        def source(which):
            return held.at[which, q] if step else mine.at[which, band]

        def landed(which):
            if step == 1:
                arrived(held.at[which, q], z_got.at[which])
            elif step and which == 0:
                arrived(held.at[:, pl.ds(q, 1)], z_got.at[step])

        landed(0)
        send(source(0), 0, q, first_got.at[0, step], to_x)
        pair_copy(step, 0, 0, q, source(0))
        landed(1)
        send(source(1), 1, q, first_got.at[1, step], to_y)
        send(source(1), 1, q, second_got.at[step], to_x)
        send(source(0), 0, q, second_got.at[step], to_y)
        pair_copy(step, 0, 1, q, source(1))

    def answered(reach):
        _, planes, met, answer = z_peers[reach]

        @pl.when(jnp.logical_and(answer, planes > plane))
        def _():
            pl.semaphore_wait(ready.at[reach % 2], 1)

    def inward(planes):
        @pl.when(plane == planes)
        def _():
            for which in range(2):
                send(mine.at[which, 1 - band], which, own, z_got.at[2], to_3)

    def z_sends():
        inward(2)
        answered(0)
        for which in range(2):
            send(mine.at[which, 1 - band], which, own, z_got.at[which], to_1)

        @pl.when(outer)
        def _():
            for which in range(2):
                outward(
                    mine.at[which, band], passing.at[which], sent.at[0], pass_got.at[0], to_1
                ).start()

        answered(2)

        @pl.when(plane == 1)
        def _():
            for which in range(2):
                outward(
                    mine.at[which, band], rising.at[which], sent.at[0], rise_got.at[0], to_3
                ).start()

        @pl.when(plane == 2)
        def _():
            for which in range(2):
                send(mine.at[which, band], which, own, z_got.at[2], to_2)

    def outward(source, target, semaphore, got, peer):
        return pltpu.make_async_remote_copy(
            src_ref=source, dst_ref=target, send_sem=semaphore, recv_sem=got, device_id=peer,
            device_id_type=pl.DeviceIdType.MESH,
        )

    def rise_on():
        @pl.when(plane == 2)
        def _():
            q = chunk(plane_3, task, core)
            arrived(rising, rise_got.at[0])
            for which in range(2):
                outward(
                    rising.at[which], held.at[which, q], sent.at[1], z_got.at[2], to_1
                ).start()

    def relay(planes):
        @pl.when(plane == planes)
        def _():
            answered(1)
            q = chunk(plane_1, task, core)
            for which in range(2):
                send(held.at[which, q], which, q, z_got.at[3], to_2)

    def pass_on():
        @pl.when(inner)
        def _():
            q = chunk(plane_1, task, core)
            arrived(passing, pass_got.at[0])
            for which in range(2):
                outward(
                    passing.at[which], held.at[which, q], sent.at[1], z_got.at[3], to_3
                ).start()

    early_rows, late_rows = pl.ds(0, tok_dev // 2), pl.ds(tok_dev // 2, tok_dev // 2)

    def part_copy(which, q, part, spot, got, peer):
        span = held.at[which, q, part]
        pltpu.make_async_remote_copy(
            src_ref=span, dst_ref=span, send_sem=sent.at[spot], recv_sem=got, device_id=peer,
            device_id_type=pl.DeviceIdType.MESH,
        ).start()

    def first_side(step):
        def relay_whole(which, q, peer):
            send(held.at[which, q], which, q, diagonal_got.at[step], peer)

        for which, tasks, member, axis, towards in ((0, task_x, 1, 0, task_y), (1, task_y, 2, 1, task_x)):
            q = chunk(order[step], tasks, core)
            peer = at(towards, plane, core)
            arrived(held.at[which, q], first_got.at[axis, step])
            if step < n_planes - 1:
                relay_whole(which, q, peer)
            else:
                @pl.when(core == 1)
                def _(which=which, q=q, peer=peer):
                    relay_whole(which, q, peer)

                @pl.when(core == 0)
                def _(which=which, q=q, peer=peer, towards=towards):
                    twin = at(towards, plane, 1)
                    part_copy(which, q, early_rows, 0, early_got.at[0], twin)
                    part_copy(which, q, late_rows, 0, late_got.at[0], peer)
                    part_copy(which, q, late_rows, 2, late_got.at[0], twin)
            pair_copy(step, member, which, q, held.at[which, q])

    def second_side(step):
        both = held.at[:, pl.ds(chunk(order[step], task_x, core), 1)]
        arrived(both, second_got.at[step])
        for which, tasks, member in ((1, task_x, 1), (0, task_y, 2)):
            q = chunk(order[step], tasks, core)
            pair_copy(step, member, which, q, held.at[which, q])

    def diagonal_step(step):
        q = chunk(order[step], task_d, core)
        arrived(held.at[:, pl.ds(q, 1)], diagonal_got.at[step])
        for which in range(2):
            pair_copy(step, 3, which, q, held.at[which, q])

    def diagonal_last():
        last = n_planes - 1

        @pl.when(core == 1)
        def _():
            diagonal_step(last)
            q = chunk(order[last], task_d, 0)
            arrived(held.at[:, pl.ds(q, 1), early_rows], early_got.at[0])
            for which in range(2):
                part_copy(which, q, early_rows, 2, pair_got.at[last + 1], to_pair)

    row_count = column_band // 2 // n_task
    padded = rows.shape[3]
    window = min(padded + LANES, column_band)
    row_start = core * (column_band // 2) + task * row_count
    base = jnp.minimum(row_start // LANES * LANES, column_band - window)
    shift = window - (row_start - base)

    everyone = (task, task_x, task_y, task_d)
    lends = [(1, member) for member in range(4)] + [(0, member) for member in LENT]
    gives = [
        (step, member) for step in range(n_planes - 1) for member in range(4)
        if step < 2 or (0, member) not in lends
    ]

    def row_copy(source, group, peer):
        return pltpu.make_async_remote_copy(
            src_ref=source, dst_ref=rows.at[group], send_sem=row_sent.at[0],
            recv_sem=row_got.at[group // n_task], device_id=peer,
            device_id_type=pl.DeviceIdType.MESH,
        )

    def cut(step, members):
        low = chunk(order[step], 0, 0)
        span = held.at[:, pl.ds(low, len(members))]
        if (step, members) != (n_planes - 1, (3,)):
            arrived(span, pair_got.at[min(step, n_planes - 1)])
        else:
            half = held.at[:, pl.ds(low, 1), late_rows]
            arrived(half, late_got.at[0])

            @pl.when(core == 0)
            def _():
                arrived(held.at[0, pl.ds(0, 3)], pair_got.at[n_planes])

        for member in members:
            tasks = everyone[member]
            group = order[step] * n_task + tasks

            def cut_into(target, group=group):
                for which in range(2):
                    span = held[
                        which, pl.ds(group * 2, 2), :, pl.ds(pl.multiple_of(base, LANES), window)
                    ]
                    span = span.reshape(2 * tok_dev, window).astype(jnp.float32)
                    span = pltpu.roll(span, shift, 1)
                    target[which] = span[:, :padded].astype(jnp.bfloat16)

            @pl.when(outer)
            def _():
                cut_into(rows.at[group])

            if (step, member) in lends:
                @pl.when(inner)
                def _():
                    cut_into(lent.at[step, tasks])

    def give_rows(step, members):
        @pl.when(outer)
        def _():
            for member in members:
                if (step, member) in gives:
                    group = order[step] * n_task + everyone[member]
                    row_copy(rows.at[group], group, to_1).start()

    def lend_rows(step, members):
        @pl.when(inner)
        def _():
            for member in members:
                if (step, member) in lends:
                    tasks = everyone[member]
                    group = order[step] * n_task + tasks
                    row_copy(lent.at[step, tasks], group, to_3).start()

    def rows_arrive(step):
        @pl.when(inner)
        def _():
            planes = product_order[step]
            span = rows.at[pl.ds(planes * n_task, n_task)]
            pltpu.make_async_remote_copy(
                src_ref=span, dst_ref=span, send_sem=row_sent.at[0], recv_sem=row_got.at[planes],
                device_id=to_1, device_id_type=pl.DeviceIdType.MESH,
            ).wait_recv()

    def multiply(step):
        rows_arrive(step)

        @pl.loop(0, 2)
        def _(which):
            piece = product(rows, held, product_order[step], which)
            if step == 0:
                total[which] = piece
            else:
                total[which] += piece

    def cut_and_give(step, cores):
        @pl.when(core == cores)
        def _():
            cut(step, every)
            give_rows(step, every)

    def multiply_when(now, step):
        @pl.when(now)
        def _():
            multiply(step)

    def cut_when(now, step, members):
        @pl.when(now)
        def _():
            cut(step, members)

    every = (0, 1, 2, 3)
    own_step(0)
    z_sends()
    first_side(0)
    own_step(1)
    inward(1)
    rise_on()
    second_side(0)
    diagonal_step(0)
    relay(2)
    first_side(1)
    pass_on()
    cut(0, every)
    give_rows(0, every)
    own_step(2)
    second_side(1)
    relay(1)
    diagonal_step(1)
    first_side(2)
    cut(1, every)
    give_rows(1, every)
    own_step(3)
    lend_rows(0, every)
    second_side(2)
    multiply(0)
    diagonal_step(2)
    lend_rows(1, every)
    cut_and_give(2, 0)
    first_side(3)
    cut_and_give(2, 1)
    multiply(1)
    multiply_when(outer, 2)
    second_side(3)
    cut_when(jnp.logical_and(outer, core == 0), 3, (0, 1, 2))
    diagonal_last()
    multiply_when(inner, 2)
    cut_when(jnp.logical_or(inner, core == 1), 3, (0, 1, 2))
    cut(3, (3,))
    rows_arrive(3)

    def all_sent(span, semaphore):
        pltpu.make_async_remote_copy(
            src_ref=span, dst_ref=span, send_sem=semaphore, recv_sem=row_got.at[0],
            device_id=to_pair, device_id_type=pl.DeviceIdType.MESH,
        ).wait_send()

    chunks = held.shape[1]
    for cores in range(2):
        for place, least in ((outer, chunks - 3), (inner, chunks - 1)):
            @pl.when(jnp.logical_and(place, core == cores))
            def _(count=least + cores):
                all_sent(held.at[:, pl.ds(0, count)], sent.at[0])

    all_sent(held.at[0, pl.ds(0, 1)], sent.at[2])

    @pl.when(plane == 1)
    def _():
        all_sent(passing, sent.at[1])

    @pl.when(plane == 2)
    def _():
        all_sent(mine, sent.at[1])

    @pl.when(inner)
    def _():
        all_sent(rows.at[pl.ds(0, len(lends))], row_sent.at[0])

    @pl.when(outer)
    def _():
        all_sent(rows.at[pl.ds(0, len(gives))], row_sent.at[0])


def gathered(hidden, attn_out, gain_attn, gain_mlp, lengths):
    _, tok_dev, width = hidden.shape
    n_tok, n_task = lax.axis_size("tok"), lax.axis_size("task")
    column_band = width // 2
    row_count = column_band // 2 // n_task
    padded = -(-row_count // LANES) * LANES
    devices = n_tok * n_task
    groups = devices // 2
    vmem, hbm = (pl.BlockSpec(memory_space=space) for space in (pltpu.VMEM, pltpu.HBM))
    semaphores = pltpu.SemaphoreType.DMA
    held, rows, total = pl.pallas_call(
        gather_kernel,
        out_shape=(
            jax.ShapeDtypeStruct((2, devices, tok_dev, column_band), jnp.bfloat16),
            jax.ShapeDtypeStruct((groups, 2, 2 * tok_dev, padded), jnp.bfloat16),
            jax.ShapeDtypeStruct((2, padded, column_band), jnp.float32),
        ),
        in_specs=[hbm] * 5,
        out_specs=(vmem,) * 3,
        scratch_shapes=[
            pltpu.VMEM((2,) + hidden.shape[1:], jnp.bfloat16),
            pltpu.VMEM(gain_attn.shape, jnp.bfloat16),
            pltpu.VMEM(gain_mlp.shape, jnp.bfloat16),
            pltpu.SMEM(lengths.shape, jnp.int32),
            pltpu.VMEM((2, 2, tok_dev, column_band), jnp.bfloat16),
            pltpu.VMEM((2, n_task, 2, 2 * tok_dev, padded), jnp.bfloat16),
            pltpu.VMEM((2, tok_dev, column_band), jnp.bfloat16),
            pltpu.VMEM((2, tok_dev, column_band), jnp.bfloat16),
            semaphores((4,)),
            pltpu.SemaphoreType.REGULAR((2,)),
            semaphores((4,)),
            semaphores((1,)),
            semaphores((1,)),
            semaphores((2, 4)),
            semaphores((4,)),
            semaphores((4,)),
            semaphores((1,)),
            semaphores((1,)),
            semaphores((5,)),
            semaphores((4,)),
            semaphores((3,)),
            semaphores((1,)),
        ],
        compiler_params=pltpu.CompilerParams(
            collective_id=0, has_side_effects=True, vmem_limit_bytes=24 * 2**20
        ),
    )(*(
        pltpu.with_memory_space_constraint(array, pltpu.HBM)
        for array in (hidden, attn_out, gain_attn, gain_mlp, lengths)
    ))
    shape = (1, row_count, column_band)
    return pl.pallas_call(
        last_kernel,
        out_shape=(jax.ShapeDtypeStruct(shape, jnp.float32),) * 2,
        in_specs=[vmem] * 3,
        out_specs=(hbm, hbm),
        scratch_shapes=[
            pltpu.VMEM((2,) + shape, jnp.float32),
            semaphores((2,)),
        ],
        compiler_params=pltpu.CompilerParams(vmem_limit_bytes=12 * 2**20),
    )(held, rows, total)


def from_partner(block, axis, distance):
    count = lax.axis_size(axis)
    route = []
    for low in range(count):
        high = low | 1 << distance
        if high != low and high < count:
            route += [(low, high), (high, low)]
    return lax.ppermute(block, axis, route)


def normed(values, gain):
    scale = lax.rsqrt(jnp.mean(values * values, axis=-1, keepdims=True) + 1e-06)
    return values * scale * gain.astype(jnp.float32)


def per_device(hidden, attn_out, gain_attn, gain_mlp, lengths):
    tok_dev = hidden.shape[1]
    width = hidden.shape[2]
    n_tok = lax.axis_size("tok")
    n_task = lax.axis_size("task")
    block_side = min(4, max(2, n_tok // 16))
    token_parts = n_tok // (block_side * block_side)
    if (n_task, n_tok, block_side) == (4, 8, 2) and width % (4 * LANES) == 0 and tok_dev % 32 == 0:
        return gathered(hidden, attn_out, gain_attn, gain_mlp, lengths)
    column_band = width // block_side
    tile_rows = column_band // token_parts
    slice_rows = tok_dev // token_parts
    seq_count = lengths.shape[1]
    seq_slots = tok_dev * n_tok // seq_count
    place = lax.axis_index("tok") * tok_dev + jnp.arange(tok_dev, dtype=jnp.int32)
    which = place // seq_slots
    offset = place % seq_slots
    owner = which[:, None] == jnp.arange(seq_count, dtype=jnp.int32)[None, :]
    limit = jnp.sum(jnp.where(owner, lengths[0][None, :], 0), axis=1)
    live = (offset < limit).astype(jnp.float32)[:, None]
    first = hidden[0].astype(jnp.float32)
    x_attn = (normed(first, gain_attn) * live).astype(jnp.bfloat16)
    mixed = first + attn_out[0].astype(jnp.float32)
    x_mlp = (normed(mixed, gain_mlp) * live).astype(jnp.bfloat16)

    def bands(values):
        split = values.reshape(token_parts, slice_rows, block_side, column_band).transpose(
            2, 0, 1, 3
        )
        shape = (block_side, block_side, token_parts, slice_rows, column_band)
        left_side = jnp.broadcast_to(split[:, None], shape).reshape(n_tok, slice_rows, column_band)
        right_side = jnp.broadcast_to(split[None], shape).reshape(n_tok, slice_rows, column_band)
        return (left_side, right_side)

    left_attn, right_attn = bands(x_attn)
    left_mlp, right_mlp = bands(x_mlp)
    arrived = (
        lax.all_to_all(left_attn, "tok", split_axis=0, concat_axis=0, tiled=True),
        lax.all_to_all(right_attn, "tok", split_axis=0, concat_axis=0, tiled=True),
        lax.all_to_all(left_mlp, "tok", split_axis=0, concat_axis=0, tiled=True),
        lax.all_to_all(right_mlp, "tok", split_axis=0, concat_axis=0, tiled=True),
    )
    contract = (((0, 1), (0, 1)), ((), ()))
    tile_attn = lax.dot_general(
        arrived[0], arrived[1], contract, preferred_element_type=jnp.float32
    )
    tile_mlp = lax.dot_general(arrived[2], arrived[3], contract, preferred_element_type=jnp.float32)
    grams = (
        tile_attn.reshape(token_parts, tile_rows, column_band),
        tile_mlp.reshape(token_parts, tile_rows, column_band),
    )
    part_index = lax.axis_index("tok") % token_parts
    depth_bits = token_parts.bit_length() - 1

    def halve(current, bit):
        upper_bit = part_index // (1 << bit) % 2 == 1
        middle = current[0].shape[0] // 2
        outgoing = tuple(
            (jnp.where(upper_bit, piece[:middle], piece[middle:]) for piece in current)
        )
        kept = tuple((jnp.where(upper_bit, piece[middle:], piece[:middle]) for piece in current))
        incoming = from_partner(outgoing, "tok", bit)
        return tuple((mine + theirs for mine, theirs in zip(kept, incoming)))

    for bit in range(depth_bits - 1, -1, -1):
        grams = halve(grams, bit)
    shaped = tuple((piece.reshape(n_task, tile_rows // n_task, column_band) for piece in grams))
    grams = lax.psum_scatter(shaped, "task", scatter_dimension=0, tiled=True)
    factor = 1.0 / (tok_dev * n_tok)
    final_attn = grams[0] * factor
    final_mlp = grams[1] * factor
    return (final_attn, final_mlp)


def solution(mesh):
    return jax.shard_map(
        per_device,
        mesh=mesh,
        in_specs=(P("task", "tok", None), P("task", "tok", None), P(), P(), P("task", None)),
        out_specs=(P("tok", "task", None), P("tok", "task", None)),
        check_vma=False,
    )
```

```python
import functools

import jax
import jax.numpy as jnp
from jax import lax
from jax.experimental import pallas as pl
from jax.experimental.pallas import tpu as pltpu
from jax.sharding import PartitionSpec as P

LANES = 128
LENT = (2, 3)


def planes_in_product_order():
    plane = lax.axis_index("tok") // 2
    inner = jnp.logical_or(plane == 1, plane == 2)
    plane_1 = plane + 1 - 2 * (plane % 2)
    plane_2 = jnp.where(plane // 2 == 1, plane - 2, plane + 2)
    plane_3 = 3 - plane
    return (
        jnp.where(inner, plane_1, plane), jnp.where(inner, plane, plane_1),
        jnp.where(inner, plane_3, plane_2), jnp.where(inner, plane_2, plane_3),
    )


def product(rows, held, plane, which):
    n_task = lax.axis_size("task")
    left = rows[pl.ds(plane * n_task, n_task), which]
    right = held[which, pl.ds(plane * 2 * n_task, 2 * n_task)]
    depth = left.shape[0] * left.shape[1]
    return lax.dot_general(
        left.reshape(depth, left.shape[2]), right.reshape(depth, right.shape[2]),
        (((0,), (0,)), ((), ())), preferred_element_type=jnp.float32,
    )


def band_edges(width):
    unit = 2 * LANES
    half = width // 2 // unit * unit
    return (0, unit, half, width), (0, width - half, width - unit, width)


def last_kernel(held, rows, total, out_attn, out_mlp, staged, sent):
    row_count, column_band = out_attn.shape[1], out_attn.shape[2]
    plane = planes_in_product_order()[3]
    factor = 1.0 / (lax.axis_size("tok") * held.shape[2])
    n_task = lax.axis_size("task")
    outs = (out_attn, out_mlp)
    lefts = []
    for which in range(2):
        left = rows[pl.ds(plane * n_task, n_task), which]
        lefts.append(left.reshape(-1, left.shape[2]).T[:row_count])
    bands = [
        (which, low, high)
        for which, edges in enumerate(band_edges(column_band))
        for low, high in zip(edges, edges[1:])
    ]

    def multiplied(which, low, high):
        right = held[which, pl.ds(plane * 2 * n_task, 2 * n_task), :, low:high]
        return jnp.dot(
            lefts[which], right.reshape(-1, high - low), preferred_element_type=jnp.float32
        )

    def put(piece, which, low, high):
        span = slice(low, high)
        staged[which, 0, :, span] = (total[which, :row_count, span] + piece) * factor
        pltpu.make_async_copy(
            staged.at[which, :, :, span], outs[which].at[:, :, span], sent.at[which]
        ).start()

    ahead = multiplied(*bands[0])
    for band, later in zip(bands, bands[1:]):
        piece, ahead = ahead, multiplied(*later)
        put(piece, *band)
    put(ahead, *bands[-1])
    for which, out in ((0, out_attn), (1, out_mlp)):
        pltpu.make_async_copy(staged.at[which], out, sent.at[which]).wait()


def gather_kernel(
    hidden_hbm, attn_hbm, gain_attn_hbm, gain_mlp_hbm, lengths_hbm, held, rows, total,
    inputs, gain_attn, gain_mlp, lengths, mine, lent, passing, rising,
    loaded, ready, z_got, pass_got, rise_got, first_got, second_got, diagonal_got, early_got, late_got, pair_got,
    row_got, sent, row_sent,
):
    task, tok = lax.axis_index("task"), lax.axis_index("tok")
    n_task = lax.axis_size("task")
    plane, core = tok // 2, tok % 2
    band = plane % 2
    tok_dev, column_band = held.shape[2], held.shape[3]
    n_planes = held.shape[1] // (2 * n_task)
    inner = jnp.logical_or(plane == 1, plane == 2)
    outer = jnp.logical_not(inner)

    def flip(value, bit):
        return value + bit - 2 * bit * (value // bit % 2)

    task_x, task_y = flip(task, 1), flip(task, 2)
    task_d = flip(task_x, 2)
    plane_1, plane_2 = flip(plane, 1), flip(plane, 2)
    plane_3 = flip(plane_1, 2)
    near, far = jnp.where(inner, plane_3, plane_2), jnp.where(inner, plane_2, plane_3)
    order = (plane, plane_1, near, far)
    product_order = planes_in_product_order()

    def at(tasks, planes, cores):
        return {"task": tasks, "tok": planes * 2 + cores}

    def chunk(planes, tasks, cores):
        return planes * (2 * n_task) + tasks * 2 + cores

    own = chunk(plane, task, core)
    to_x, to_y, to_pair = at(task_x, plane, core), at(task_y, plane, core), at(task, plane, 1 - core)
    to_1, to_2, to_3 = at(task, plane_1, core), at(task, plane_2, core), at(task, plane_3, core)

    barrier = pltpu.get_barrier_semaphore()
    always, odd = plane >= 0, plane % 2 == 1
    z_peers = (
        (to_1, plane_1, always, always), (to_2, plane_2, always, odd),
        (to_3, plane_3, inner, inner),
    )

    def signal(semaphore, peer):
        pl.semaphore_signal(
            semaphore, inc=1, device_id=peer, device_id_type=pl.DeviceIdType.MESH
        )

    for spot, source, target in (
        (0, hidden_hbm, inputs.at[pl.ds(0, 1)]), (0, attn_hbm, inputs.at[pl.ds(1, 1)]),
        (1, gain_attn_hbm, gain_attn), (2, gain_mlp_hbm, gain_mlp),
        (3, lengths_hbm, lengths),
    ):
        pltpu.make_async_copy(source, target, loaded.at[spot]).start()
    for peer in (to_x, to_y, to_pair):
        signal(barrier, peer)

    @pl.when(core == 1)
    def _():
        for tasks in (task_x, task_y):
            signal(barrier, at(tasks, plane, 0))

    for peer, planes, met, _ in z_peers:
        @pl.when(jnp.logical_and(met, planes > plane))
        def _(peer=peer):
            signal(barrier, peer)

    pltpu.make_async_copy(inputs, inputs, loaded.at[0]).wait()
    pltpu.make_async_copy(gain_attn_hbm, gain_attn, loaded.at[1]).wait()
    pltpu.make_async_copy(gain_mlp_hbm, gain_mlp, loaded.at[2]).wait()
    pltpu.make_async_copy(lengths_hbm, lengths, loaded.at[3]).wait()
    slab = 8
    seq_count = lengths.shape[1]
    seq_slots = tok_dev * lax.axis_size("tok") // seq_count
    half = tok_dev // 2
    early_rows, late_rows = pl.ds(0, half), pl.ds(half, half)

    def norm_rows(start, part):
        for low in range(start, start + half, slab):
            spot = pl.ds(low, slab)
            place = tok * tok_dev + low + lax.broadcasted_iota(jnp.int32, (slab, 1), 0)
            live = jnp.zeros((slab, 1), jnp.float32)
            for seq in range(seq_count):
                offset = place - seq * seq_slots
                inside = (offset >= 0) & (offset < seq_slots) & (offset < lengths[0, seq])
                live = jnp.where(inside, 1.0, live)
            first = inputs[0, spot, :].astype(jnp.float32)
            mixed = first + inputs[1, spot, :].astype(jnp.float32)
            for which, values, gain in ((0, first, gain_attn), (1, mixed, gain_mlp)):
                mean = jnp.mean(values * values, axis=-1, keepdims=True)
                scale = lax.rsqrt(mean + 1e-06) * live
                weight = gain[...].reshape(1, -1).astype(jnp.float32)
                done = (values * scale * weight).astype(jnp.bfloat16)
                for side in range(2):
                    span = slice(side * column_band, (side + 1) * column_band)
                    mine[which, side, spot, :] = done[:, span]
        for which in range(2):
            held[which, own, part] = mine[which, band, part]

    def first_copies(part):
        for which, peer in ((0, to_x), (1, to_y)):
            pltpu.make_async_remote_copy(
                src_ref=mine.at[which, band, part], dst_ref=held.at[which, own, part],
                send_sem=sent.at[0], recv_sem=first_got.at[which, 0], device_id=peer,
                device_id_type=pl.DeviceIdType.MESH,
            ).start()

    norm_rows(0, early_rows)
    pl.semaphore_wait(barrier, 5 - 2 * core + jnp.minimum(plane, 2))
    first_copies(early_rows)
    for reach, (peer, planes, _, answer) in enumerate(z_peers):
        @pl.when(jnp.logical_and(answer, planes < plane))
        def _(reach=reach, peer=peer):
            signal(ready.at[reach % 2], peer)
    norm_rows(half, late_rows)
    first_copies(late_rows)

    def copy(source, which, q, got, peer):
        return pltpu.make_async_remote_copy(
            src_ref=source, dst_ref=held.at[which, q], send_sem=sent.at[0],
            recv_sem=got, device_id=peer, device_id_type=pl.DeviceIdType.MESH,
        )

    def send(*arguments):
        copy(*arguments).start()

    def arrived(span, got):
        pltpu.make_async_remote_copy(
            src_ref=span, dst_ref=span, send_sem=sent.at[0], recv_sem=got,
            device_id=to_pair, device_id_type=pl.DeviceIdType.MESH,
        ).wait_recv()

    def pair_copy(step, member, which, q, source):
        spot = step if step < n_planes - 1 else n_planes - 1 + member // 3
        send(source, which, q, pair_got.at[spot], to_pair)

    def own_step(step):
        q = chunk(order[step], task, core)

        def source(which):
            return held.at[which, q] if step else mine.at[which, band]

        def landed(which):
            if step == 1:
                arrived(held.at[which, q], z_got.at[which])
            elif step and which == 0:
                arrived(held.at[:, pl.ds(q, 1)], z_got.at[step])

        landed(0)
        if step:
            send(source(0), 0, q, first_got.at[0, step], to_x)
        pair_copy(step, 0, 0, q, source(0))
        landed(1)
        if step:
            send(source(1), 1, q, first_got.at[1, step], to_y)
        send(source(1), 1, q, second_got.at[step], to_x)
        send(source(0), 0, q, second_got.at[step], to_y)
        pair_copy(step, 0, 1, q, source(1))

    def answered(reach):
        _, planes, met, answer = z_peers[reach]

        @pl.when(jnp.logical_and(answer, planes > plane))
        def _():
            pl.semaphore_wait(ready.at[reach % 2], 1)

    def inward(planes):
        @pl.when(plane == planes)
        def _():
            for which in range(2):
                send(mine.at[which, 1 - band], which, own, z_got.at[2], to_3)

    def z_sends():
        inward(2)
        answered(0)
        for which in range(2):
            send(mine.at[which, 1 - band], which, own, z_got.at[which], to_1)

        @pl.when(outer)
        def _():
            for which in range(2):
                outward(
                    mine.at[which, band], passing.at[which], sent.at[0], pass_got.at[0], to_1
                ).start()

        answered(2)

        @pl.when(plane == 1)
        def _():
            for which in range(2):
                outward(
                    mine.at[which, band], rising.at[which], sent.at[0], rise_got.at[0], to_3
                ).start()

        @pl.when(plane == 2)
        def _():
            for which in range(2):
                send(mine.at[which, band], which, own, z_got.at[2], to_2)

    def outward(source, target, semaphore, got, peer):
        return pltpu.make_async_remote_copy(
            src_ref=source, dst_ref=target, send_sem=semaphore, recv_sem=got, device_id=peer,
            device_id_type=pl.DeviceIdType.MESH,
        )

    def rise_on():
        @pl.when(plane == 2)
        def _():
            q = chunk(plane_3, task, core)
            arrived(rising, rise_got.at[0])
            for which in range(2):
                outward(
                    rising.at[which], held.at[which, q], sent.at[1], z_got.at[2], to_1
                ).start()

    def relay(planes):
        @pl.when(plane == planes)
        def _():
            answered(1)
            q = chunk(plane_1, task, core)
            for which in range(2):
                send(held.at[which, q], which, q, z_got.at[3], to_2)

    def pass_on():
        @pl.when(inner)
        def _():
            q = chunk(plane_1, task, core)
            arrived(passing, pass_got.at[0])
            for which in range(2):
                outward(
                    passing.at[which], held.at[which, q], sent.at[1], z_got.at[3], to_3
                ).start()

    def part_copy(which, q, part, spot, got, peer):
        span = held.at[which, q, part]
        pltpu.make_async_remote_copy(
            src_ref=span, dst_ref=span, send_sem=sent.at[spot], recv_sem=got, device_id=peer,
            device_id_type=pl.DeviceIdType.MESH,
        ).start()

    def first_side(step):
        def relay_whole(which, q, peer):
            send(held.at[which, q], which, q, diagonal_got.at[step], peer)

        for which, tasks, member, axis, towards in ((0, task_x, 1, 0, task_y), (1, task_y, 2, 1, task_x)):
            q = chunk(order[step], tasks, core)
            peer = at(towards, plane, core)
            arrived(held.at[which, q], first_got.at[axis, step])
            if step < n_planes - 1:
                relay_whole(which, q, peer)
            else:
                @pl.when(core == 1)
                def _(which=which, q=q, peer=peer):
                    relay_whole(which, q, peer)

                @pl.when(core == 0)
                def _(which=which, q=q, peer=peer, towards=towards):
                    twin = at(towards, plane, 1)
                    part_copy(which, q, early_rows, 0, early_got.at[0], twin)
                    part_copy(which, q, late_rows, 0, late_got.at[0], peer)
                    part_copy(which, q, late_rows, 2, late_got.at[0], twin)
            pair_copy(step, member, which, q, held.at[which, q])

    def second_side(step):
        both = held.at[:, pl.ds(chunk(order[step], task_x, core), 1)]
        arrived(both, second_got.at[step])
        for which, tasks, member in ((1, task_x, 1), (0, task_y, 2)):
            q = chunk(order[step], tasks, core)
            pair_copy(step, member, which, q, held.at[which, q])

    def diagonal_step(step):
        q = chunk(order[step], task_d, core)
        arrived(held.at[:, pl.ds(q, 1)], diagonal_got.at[step])
        for which in range(2):
            pair_copy(step, 3, which, q, held.at[which, q])

    def diagonal_last():
        last = n_planes - 1

        @pl.when(core == 1)
        def _():
            diagonal_step(last)
            q = chunk(order[last], task_d, 0)
            arrived(held.at[:, pl.ds(q, 1), early_rows], early_got.at[0])
            for which in range(2):
                part_copy(which, q, early_rows, 2, pair_got.at[last + 1], to_pair)

    row_count = column_band // 2 // n_task
    padded = rows.shape[3]
    window = min(padded + LANES, column_band)
    row_start = core * (column_band // 2) + task * row_count
    base = jnp.minimum(row_start // LANES * LANES, column_band - window)
    shift = window - (row_start - base)

    everyone = (task, task_x, task_y, task_d)
    lends = [(1, member) for member in range(4)] + [(0, member) for member in LENT]
    gives = [
        (step, member) for step in range(n_planes - 1) for member in range(4)
        if step < 2 or (0, member) not in lends
    ]

    def row_copy(source, group, peer):
        return pltpu.make_async_remote_copy(
            src_ref=source, dst_ref=rows.at[group], send_sem=row_sent.at[0],
            recv_sem=row_got.at[group // n_task], device_id=peer,
            device_id_type=pl.DeviceIdType.MESH,
        )

    def cut(step, members):
        low = chunk(order[step], 0, 0)
        span = held.at[:, pl.ds(low, len(members))]
        if (step, members) != (n_planes - 1, (3,)):
            arrived(span, pair_got.at[min(step, n_planes - 1)])
        else:
            half = held.at[:, pl.ds(low, 1), late_rows]
            arrived(half, late_got.at[0])

            @pl.when(core == 0)
            def _():
                arrived(held.at[0, pl.ds(0, 3)], pair_got.at[n_planes])

        for member in members:
            tasks = everyone[member]
            group = order[step] * n_task + tasks

            def cut_into(target, group=group):
                for which in range(2):
                    span = held[
                        which, pl.ds(group * 2, 2), :, pl.ds(pl.multiple_of(base, LANES), window)
                    ]
                    span = span.reshape(2 * tok_dev, window).astype(jnp.float32)
                    span = pltpu.roll(span, shift, 1)
                    target[which] = span[:, :padded].astype(jnp.bfloat16)

            @pl.when(outer)
            def _():
                cut_into(rows.at[group])

            if (step, member) in lends:
                @pl.when(inner)
                def _():
                    cut_into(lent.at[step, tasks])

    def give_rows(step, members):
        @pl.when(outer)
        def _():
            for member in members:
                if (step, member) in gives:
                    group = order[step] * n_task + everyone[member]
                    row_copy(rows.at[group], group, to_1).start()

    def lend_rows(step, members):
        @pl.when(inner)
        def _():
            for member in members:
                if (step, member) in lends:
                    tasks = everyone[member]
                    group = order[step] * n_task + tasks
                    row_copy(lent.at[step, tasks], group, to_3).start()

    def rows_arrive(step):
        @pl.when(inner)
        def _():
            planes = product_order[step]
            span = rows.at[pl.ds(planes * n_task, n_task)]
            pltpu.make_async_remote_copy(
                src_ref=span, dst_ref=span, send_sem=row_sent.at[0], recv_sem=row_got.at[planes],
                device_id=to_1, device_id_type=pl.DeviceIdType.MESH,
            ).wait_recv()

    def multiply(step):
        rows_arrive(step)

        @pl.loop(0, 2)
        def _(which):
            piece = product(rows, held, product_order[step], which)
            if step == 0:
                total[which] = piece
            else:
                total[which] += piece

    def cut_and_give(step, cores):
        @pl.when(core == cores)
        def _():
            cut(step, every)
            give_rows(step, every)

    def multiply_when(now, step):
        @pl.when(now)
        def _():
            multiply(step)

    def cut_when(now, step, members):
        @pl.when(now)
        def _():
            cut(step, members)

    every = (0, 1, 2, 3)
    own_step(0)
    z_sends()
    first_side(0)
    own_step(1)
    inward(1)
    rise_on()
    second_side(0)
    diagonal_step(0)
    relay(2)
    first_side(1)
    pass_on()
    cut(0, every)
    give_rows(0, every)
    own_step(2)
    second_side(1)
    relay(1)
    diagonal_step(1)
    first_side(2)
    cut(1, every)
    give_rows(1, every)
    own_step(3)
    lend_rows(0, every)
    second_side(2)
    multiply(0)
    diagonal_step(2)
    lend_rows(1, every)
    cut_and_give(2, 0)
    first_side(3)
    cut_and_give(2, 1)
    multiply(1)
    multiply_when(outer, 2)
    second_side(3)
    cut_when(jnp.logical_and(outer, core == 0), 3, (0, 1, 2))
    diagonal_last()
    multiply_when(inner, 2)
    cut_when(jnp.logical_or(inner, core == 1), 3, (0, 1, 2))
    cut(3, (3,))
    rows_arrive(3)

    def all_sent(span, semaphore):
        pltpu.make_async_remote_copy(
            src_ref=span, dst_ref=span, send_sem=semaphore, recv_sem=row_got.at[0],
            device_id=to_pair, device_id_type=pl.DeviceIdType.MESH,
        ).wait_send()

    chunks = held.shape[1]
    for cores in range(2):
        for place, least in ((outer, chunks - 3), (inner, chunks - 1)):
            @pl.when(jnp.logical_and(place, core == cores))
            def _(count=least + cores):
                all_sent(held.at[:, pl.ds(0, count)], sent.at[0])

    all_sent(held.at[0, pl.ds(0, 1)], sent.at[2])

    @pl.when(plane == 1)
    def _():
        all_sent(passing, sent.at[1])

    @pl.when(plane == 2)
    def _():
        all_sent(mine, sent.at[1])

    @pl.when(inner)
    def _():
        all_sent(rows.at[pl.ds(0, len(lends))], row_sent.at[0])

    @pl.when(outer)
    def _():
        all_sent(rows.at[pl.ds(0, len(gives))], row_sent.at[0])


def gathered(hidden, attn_out, gain_attn, gain_mlp, lengths):
    _, tok_dev, width = hidden.shape
    n_tok, n_task = lax.axis_size("tok"), lax.axis_size("task")
    column_band = width // 2
    row_count = column_band // 2 // n_task
    padded = -(-row_count // LANES) * LANES
    devices = n_tok * n_task
    groups = devices // 2
    vmem, hbm = (pl.BlockSpec(memory_space=space) for space in (pltpu.VMEM, pltpu.HBM))
    semaphores = pltpu.SemaphoreType.DMA
    held, rows, total = pl.pallas_call(
        gather_kernel,
        out_shape=(
            jax.ShapeDtypeStruct((2, devices, tok_dev, column_band), jnp.bfloat16),
            jax.ShapeDtypeStruct((groups, 2, 2 * tok_dev, padded), jnp.bfloat16),
            jax.ShapeDtypeStruct((2, padded, column_band), jnp.float32),
        ),
        in_specs=[hbm] * 5,
        out_specs=(vmem,) * 3,
        scratch_shapes=[
            pltpu.VMEM((2,) + hidden.shape[1:], jnp.bfloat16),
            pltpu.VMEM(gain_attn.shape, jnp.bfloat16),
            pltpu.VMEM(gain_mlp.shape, jnp.bfloat16),
            pltpu.SMEM(lengths.shape, jnp.int32),
            pltpu.VMEM((2, 2, tok_dev, column_band), jnp.bfloat16),
            pltpu.VMEM((2, n_task, 2, 2 * tok_dev, padded), jnp.bfloat16),
            pltpu.VMEM((2, tok_dev, column_band), jnp.bfloat16),
            pltpu.VMEM((2, tok_dev, column_band), jnp.bfloat16),
            semaphores((4,)),
            pltpu.SemaphoreType.REGULAR((2,)),
            semaphores((4,)),
            semaphores((1,)),
            semaphores((1,)),
            semaphores((2, 4)),
            semaphores((4,)),
            semaphores((4,)),
            semaphores((1,)),
            semaphores((1,)),
            semaphores((5,)),
            semaphores((4,)),
            semaphores((3,)),
            semaphores((1,)),
        ],
        compiler_params=pltpu.CompilerParams(
            collective_id=0, has_side_effects=True, vmem_limit_bytes=24 * 2**20
        ),
    )(*(
        pltpu.with_memory_space_constraint(array, pltpu.HBM)
        for array in (hidden, attn_out, gain_attn, gain_mlp, lengths)
    ))
    shape = (1, row_count, column_band)
    return pl.pallas_call(
        last_kernel,
        out_shape=(jax.ShapeDtypeStruct(shape, jnp.float32),) * 2,
        in_specs=[vmem] * 3,
        out_specs=(hbm, hbm),
        scratch_shapes=[
            pltpu.VMEM((2,) + shape, jnp.float32),
            semaphores((2,)),
        ],
        compiler_params=pltpu.CompilerParams(vmem_limit_bytes=12 * 2**20),
    )(held, rows, total)


def from_partner(block, axis, distance):
    count = lax.axis_size(axis)
    route = []
    for low in range(count):
        high = low | 1 << distance
        if high != low and high < count:
            route += [(low, high), (high, low)]
    return lax.ppermute(block, axis, route)


def normed(values, gain):
    scale = lax.rsqrt(jnp.mean(values * values, axis=-1, keepdims=True) + 1e-06)
    return values * scale * gain.astype(jnp.float32)


def per_device(hidden, attn_out, gain_attn, gain_mlp, lengths):
    tok_dev = hidden.shape[1]
    width = hidden.shape[2]
    n_tok = lax.axis_size("tok")
    n_task = lax.axis_size("task")
    block_side = min(4, max(2, n_tok // 16))
    token_parts = n_tok // (block_side * block_side)
    if (n_task, n_tok, block_side) == (4, 8, 2) and width % (4 * LANES) == 0 and tok_dev % 32 == 0:
        return gathered(hidden, attn_out, gain_attn, gain_mlp, lengths)
    column_band = width // block_side
    tile_rows = column_band // token_parts
    slice_rows = tok_dev // token_parts
    seq_count = lengths.shape[1]
    seq_slots = tok_dev * n_tok // seq_count
    place = lax.axis_index("tok") * tok_dev + jnp.arange(tok_dev, dtype=jnp.int32)
    which = place // seq_slots
    offset = place % seq_slots
    owner = which[:, None] == jnp.arange(seq_count, dtype=jnp.int32)[None, :]
    limit = jnp.sum(jnp.where(owner, lengths[0][None, :], 0), axis=1)
    live = (offset < limit).astype(jnp.float32)[:, None]
    first = hidden[0].astype(jnp.float32)
    x_attn = (normed(first, gain_attn) * live).astype(jnp.bfloat16)
    mixed = first + attn_out[0].astype(jnp.float32)
    x_mlp = (normed(mixed, gain_mlp) * live).astype(jnp.bfloat16)

    def bands(values):
        split = values.reshape(token_parts, slice_rows, block_side, column_band).transpose(
            2, 0, 1, 3
        )
        shape = (block_side, block_side, token_parts, slice_rows, column_band)
        left_side = jnp.broadcast_to(split[:, None], shape).reshape(n_tok, slice_rows, column_band)
        right_side = jnp.broadcast_to(split[None], shape).reshape(n_tok, slice_rows, column_band)
        return (left_side, right_side)

    left_attn, right_attn = bands(x_attn)
    left_mlp, right_mlp = bands(x_mlp)
    arrived = (
        lax.all_to_all(left_attn, "tok", split_axis=0, concat_axis=0, tiled=True),
        lax.all_to_all(right_attn, "tok", split_axis=0, concat_axis=0, tiled=True),
        lax.all_to_all(left_mlp, "tok", split_axis=0, concat_axis=0, tiled=True),
        lax.all_to_all(right_mlp, "tok", split_axis=0, concat_axis=0, tiled=True),
    )
    contract = (((0, 1), (0, 1)), ((), ()))
    tile_attn = lax.dot_general(
        arrived[0], arrived[1], contract, preferred_element_type=jnp.float32
    )
    tile_mlp = lax.dot_general(arrived[2], arrived[3], contract, preferred_element_type=jnp.float32)
    grams = (
        tile_attn.reshape(token_parts, tile_rows, column_band),
        tile_mlp.reshape(token_parts, tile_rows, column_band),
    )
    part_index = lax.axis_index("tok") % token_parts
    depth_bits = token_parts.bit_length() - 1

    def halve(current, bit):
        upper_bit = part_index // (1 << bit) % 2 == 1
        middle = current[0].shape[0] // 2
        outgoing = tuple(
            (jnp.where(upper_bit, piece[:middle], piece[middle:]) for piece in current)
        )
        kept = tuple((jnp.where(upper_bit, piece[middle:], piece[:middle]) for piece in current))
        incoming = from_partner(outgoing, "tok", bit)
        return tuple((mine + theirs for mine, theirs in zip(kept, incoming)))

    for bit in range(depth_bits - 1, -1, -1):
        grams = halve(grams, bit)
    shaped = tuple((piece.reshape(n_task, tile_rows // n_task, column_band) for piece in grams))
    grams = lax.psum_scatter(shaped, "task", scatter_dimension=0, tiled=True)
    factor = 1.0 / (tok_dev * n_tok)
    final_attn = grams[0] * factor
    final_mlp = grams[1] * factor
    return (final_attn, final_mlp)


def solution(mesh):
    return jax.shard_map(
        per_device,
        mesh=mesh,
        in_specs=(P("task", "tok", None), P("task", "tok", None), P(), P(), P("task", None)),
        out_specs=(P("tok", "task", None), P("tok", "task", None)),
        check_vma=False,
    )
```

```python
import functools

import jax
import jax.numpy as jnp
from jax import lax
from jax.experimental import pallas as pl
from jax.experimental.pallas import tpu as pltpu
from jax.sharding import PartitionSpec as P

LANES = 128
LENT = (2, 3)


def planes_in_product_order():
    plane = lax.axis_index("tok") // 2
    inner = jnp.logical_or(plane == 1, plane == 2)
    plane_1 = plane + 1 - 2 * (plane % 2)
    plane_2 = jnp.where(plane // 2 == 1, plane - 2, plane + 2)
    plane_3 = 3 - plane
    return (
        jnp.where(inner, plane_1, plane), jnp.where(inner, plane, plane_1),
        jnp.where(inner, plane_3, plane_2), jnp.where(inner, plane_2, plane_3),
    )


def product(rows, held, plane, which):
    n_task = lax.axis_size("task")
    left = rows[pl.ds(plane * n_task, n_task), which]
    right = held[which, pl.ds(plane * 2 * n_task, 2 * n_task)]
    depth = left.shape[0] * left.shape[1]
    return lax.dot_general(
        left.reshape(depth, left.shape[2]), right.reshape(depth, right.shape[2]),
        (((0,), (0,)), ((), ())), preferred_element_type=jnp.float32,
    )


def band_edges(width):
    unit = 2 * LANES
    half = width // 2 // unit * unit
    return (0, unit, half, width), (0, width - half, width - unit, width)


def last_kernel(held, rows, total, out_attn, out_mlp, staged, sent):
    row_count, column_band = out_attn.shape[1], out_attn.shape[2]
    plane = planes_in_product_order()[3]
    factor = 1.0 / (lax.axis_size("tok") * held.shape[2])
    n_task = lax.axis_size("task")
    outs = (out_attn, out_mlp)
    lefts = []
    for which in range(2):
        left = rows[pl.ds(plane * n_task, n_task), which]
        lefts.append(left.reshape(-1, left.shape[2]).T[:row_count])
    bands = [
        (which, low, high)
        for which, edges in enumerate(band_edges(column_band))
        for low, high in zip(edges, edges[1:])
    ]

    def multiplied(which, low, high):
        right = held[which, pl.ds(plane * 2 * n_task, 2 * n_task), :, low:high]
        return jnp.dot(
            lefts[which], right.reshape(-1, high - low), preferred_element_type=jnp.float32
        )

    def put(piece, which, low, high):
        span = slice(low, high)
        staged[which, 0, :, span] = (total[which, :row_count, span] + piece) * factor
        pltpu.make_async_copy(
            staged.at[which, :, :, span], outs[which].at[:, :, span], sent.at[which]
        ).start()

    ahead = multiplied(*bands[0])
    for band, later in zip(bands, bands[1:]):
        piece, ahead = ahead, multiplied(*later)
        put(piece, *band)
    put(ahead, *bands[-1])
    for which, out in ((0, out_attn), (1, out_mlp)):
        pltpu.make_async_copy(staged.at[which], out, sent.at[which]).wait()


def gather_kernel(
    hidden_hbm, attn_hbm, gain_attn_hbm, gain_mlp_hbm, lengths_hbm, held, rows, total,
    inputs, gain_attn, gain_mlp, lengths, mine, lent, passing, rising,
    ready, z_got, pass_got, rise_got, first_got, second_got, diagonal_got, early_got, late_got, pair_got,
    row_got, sent, row_sent,
):
    task, tok = lax.axis_index("task"), lax.axis_index("tok")
    n_task = lax.axis_size("task")
    plane, core = tok // 2, tok % 2
    band = plane % 2
    tok_dev, column_band = held.shape[2], held.shape[3]
    n_planes = held.shape[1] // (2 * n_task)
    inner = jnp.logical_or(plane == 1, plane == 2)
    outer = jnp.logical_not(inner)

    def flip(value, bit):
        return value + bit - 2 * bit * (value // bit % 2)

    task_x, task_y = flip(task, 1), flip(task, 2)
    task_d = flip(task_x, 2)
    plane_1, plane_2 = flip(plane, 1), flip(plane, 2)
    plane_3 = flip(plane_1, 2)
    near, far = jnp.where(inner, plane_3, plane_2), jnp.where(inner, plane_2, plane_3)
    order = (plane, plane_1, near, far)
    product_order = planes_in_product_order()

    def at(tasks, planes, cores):
        return {"task": tasks, "tok": planes * 2 + cores}

    def chunk(planes, tasks, cores):
        return planes * (2 * n_task) + tasks * 2 + cores

    own = chunk(plane, task, core)
    to_x, to_y, to_pair = at(task_x, plane, core), at(task_y, plane, core), at(task, plane, 1 - core)
    to_1, to_2, to_3 = at(task, plane_1, core), at(task, plane_2, core), at(task, plane_3, core)

    barrier = pltpu.get_barrier_semaphore()
    always, odd = plane >= 0, plane % 2 == 1
    z_peers = (
        (to_1, plane_1, always, always), (to_2, plane_2, always, odd),
        (to_3, plane_3, inner, inner),
    )

    def signal(semaphore, peer):
        pl.semaphore_signal(
            semaphore, inc=1, device_id=peer, device_id_type=pl.DeviceIdType.MESH
        )

    for semaphore, source, target in (
        (sent.at[0], hidden_hbm, inputs.at[pl.ds(0, 1)]),
        (sent.at[0], attn_hbm, inputs.at[pl.ds(1, 1)]),
        (sent.at[1], gain_attn_hbm, gain_attn), (sent.at[2], gain_mlp_hbm, gain_mlp),
        (row_sent.at[0], lengths_hbm, lengths),
    ):
        pltpu.make_async_copy(source, target, semaphore).start()
    for peer in (to_x, to_y, to_pair):
        signal(barrier, peer)

    @pl.when(core == 1)
    def _():
        for tasks in (task_x, task_y):
            signal(barrier, at(tasks, plane, 0))

    for peer, planes, met, _ in z_peers:
        @pl.when(jnp.logical_and(met, planes > plane))
        def _(peer=peer):
            signal(barrier, peer)

    pltpu.make_async_copy(inputs, inputs, sent.at[0]).wait()
    pltpu.make_async_copy(gain_attn_hbm, gain_attn, sent.at[1]).wait()
    pltpu.make_async_copy(gain_mlp_hbm, gain_mlp, sent.at[2]).wait()
    pltpu.make_async_copy(lengths_hbm, lengths, row_sent.at[0]).wait()
    slab = 8
    seq_count = lengths.shape[1]
    seq_slots = tok_dev * lax.axis_size("tok") // seq_count
    for low in range(0, tok_dev, slab):
        part = pl.ds(low, slab)
        place = tok * tok_dev + low + lax.broadcasted_iota(jnp.int32, (slab, 1), 0)
        live = jnp.zeros((slab, 1), jnp.float32)
        for seq in range(seq_count):
            offset = place - seq * seq_slots
            inside = (offset >= 0) & (offset < seq_slots) & (offset < lengths[0, seq])
            live = jnp.where(inside, 1.0, live)
        first = inputs[0, part, :].astype(jnp.float32)
        mixed = first + inputs[1, part, :].astype(jnp.float32)
        for which, values, gain in ((0, first, gain_attn), (1, mixed, gain_mlp)):
            scale = lax.rsqrt(jnp.mean(values * values, axis=-1, keepdims=True) + 1e-06) * live
            weight = gain[...].reshape(1, -1).astype(jnp.float32)
            done = (values * scale * weight).astype(jnp.bfloat16)
            for side in range(2):
                mine[which, side, part, :] = done[:, side * column_band : (side + 1) * column_band]
    for which in range(2):
        held[which, own] = mine[which, band]
    pl.semaphore_wait(barrier, 5 - 2 * core + jnp.minimum(plane, 2))
    for reach, (peer, planes, _, answer) in enumerate(z_peers):
        @pl.when(jnp.logical_and(answer, planes < plane))
        def _(reach=reach, peer=peer):
            signal(ready.at[reach % 2], peer)

    def copy(source, which, q, got, peer):
        return pltpu.make_async_remote_copy(
            src_ref=source, dst_ref=held.at[which, q], send_sem=sent.at[0],
            recv_sem=got, device_id=peer, device_id_type=pl.DeviceIdType.MESH,
        )

    def send(*arguments):
        copy(*arguments).start()

    def arrived(span, got):
        pltpu.make_async_remote_copy(
            src_ref=span, dst_ref=span, send_sem=sent.at[0], recv_sem=got,
            device_id=to_pair, device_id_type=pl.DeviceIdType.MESH,
        ).wait_recv()

    def pair_copy(step, member, which, q, source):
        spot = step if step < n_planes - 1 else n_planes - 1 + member // 3
        send(source, which, q, pair_got.at[spot], to_pair)

    def own_step(step):
        q = chunk(order[step], task, core)

        def source(which):
            return held.at[which, q] if step else mine.at[which, band]

        def landed(which):
            if step == 1:
                arrived(held.at[which, q], z_got.at[which])
            elif step and which == 0:
                arrived(held.at[:, pl.ds(q, 1)], z_got.at[step])

        landed(0)
        send(source(0), 0, q, first_got.at[0, step], to_x)
        pair_copy(step, 0, 0, q, source(0))
        landed(1)
        send(source(1), 1, q, first_got.at[1, step], to_y)
        send(source(1), 1, q, second_got.at[step], to_x)
        send(source(0), 0, q, second_got.at[step], to_y)
        pair_copy(step, 0, 1, q, source(1))

    def answered(reach):
        _, planes, met, answer = z_peers[reach]

        @pl.when(jnp.logical_and(answer, planes > plane))
        def _():
            pl.semaphore_wait(ready.at[reach % 2], 1)

    def inward(planes):
        @pl.when(plane == planes)
        def _():
            for which in range(2):
                send(mine.at[which, 1 - band], which, own, z_got.at[2], to_3)

    def z_sends():
        inward(2)
        answered(0)
        for which in range(2):
            send(mine.at[which, 1 - band], which, own, z_got.at[which], to_1)

        @pl.when(outer)
        def _():
            for which in range(2):
                outward(
                    mine.at[which, band], passing.at[which], sent.at[0], pass_got.at[0], to_1
                ).start()

        answered(2)

        @pl.when(plane == 1)
        def _():
            for which in range(2):
                outward(
                    mine.at[which, band], rising.at[which], sent.at[0], rise_got.at[0], to_3
                ).start()

        @pl.when(plane == 2)
        def _():
            for which in range(2):
                send(mine.at[which, band], which, own, z_got.at[2], to_2)

    def outward(source, target, semaphore, got, peer):
        return pltpu.make_async_remote_copy(
            src_ref=source, dst_ref=target, send_sem=semaphore, recv_sem=got, device_id=peer,
            device_id_type=pl.DeviceIdType.MESH,
        )

    def rise_on():
        @pl.when(plane == 2)
        def _():
            q = chunk(plane_3, task, core)
            arrived(rising, rise_got.at[0])
            for which in range(2):
                outward(
                    rising.at[which], held.at[which, q], sent.at[1], z_got.at[2], to_1
                ).start()

    def relay(planes):
        @pl.when(plane == planes)
        def _():
            answered(1)
            q = chunk(plane_1, task, core)
            for which in range(2):
                send(held.at[which, q], which, q, z_got.at[3], to_2)

    def pass_on():
        @pl.when(inner)
        def _():
            q = chunk(plane_1, task, core)
            arrived(passing, pass_got.at[0])
            for which in range(2):
                outward(
                    passing.at[which], held.at[which, q], sent.at[1], z_got.at[3], to_3
                ).start()

    early_rows, late_rows = pl.ds(0, tok_dev // 2), pl.ds(tok_dev // 2, tok_dev // 2)

    def part_copy(which, q, part, spot, got, peer):
        span = held.at[which, q, part]
        pltpu.make_async_remote_copy(
            src_ref=span, dst_ref=span, send_sem=sent.at[spot], recv_sem=got, device_id=peer,
            device_id_type=pl.DeviceIdType.MESH,
        ).start()

    def first_side(step):
        def relay_whole(which, q, peer):
            send(held.at[which, q], which, q, diagonal_got.at[step], peer)

        for which, tasks, member, axis, towards in ((0, task_x, 1, 0, task_y), (1, task_y, 2, 1, task_x)):
            q = chunk(order[step], tasks, core)
            peer = at(towards, plane, core)
            arrived(held.at[which, q], first_got.at[axis, step])
            if step < n_planes - 1:
                relay_whole(which, q, peer)
            else:
                @pl.when(core == 1)
                def _(which=which, q=q, peer=peer):
                    relay_whole(which, q, peer)

                @pl.when(core == 0)
                def _(which=which, q=q, peer=peer, towards=towards):
                    twin = at(towards, plane, 1)
                    part_copy(which, q, early_rows, 0, early_got.at[0], twin)
                    part_copy(which, q, late_rows, 0, late_got.at[0], peer)
                    part_copy(which, q, late_rows, 2, late_got.at[0], twin)
            pair_copy(step, member, which, q, held.at[which, q])

    def second_side(step):
        both = held.at[:, pl.ds(chunk(order[step], task_x, core), 1)]
        arrived(both, second_got.at[step])
        for which, tasks, member in ((1, task_x, 1), (0, task_y, 2)):
            q = chunk(order[step], tasks, core)
            pair_copy(step, member, which, q, held.at[which, q])

    def diagonal_step(step):
        q = chunk(order[step], task_d, core)
        arrived(held.at[:, pl.ds(q, 1)], diagonal_got.at[step])
        for which in range(2):
            pair_copy(step, 3, which, q, held.at[which, q])

    def diagonal_last():
        last = n_planes - 1

        @pl.when(core == 1)
        def _():
            diagonal_step(last)
            q = chunk(order[last], task_d, 0)
            arrived(held.at[:, pl.ds(q, 1), early_rows], early_got.at[0])
            for which in range(2):
                part_copy(which, q, early_rows, 2, pair_got.at[last + 1], to_pair)

    row_count = column_band // 2 // n_task
    padded = rows.shape[3]
    window = min(padded + LANES, column_band)
    row_start = core * (column_band // 2) + task * row_count
    base = jnp.minimum(row_start // LANES * LANES, column_band - window)
    shift = window - (row_start - base)

    everyone = (task, task_x, task_y, task_d)
    lends = [(1, member) for member in range(4)] + [(0, member) for member in LENT]
    gives = [
        (step, member) for step in range(n_planes - 1) for member in range(4)
        if step < 2 or (0, member) not in lends
    ]

    def row_copy(source, group, peer):
        return pltpu.make_async_remote_copy(
            src_ref=source, dst_ref=rows.at[group], send_sem=row_sent.at[0],
            recv_sem=row_got.at[group // n_task], device_id=peer,
            device_id_type=pl.DeviceIdType.MESH,
        )

    def cut(step, members):
        low = chunk(order[step], 0, 0)
        span = held.at[:, pl.ds(low, len(members))]
        if (step, members) != (n_planes - 1, (3,)):
            arrived(span, pair_got.at[min(step, n_planes - 1)])
        else:
            half = held.at[:, pl.ds(low, 1), late_rows]
            arrived(half, late_got.at[0])

            @pl.when(core == 0)
            def _():
                arrived(held.at[0, pl.ds(0, 3)], pair_got.at[n_planes])

        for member in members:
            tasks = everyone[member]
            group = order[step] * n_task + tasks

            def cut_into(target, group=group):
                for which in range(2):
                    span = held[
                        which, pl.ds(group * 2, 2), :, pl.ds(pl.multiple_of(base, LANES), window)
                    ]
                    span = span.reshape(2 * tok_dev, window).astype(jnp.float32)
                    span = pltpu.roll(span, shift, 1)
                    target[which] = span[:, :padded].astype(jnp.bfloat16)

            @pl.when(outer)
            def _():
                cut_into(rows.at[group])

            if (step, member) in lends:
                @pl.when(inner)
                def _():
                    cut_into(lent.at[step, tasks])

    def give_rows(step, members):
        @pl.when(outer)
        def _():
            for member in members:
                if (step, member) in gives:
                    group = order[step] * n_task + everyone[member]
                    row_copy(rows.at[group], group, to_1).start()

    def lend_rows(step, members):
        @pl.when(inner)
        def _():
            for member in members:
                if (step, member) in lends:
                    tasks = everyone[member]
                    group = order[step] * n_task + tasks
                    row_copy(lent.at[step, tasks], group, to_3).start()

    def rows_arrive(step):
        @pl.when(inner)
        def _():
            planes = product_order[step]
            span = rows.at[pl.ds(planes * n_task, n_task)]
            pltpu.make_async_remote_copy(
                src_ref=span, dst_ref=span, send_sem=row_sent.at[0], recv_sem=row_got.at[planes],
                device_id=to_1, device_id_type=pl.DeviceIdType.MESH,
            ).wait_recv()

    def multiply(step):
        rows_arrive(step)

        @pl.loop(0, 2)
        def _(which):
            piece = product(rows, held, product_order[step], which)
            if step == 0:
                total[which] = piece
            else:
                total[which] += piece

    def cut_and_give(step, cores):
        @pl.when(core == cores)
        def _():
            cut(step, every)
            give_rows(step, every)

    def multiply_when(now, step):
        @pl.when(now)
        def _():
            multiply(step)

    def cut_when(now, step, members):
        @pl.when(now)
        def _():
            cut(step, members)

    every = (0, 1, 2, 3)
    own_step(0)
    z_sends()
    first_side(0)
    own_step(1)
    inward(1)
    rise_on()
    second_side(0)
    diagonal_step(0)
    relay(2)
    first_side(1)
    pass_on()
    cut(0, every)
    give_rows(0, every)
    own_step(2)
    second_side(1)
    relay(1)
    diagonal_step(1)
    first_side(2)
    cut(1, every)
    give_rows(1, every)
    own_step(3)
    lend_rows(0, every)
    second_side(2)
    multiply(0)
    diagonal_step(2)
    lend_rows(1, every)
    cut_and_give(2, 0)
    first_side(3)
    cut_and_give(2, 1)
    multiply(1)
    multiply_when(outer, 2)
    second_side(3)
    cut_when(jnp.logical_and(outer, core == 0), 3, (0, 1, 2))
    diagonal_last()
    multiply_when(inner, 2)
    cut_when(jnp.logical_or(inner, core == 1), 3, (0, 1, 2))
    cut(3, (3,))
    rows_arrive(3)

    def all_sent(span, semaphore):
        pltpu.make_async_remote_copy(
            src_ref=span, dst_ref=span, send_sem=semaphore, recv_sem=row_got.at[0],
            device_id=to_pair, device_id_type=pl.DeviceIdType.MESH,
        ).wait_send()

    chunks = held.shape[1]
    for cores in range(2):
        for place, least in ((outer, chunks - 3), (inner, chunks - 1)):
            @pl.when(jnp.logical_and(place, core == cores))
            def _(count=least + cores):
                all_sent(held.at[:, pl.ds(0, count)], sent.at[0])

    all_sent(held.at[0, pl.ds(0, 1)], sent.at[2])

    @pl.when(plane == 1)
    def _():
        all_sent(passing, sent.at[1])

    @pl.when(plane == 2)
    def _():
        all_sent(mine, sent.at[1])

    @pl.when(inner)
    def _():
        all_sent(rows.at[pl.ds(0, len(lends))], row_sent.at[0])

    @pl.when(outer)
    def _():
        all_sent(rows.at[pl.ds(0, len(gives))], row_sent.at[0])


def gathered(hidden, attn_out, gain_attn, gain_mlp, lengths):
    _, tok_dev, width = hidden.shape
    n_tok, n_task = lax.axis_size("tok"), lax.axis_size("task")
    column_band = width // 2
    row_count = column_band // 2 // n_task
    padded = -(-row_count // LANES) * LANES
    devices = n_tok * n_task
    groups = devices // 2
    vmem, hbm = (pl.BlockSpec(memory_space=space) for space in (pltpu.VMEM, pltpu.HBM))
    semaphores = pltpu.SemaphoreType.DMA
    held, rows, total = pl.pallas_call(
        gather_kernel,
        out_shape=(
            jax.ShapeDtypeStruct((2, devices, tok_dev, column_band), jnp.bfloat16),
            jax.ShapeDtypeStruct((groups, 2, 2 * tok_dev, padded), jnp.bfloat16),
            jax.ShapeDtypeStruct((2, padded, column_band), jnp.float32),
        ),
        in_specs=[hbm] * 5,
        out_specs=(vmem,) * 3,
        scratch_shapes=[
            pltpu.VMEM((2,) + hidden.shape[1:], jnp.bfloat16),
            pltpu.VMEM(gain_attn.shape, jnp.bfloat16),
            pltpu.VMEM(gain_mlp.shape, jnp.bfloat16),
            pltpu.SMEM(lengths.shape, jnp.int32),
            pltpu.VMEM((2, 2, tok_dev, column_band), jnp.bfloat16),
            pltpu.VMEM((2, n_task, 2, 2 * tok_dev, padded), jnp.bfloat16),
            pltpu.VMEM((2, tok_dev, column_band), jnp.bfloat16),
            pltpu.VMEM((2, tok_dev, column_band), jnp.bfloat16),
            pltpu.SemaphoreType.REGULAR((2,)),
            semaphores((4,)),
            semaphores((1,)),
            semaphores((1,)),
            semaphores((2, 4)),
            semaphores((4,)),
            semaphores((4,)),
            semaphores((1,)),
            semaphores((1,)),
            semaphores((5,)),
            semaphores((4,)),
            semaphores((3,)),
            semaphores((1,)),
        ],
        compiler_params=pltpu.CompilerParams(
            collective_id=0, has_side_effects=True, vmem_limit_bytes=24 * 2**20
        ),
    )(*(
        pltpu.with_memory_space_constraint(array, pltpu.HBM)
        for array in (hidden, attn_out, gain_attn, gain_mlp, lengths)
    ))
    shape = (1, row_count, column_band)
    return pl.pallas_call(
        last_kernel,
        out_shape=(jax.ShapeDtypeStruct(shape, jnp.float32),) * 2,
        in_specs=[vmem] * 3,
        out_specs=(hbm, hbm),
        scratch_shapes=[
            pltpu.VMEM((2,) + shape, jnp.float32),
            semaphores((2,)),
        ],
        compiler_params=pltpu.CompilerParams(vmem_limit_bytes=12 * 2**20),
    )(held, rows, total)


def from_partner(block, axis, distance):
    count = lax.axis_size(axis)
    route = []
    for low in range(count):
        high = low | 1 << distance
        if high != low and high < count:
            route += [(low, high), (high, low)]
    return lax.ppermute(block, axis, route)


def normed(values, gain):
    scale = lax.rsqrt(jnp.mean(values * values, axis=-1, keepdims=True) + 1e-06)
    return values * scale * gain.astype(jnp.float32)


def per_device(hidden, attn_out, gain_attn, gain_mlp, lengths):
    tok_dev = hidden.shape[1]
    width = hidden.shape[2]
    n_tok = lax.axis_size("tok")
    n_task = lax.axis_size("task")
    block_side = min(4, max(2, n_tok // 16))
    token_parts = n_tok // (block_side * block_side)
    if (n_task, n_tok, block_side) == (4, 8, 2) and width % (4 * LANES) == 0 and tok_dev % 32 == 0:
        return gathered(hidden, attn_out, gain_attn, gain_mlp, lengths)
    column_band = width // block_side
    tile_rows = column_band // token_parts
    slice_rows = tok_dev // token_parts
    seq_count = lengths.shape[1]
    seq_slots = tok_dev * n_tok // seq_count
    place = lax.axis_index("tok") * tok_dev + jnp.arange(tok_dev, dtype=jnp.int32)
    which = place // seq_slots
    offset = place % seq_slots
    owner = which[:, None] == jnp.arange(seq_count, dtype=jnp.int32)[None, :]
    limit = jnp.sum(jnp.where(owner, lengths[0][None, :], 0), axis=1)
    live = (offset < limit).astype(jnp.float32)[:, None]
    first = hidden[0].astype(jnp.float32)
    x_attn = (normed(first, gain_attn) * live).astype(jnp.bfloat16)
    mixed = first + attn_out[0].astype(jnp.float32)
    x_mlp = (normed(mixed, gain_mlp) * live).astype(jnp.bfloat16)

    def bands(values):
        split = values.reshape(token_parts, slice_rows, block_side, column_band).transpose(
            2, 0, 1, 3
        )
        shape = (block_side, block_side, token_parts, slice_rows, column_band)
        left_side = jnp.broadcast_to(split[:, None], shape).reshape(n_tok, slice_rows, column_band)
        right_side = jnp.broadcast_to(split[None], shape).reshape(n_tok, slice_rows, column_band)
        return (left_side, right_side)

    left_attn, right_attn = bands(x_attn)
    left_mlp, right_mlp = bands(x_mlp)
    arrived = (
        lax.all_to_all(left_attn, "tok", split_axis=0, concat_axis=0, tiled=True),
        lax.all_to_all(right_attn, "tok", split_axis=0, concat_axis=0, tiled=True),
        lax.all_to_all(left_mlp, "tok", split_axis=0, concat_axis=0, tiled=True),
        lax.all_to_all(right_mlp, "tok", split_axis=0, concat_axis=0, tiled=True),
    )
    contract = (((0, 1), (0, 1)), ((), ()))
    tile_attn = lax.dot_general(
        arrived[0], arrived[1], contract, preferred_element_type=jnp.float32
    )
    tile_mlp = lax.dot_general(arrived[2], arrived[3], contract, preferred_element_type=jnp.float32)
    grams = (
        tile_attn.reshape(token_parts, tile_rows, column_band),
        tile_mlp.reshape(token_parts, tile_rows, column_band),
    )
    part_index = lax.axis_index("tok") % token_parts
    depth_bits = token_parts.bit_length() - 1

    def halve(current, bit):
        upper_bit = part_index // (1 << bit) % 2 == 1
        middle = current[0].shape[0] // 2
        outgoing = tuple(
            (jnp.where(upper_bit, piece[:middle], piece[middle:]) for piece in current)
        )
        kept = tuple((jnp.where(upper_bit, piece[middle:], piece[:middle]) for piece in current))
        incoming = from_partner(outgoing, "tok", bit)
        return tuple((mine + theirs for mine, theirs in zip(kept, incoming)))

    for bit in range(depth_bits - 1, -1, -1):
        grams = halve(grams, bit)
    shaped = tuple((piece.reshape(n_task, tile_rows // n_task, column_band) for piece in grams))
    grams = lax.psum_scatter(shaped, "task", scatter_dimension=0, tiled=True)
    factor = 1.0 / (tok_dev * n_tok)
    final_attn = grams[0] * factor
    final_mlp = grams[1] * factor
    return (final_attn, final_mlp)


def solution(mesh):
    return jax.shard_map(
        per_device,
        mesh=mesh,
        in_specs=(P("task", "tok", None), P("task", "tok", None), P(), P(), P("task", None)),
        out_specs=(P("tok", "task", None), P("tok", "task", None)),
        check_vma=False,
    )
```

```python
import functools

import jax
import jax.numpy as jnp
from jax import lax
from jax.experimental import pallas as pl
from jax.experimental.pallas import tpu as pltpu
from jax.sharding import PartitionSpec as P

LANES = 128
LENT = (2, 3)


def planes_in_product_order():
    plane = lax.axis_index("tok") // 2
    inner = jnp.logical_or(plane == 1, plane == 2)
    plane_1 = plane + 1 - 2 * (plane % 2)
    plane_2 = jnp.where(plane // 2 == 1, plane - 2, plane + 2)
    plane_3 = 3 - plane
    return (
        jnp.where(inner, plane_1, plane), jnp.where(inner, plane, plane_1),
        jnp.where(inner, plane_3, plane_2), jnp.where(inner, plane_2, plane_3),
    )


def product(rows, held, plane, which):
    n_task = lax.axis_size("task")
    left = rows[pl.ds(plane * n_task, n_task), which]
    right = held[which, pl.ds(plane * 2 * n_task, 2 * n_task)]
    depth = left.shape[0] * left.shape[1]
    return lax.dot_general(
        left.reshape(depth, left.shape[2]), right.reshape(depth, right.shape[2]),
        (((0,), (0,)), ((), ())), preferred_element_type=jnp.float32,
    )


def band_edges(width):
    unit = 2 * LANES
    half = width // 2 // unit * unit
    return (0, unit, half, width), (0, width - half, width - unit, width)


def last_kernel(held, rows, total, out_attn, out_mlp, staged, sent):
    row_count, column_band = out_attn.shape[1], out_attn.shape[2]
    plane = planes_in_product_order()[3]
    factor = 1.0 / (lax.axis_size("tok") * held.shape[2])
    n_task = lax.axis_size("task")
    outs = (out_attn, out_mlp)
    lefts = []
    for which in range(2):
        left = rows[pl.ds(plane * n_task, n_task), which]
        lefts.append(left.reshape(-1, left.shape[2]).T[:row_count])
    bands = [
        (which, low, high)
        for which, edges in enumerate(band_edges(column_band))
        for low, high in zip(edges, edges[1:])
    ]

    def multiplied(which, low, high):
        right = held[which, pl.ds(plane * 2 * n_task, 2 * n_task), :, low:high]
        return jnp.dot(
            lefts[which], right.reshape(-1, high - low), preferred_element_type=jnp.float32
        )

    def put(piece, which, low, high):
        span = slice(low, high)
        staged[which, 0, :, span] = (total[which, :row_count, span] + piece) * factor
        pltpu.make_async_copy(
            staged.at[which, :, :, span], outs[which].at[:, :, span], sent.at[which]
        ).start()

    ahead = multiplied(*bands[0])
    for band, later in zip(bands, bands[1:]):
        piece, ahead = ahead, multiplied(*later)
        put(piece, *band)
    put(ahead, *bands[-1])
    for which, out in ((0, out_attn), (1, out_mlp)):
        pltpu.make_async_copy(staged.at[which], out, sent.at[which]).wait()


def gather_kernel(
    hidden_hbm, attn_hbm, gain_attn_hbm, gain_mlp_hbm, lengths_hbm, held, rows, total,
    inputs, gain_attn, gain_mlp, lengths, mine, lent, passing, rising,
    ready, z_got, pass_got, rise_got, first_got, second_got, diagonal_got, early_got, late_got, pair_got,
    row_got, sent, row_sent,
):
    task, tok = lax.axis_index("task"), lax.axis_index("tok")
    n_task = lax.axis_size("task")
    plane, core = tok // 2, tok % 2
    band = plane % 2
    tok_dev, column_band = held.shape[2], held.shape[3]
    n_planes = held.shape[1] // (2 * n_task)
    inner = jnp.logical_or(plane == 1, plane == 2)
    outer = jnp.logical_not(inner)

    def flip(value, bit):
        return value + bit - 2 * bit * (value // bit % 2)

    task_x, task_y = flip(task, 1), flip(task, 2)
    task_d = flip(task_x, 2)
    plane_1, plane_2 = flip(plane, 1), flip(plane, 2)
    plane_3 = flip(plane_1, 2)
    near, far = jnp.where(inner, plane_3, plane_2), jnp.where(inner, plane_2, plane_3)
    order = (plane, plane_1, near, far)
    product_order = planes_in_product_order()

    def at(tasks, planes, cores):
        return {"task": tasks, "tok": planes * 2 + cores}

    def chunk(planes, tasks, cores):
        return planes * (2 * n_task) + tasks * 2 + cores

    own = chunk(plane, task, core)
    to_x, to_y, to_pair = at(task_x, plane, core), at(task_y, plane, core), at(task, plane, 1 - core)
    to_1, to_2, to_3 = at(task, plane_1, core), at(task, plane_2, core), at(task, plane_3, core)

    barrier = pltpu.get_barrier_semaphore()
    always, odd = plane >= 0, plane % 2 == 1
    z_peers = (
        (to_1, plane_1, always, always), (to_2, plane_2, always, odd),
        (to_3, plane_3, inner, inner),
    )

    def signal(semaphore, peer):
        pl.semaphore_signal(
            semaphore, inc=1, device_id=peer, device_id_type=pl.DeviceIdType.MESH
        )

    for semaphore, source, target in (
        (sent.at[0], hidden_hbm, inputs.at[pl.ds(0, 1)]),
        (sent.at[0], attn_hbm, inputs.at[pl.ds(1, 1)]),
        (sent.at[1], gain_attn_hbm, gain_attn), (sent.at[2], gain_mlp_hbm, gain_mlp),
        (row_sent.at[0], lengths_hbm, lengths),
    ):
        pltpu.make_async_copy(source, target, semaphore).start()
    for peer in (to_x, to_y, to_pair):
        signal(barrier, peer)

    @pl.when(core == 1)
    def _():
        for tasks in (task_x, task_y):
            signal(barrier, at(tasks, plane, 0))

    for peer, planes, met, _ in z_peers:
        @pl.when(jnp.logical_and(met, planes > plane))
        def _(peer=peer):
            signal(barrier, peer)

    pltpu.make_async_copy(inputs, inputs, sent.at[0]).wait()
    pltpu.make_async_copy(gain_attn_hbm, gain_attn, sent.at[1]).wait()
    pltpu.make_async_copy(gain_mlp_hbm, gain_mlp, sent.at[2]).wait()
    pltpu.make_async_copy(lengths_hbm, lengths, row_sent.at[0]).wait()
    slab = 8
    seq_count = lengths.shape[1]
    seq_slots = tok_dev * lax.axis_size("tok") // seq_count
    half = tok_dev // 2
    early_rows, late_rows = pl.ds(0, half), pl.ds(half, half)

    def norm_rows(start, part):
        for low in range(start, start + half, slab):
            spot = pl.ds(low, slab)
            place = tok * tok_dev + low + lax.broadcasted_iota(jnp.int32, (slab, 1), 0)
            live = jnp.zeros((slab, 1), jnp.float32)
            for seq in range(seq_count):
                offset = place - seq * seq_slots
                inside = (offset >= 0) & (offset < seq_slots) & (offset < lengths[0, seq])
                live = jnp.where(inside, 1.0, live)
            first = inputs[0, spot, :].astype(jnp.float32)
            mixed = first + inputs[1, spot, :].astype(jnp.float32)
            for which, values, gain in ((0, first, gain_attn), (1, mixed, gain_mlp)):
                mean = jnp.mean(values * values, axis=-1, keepdims=True)
                scale = lax.rsqrt(mean + 1e-06) * live
                weight = gain[...].reshape(1, -1).astype(jnp.float32)
                done = (values * scale * weight).astype(jnp.bfloat16)
                for side in range(2):
                    span = slice(side * column_band, (side + 1) * column_band)
                    mine[which, side, spot, :] = done[:, span]
        for which in range(2):
            held[which, own, part] = mine[which, band, part]

    def first_copies(part):
        for which, peer in ((0, to_x), (1, to_y)):
            pltpu.make_async_remote_copy(
                src_ref=mine.at[which, band, part], dst_ref=held.at[which, own, part],
                send_sem=sent.at[0], recv_sem=first_got.at[which, 0], device_id=peer,
                device_id_type=pl.DeviceIdType.MESH,
            ).start()

    norm_rows(0, early_rows)
    pl.semaphore_wait(barrier, 5 - 2 * core + jnp.minimum(plane, 2))
    first_copies(early_rows)
    for reach, (peer, planes, _, answer) in enumerate(z_peers):
        @pl.when(jnp.logical_and(answer, planes < plane))
        def _(reach=reach, peer=peer):
            signal(ready.at[reach % 2], peer)
    norm_rows(half, late_rows)
    first_copies(late_rows)

    def copy(source, which, q, got, peer):
        return pltpu.make_async_remote_copy(
            src_ref=source, dst_ref=held.at[which, q], send_sem=sent.at[0],
            recv_sem=got, device_id=peer, device_id_type=pl.DeviceIdType.MESH,
        )

    def send(*arguments):
        copy(*arguments).start()

    def arrived(span, got):
        pltpu.make_async_remote_copy(
            src_ref=span, dst_ref=span, send_sem=sent.at[0], recv_sem=got,
            device_id=to_pair, device_id_type=pl.DeviceIdType.MESH,
        ).wait_recv()

    def pair_copy(step, member, which, q, source):
        spot = step if step < n_planes - 1 else n_planes - 1 + member // 3
        send(source, which, q, pair_got.at[spot], to_pair)

    def own_step(step):
        q = chunk(order[step], task, core)

        def source(which):
            return held.at[which, q] if step else mine.at[which, band]

        def landed(which):
            if step == 1:
                arrived(held.at[which, q], z_got.at[which])
            elif step and which == 0:
                arrived(held.at[:, pl.ds(q, 1)], z_got.at[step])

        landed(0)
        if step:
            send(source(0), 0, q, first_got.at[0, step], to_x)
        pair_copy(step, 0, 0, q, source(0))
        landed(1)
        if step:
            send(source(1), 1, q, first_got.at[1, step], to_y)
        send(source(1), 1, q, second_got.at[step], to_x)
        send(source(0), 0, q, second_got.at[step], to_y)
        pair_copy(step, 0, 1, q, source(1))

    def answered(reach):
        _, planes, met, answer = z_peers[reach]

        @pl.when(jnp.logical_and(answer, planes > plane))
        def _():
            pl.semaphore_wait(ready.at[reach % 2], 1)

    def inward(planes):
        @pl.when(plane == planes)
        def _():
            for which in range(2):
                send(mine.at[which, 1 - band], which, own, z_got.at[2], to_3)

    def z_sends():
        inward(2)
        answered(0)
        for which in range(2):
            send(mine.at[which, 1 - band], which, own, z_got.at[which], to_1)

        @pl.when(outer)
        def _():
            for which in range(2):
                outward(
                    mine.at[which, band], passing.at[which], sent.at[0], pass_got.at[0], to_1
                ).start()

        answered(2)

        @pl.when(plane == 1)
        def _():
            for which in range(2):
                outward(
                    mine.at[which, band], rising.at[which], sent.at[0], rise_got.at[0], to_3
                ).start()

        @pl.when(plane == 2)
        def _():
            for which in range(2):
                send(mine.at[which, band], which, own, z_got.at[2], to_2)

    def outward(source, target, semaphore, got, peer):
        return pltpu.make_async_remote_copy(
            src_ref=source, dst_ref=target, send_sem=semaphore, recv_sem=got, device_id=peer,
            device_id_type=pl.DeviceIdType.MESH,
        )

    def rise_on():
        @pl.when(plane == 2)
        def _():
            q = chunk(plane_3, task, core)
            arrived(rising, rise_got.at[0])
            for which in range(2):
                outward(
                    rising.at[which], held.at[which, q], sent.at[1], z_got.at[2], to_1
                ).start()

    def relay(planes):
        @pl.when(plane == planes)
        def _():
            answered(1)
            q = chunk(plane_1, task, core)
            for which in range(2):
                send(held.at[which, q], which, q, z_got.at[3], to_2)

    def pass_on():
        @pl.when(inner)
        def _():
            q = chunk(plane_1, task, core)
            arrived(passing, pass_got.at[0])
            for which in range(2):
                outward(
                    passing.at[which], held.at[which, q], sent.at[1], z_got.at[3], to_3
                ).start()

    def part_copy(which, q, part, spot, got, peer):
        span = held.at[which, q, part]
        pltpu.make_async_remote_copy(
            src_ref=span, dst_ref=span, send_sem=sent.at[spot], recv_sem=got, device_id=peer,
            device_id_type=pl.DeviceIdType.MESH,
        ).start()

    def first_side(step):
        def relay_whole(which, q, peer):
            send(held.at[which, q], which, q, diagonal_got.at[step], peer)

        for which, tasks, member, axis, towards in ((0, task_x, 1, 0, task_y), (1, task_y, 2, 1, task_x)):
            q = chunk(order[step], tasks, core)
            peer = at(towards, plane, core)
            arrived(held.at[which, q], first_got.at[axis, step])
            if step < n_planes - 1:
                relay_whole(which, q, peer)
            else:
                @pl.when(core == 1)
                def _(which=which, q=q, peer=peer):
                    relay_whole(which, q, peer)

                @pl.when(core == 0)
                def _(which=which, q=q, peer=peer, towards=towards):
                    twin = at(towards, plane, 1)
                    part_copy(which, q, early_rows, 0, early_got.at[0], twin)
                    part_copy(which, q, late_rows, 0, late_got.at[0], peer)
                    part_copy(which, q, late_rows, 2, late_got.at[0], twin)
            pair_copy(step, member, which, q, held.at[which, q])

    def second_side(step):
        both = held.at[:, pl.ds(chunk(order[step], task_x, core), 1)]
        arrived(both, second_got.at[step])
        for which, tasks, member in ((1, task_x, 1), (0, task_y, 2)):
            q = chunk(order[step], tasks, core)
            pair_copy(step, member, which, q, held.at[which, q])

    def diagonal_step(step):
        q = chunk(order[step], task_d, core)
        arrived(held.at[:, pl.ds(q, 1)], diagonal_got.at[step])
        for which in range(2):
            pair_copy(step, 3, which, q, held.at[which, q])

    def diagonal_last():
        last = n_planes - 1

        @pl.when(core == 1)
        def _():
            diagonal_step(last)
            q = chunk(order[last], task_d, 0)
            arrived(held.at[:, pl.ds(q, 1), early_rows], early_got.at[0])
            for which in range(2):
                part_copy(which, q, early_rows, 2, pair_got.at[last + 1], to_pair)

    row_count = column_band // 2 // n_task
    padded = rows.shape[3]
    window = min(padded + LANES, column_band)
    row_start = core * (column_band // 2) + task * row_count
    base = jnp.minimum(row_start // LANES * LANES, column_band - window)
    shift = window - (row_start - base)

    everyone = (task, task_x, task_y, task_d)
    lends = [(1, member) for member in range(4)] + [(0, member) for member in LENT]
    gives = [
        (step, member) for step in range(n_planes - 1) for member in range(4)
        if step < 2 or (0, member) not in lends
    ]

    def row_copy(source, group, peer):
        return pltpu.make_async_remote_copy(
            src_ref=source, dst_ref=rows.at[group], send_sem=row_sent.at[0],
            recv_sem=row_got.at[group // n_task], device_id=peer,
            device_id_type=pl.DeviceIdType.MESH,
        )

    def cut(step, members):
        low = chunk(order[step], 0, 0)
        span = held.at[:, pl.ds(low, len(members))]
        if (step, members) != (n_planes - 1, (3,)):
            arrived(span, pair_got.at[min(step, n_planes - 1)])
        else:
            half = held.at[:, pl.ds(low, 1), late_rows]
            arrived(half, late_got.at[0])

            @pl.when(core == 0)
            def _():
                arrived(held.at[0, pl.ds(0, 3)], pair_got.at[n_planes])

        for member in members:
            tasks = everyone[member]
            group = order[step] * n_task + tasks

            def cut_into(target, group=group):
                for which in range(2):
                    span = held[
                        which, pl.ds(group * 2, 2), :, pl.ds(pl.multiple_of(base, LANES), window)
                    ]
                    span = span.reshape(2 * tok_dev, window).astype(jnp.float32)
                    span = pltpu.roll(span, shift, 1)
                    target[which] = span[:, :padded].astype(jnp.bfloat16)

            @pl.when(outer)
            def _():
                cut_into(rows.at[group])

            if (step, member) in lends:
                @pl.when(inner)
                def _():
                    cut_into(lent.at[step, tasks])

    def give_rows(step, members):
        @pl.when(outer)
        def _():
            for member in members:
                if (step, member) in gives:
                    group = order[step] * n_task + everyone[member]
                    row_copy(rows.at[group], group, to_1).start()

    def lend_rows(step, members):
        @pl.when(inner)
        def _():
            for member in members:
                if (step, member) in lends:
                    tasks = everyone[member]
                    group = order[step] * n_task + tasks
                    row_copy(lent.at[step, tasks], group, to_3).start()

    def rows_arrive(step):
        @pl.when(inner)
        def _():
            planes = product_order[step]
            span = rows.at[pl.ds(planes * n_task, n_task)]
            pltpu.make_async_remote_copy(
                src_ref=span, dst_ref=span, send_sem=row_sent.at[0], recv_sem=row_got.at[planes],
                device_id=to_1, device_id_type=pl.DeviceIdType.MESH,
            ).wait_recv()

    def multiply(step):
        rows_arrive(step)

        @pl.loop(0, 2)
        def _(which):
            piece = product(rows, held, product_order[step], which)
            if step == 0:
                total[which] = piece
            else:
                total[which] += piece

    def cut_and_give(step, cores):
        @pl.when(core == cores)
        def _():
            cut(step, every)
            give_rows(step, every)

    def multiply_when(now, step):
        @pl.when(now)
        def _():
            multiply(step)

    def cut_when(now, step, members):
        @pl.when(now)
        def _():
            cut(step, members)

    every = (0, 1, 2, 3)
    own_step(0)
    z_sends()
    first_side(0)
    own_step(1)
    inward(1)
    rise_on()
    second_side(0)
    diagonal_step(0)
    relay(2)
    first_side(1)
    pass_on()
    cut(0, every)
    give_rows(0, every)
    own_step(2)
    second_side(1)
    relay(1)
    diagonal_step(1)
    first_side(2)
    cut(1, every)
    give_rows(1, every)
    own_step(3)
    lend_rows(0, every)
    second_side(2)
    multiply(0)
    diagonal_step(2)
    lend_rows(1, every)
    cut_and_give(2, 0)
    first_side(3)
    cut_and_give(2, 1)
    multiply(1)
    multiply_when(outer, 2)
    second_side(3)
    cut_when(jnp.logical_and(outer, core == 0), 3, (0, 1, 2))
    diagonal_last()
    multiply_when(inner, 2)
    cut_when(jnp.logical_or(inner, core == 1), 3, (0, 1, 2))
    cut(3, (3,))
    rows_arrive(3)

    def all_sent(span, semaphore):
        pltpu.make_async_remote_copy(
            src_ref=span, dst_ref=span, send_sem=semaphore, recv_sem=row_got.at[0],
            device_id=to_pair, device_id_type=pl.DeviceIdType.MESH,
        ).wait_send()

    chunks = held.shape[1]
    for cores in range(2):
        for place, least in ((outer, chunks - 3), (inner, chunks - 1)):
            @pl.when(jnp.logical_and(place, core == cores))
            def _(count=least + cores):
                all_sent(held.at[:, pl.ds(0, count)], sent.at[0])

    all_sent(held.at[0, pl.ds(0, 1)], sent.at[2])

    @pl.when(plane == 1)
    def _():
        all_sent(passing, sent.at[1])

    @pl.when(plane == 2)
    def _():
        all_sent(mine, sent.at[1])

    @pl.when(inner)
    def _():
        all_sent(rows.at[pl.ds(0, len(lends))], row_sent.at[0])

    @pl.when(outer)
    def _():
        all_sent(rows.at[pl.ds(0, len(gives))], row_sent.at[0])


def gathered(hidden, attn_out, gain_attn, gain_mlp, lengths):
    _, tok_dev, width = hidden.shape
    n_tok, n_task = lax.axis_size("tok"), lax.axis_size("task")
    column_band = width // 2
    row_count = column_band // 2 // n_task
    padded = -(-row_count // LANES) * LANES
    devices = n_tok * n_task
    groups = devices // 2
    vmem, hbm = (pl.BlockSpec(memory_space=space) for space in (pltpu.VMEM, pltpu.HBM))
    semaphores = pltpu.SemaphoreType.DMA
    held, rows, total = pl.pallas_call(
        gather_kernel,
        out_shape=(
            jax.ShapeDtypeStruct((2, devices, tok_dev, column_band), jnp.bfloat16),
            jax.ShapeDtypeStruct((groups, 2, 2 * tok_dev, padded), jnp.bfloat16),
            jax.ShapeDtypeStruct((2, padded, column_band), jnp.float32),
        ),
        in_specs=[hbm] * 5,
        out_specs=(vmem,) * 3,
        scratch_shapes=[
            pltpu.VMEM((2,) + hidden.shape[1:], jnp.bfloat16),
            pltpu.VMEM(gain_attn.shape, jnp.bfloat16),
            pltpu.VMEM(gain_mlp.shape, jnp.bfloat16),
            pltpu.SMEM(lengths.shape, jnp.int32),
            pltpu.VMEM((2, 2, tok_dev, column_band), jnp.bfloat16),
            pltpu.VMEM((2, n_task, 2, 2 * tok_dev, padded), jnp.bfloat16),
            pltpu.VMEM((2, tok_dev, column_band), jnp.bfloat16),
            pltpu.VMEM((2, tok_dev, column_band), jnp.bfloat16),
            pltpu.SemaphoreType.REGULAR((2,)),
            semaphores((4,)),
            semaphores((1,)),
            semaphores((1,)),
            semaphores((2, 4)),
            semaphores((4,)),
            semaphores((4,)),
            semaphores((1,)),
            semaphores((1,)),
            semaphores((5,)),
            semaphores((4,)),
            semaphores((3,)),
            semaphores((1,)),
        ],
        compiler_params=pltpu.CompilerParams(
            collective_id=0, has_side_effects=True, vmem_limit_bytes=24 * 2**20
        ),
    )(*(
        pltpu.with_memory_space_constraint(array, pltpu.HBM)
        for array in (hidden, attn_out, gain_attn, gain_mlp, lengths)
    ))
    shape = (1, row_count, column_band)
    return pl.pallas_call(
        last_kernel,
        out_shape=(jax.ShapeDtypeStruct(shape, jnp.float32),) * 2,
        in_specs=[vmem] * 3,
        out_specs=(hbm, hbm),
        scratch_shapes=[
            pltpu.VMEM((2,) + shape, jnp.float32),
            semaphores((2,)),
        ],
        compiler_params=pltpu.CompilerParams(vmem_limit_bytes=12 * 2**20),
    )(held, rows, total)


def from_partner(block, axis, distance):
    count = lax.axis_size(axis)
    route = []
    for low in range(count):
        high = low | 1 << distance
        if high != low and high < count:
            route += [(low, high), (high, low)]
    return lax.ppermute(block, axis, route)


def normed(values, gain):
    scale = lax.rsqrt(jnp.mean(values * values, axis=-1, keepdims=True) + 1e-06)
    return values * scale * gain.astype(jnp.float32)


def per_device(hidden, attn_out, gain_attn, gain_mlp, lengths):
    tok_dev = hidden.shape[1]
    width = hidden.shape[2]
    n_tok = lax.axis_size("tok")
    n_task = lax.axis_size("task")
    block_side = min(4, max(2, n_tok // 16))
    token_parts = n_tok // (block_side * block_side)
    if (n_task, n_tok, block_side) == (4, 8, 2) and width % (4 * LANES) == 0 and tok_dev % 32 == 0:
        return gathered(hidden, attn_out, gain_attn, gain_mlp, lengths)
    column_band = width // block_side
    tile_rows = column_band // token_parts
    slice_rows = tok_dev // token_parts
    seq_count = lengths.shape[1]
    seq_slots = tok_dev * n_tok // seq_count
    place = lax.axis_index("tok") * tok_dev + jnp.arange(tok_dev, dtype=jnp.int32)
    which = place // seq_slots
    offset = place % seq_slots
    owner = which[:, None] == jnp.arange(seq_count, dtype=jnp.int32)[None, :]
    limit = jnp.sum(jnp.where(owner, lengths[0][None, :], 0), axis=1)
    live = (offset < limit).astype(jnp.float32)[:, None]
    first = hidden[0].astype(jnp.float32)
    x_attn = (normed(first, gain_attn) * live).astype(jnp.bfloat16)
    mixed = first + attn_out[0].astype(jnp.float32)
    x_mlp = (normed(mixed, gain_mlp) * live).astype(jnp.bfloat16)

    def bands(values):
        split = values.reshape(token_parts, slice_rows, block_side, column_band).transpose(
            2, 0, 1, 3
        )
        shape = (block_side, block_side, token_parts, slice_rows, column_band)
        left_side = jnp.broadcast_to(split[:, None], shape).reshape(n_tok, slice_rows, column_band)
        right_side = jnp.broadcast_to(split[None], shape).reshape(n_tok, slice_rows, column_band)
        return (left_side, right_side)

    left_attn, right_attn = bands(x_attn)
    left_mlp, right_mlp = bands(x_mlp)
    arrived = (
        lax.all_to_all(left_attn, "tok", split_axis=0, concat_axis=0, tiled=True),
        lax.all_to_all(right_attn, "tok", split_axis=0, concat_axis=0, tiled=True),
        lax.all_to_all(left_mlp, "tok", split_axis=0, concat_axis=0, tiled=True),
        lax.all_to_all(right_mlp, "tok", split_axis=0, concat_axis=0, tiled=True),
    )
    contract = (((0, 1), (0, 1)), ((), ()))
    tile_attn = lax.dot_general(
        arrived[0], arrived[1], contract, preferred_element_type=jnp.float32
    )
    tile_mlp = lax.dot_general(arrived[2], arrived[3], contract, preferred_element_type=jnp.float32)
    grams = (
        tile_attn.reshape(token_parts, tile_rows, column_band),
        tile_mlp.reshape(token_parts, tile_rows, column_band),
    )
    part_index = lax.axis_index("tok") % token_parts
    depth_bits = token_parts.bit_length() - 1

    def halve(current, bit):
        upper_bit = part_index // (1 << bit) % 2 == 1
        middle = current[0].shape[0] // 2
        outgoing = tuple(
            (jnp.where(upper_bit, piece[:middle], piece[middle:]) for piece in current)
        )
        kept = tuple((jnp.where(upper_bit, piece[middle:], piece[:middle]) for piece in current))
        incoming = from_partner(outgoing, "tok", bit)
        return tuple((mine + theirs for mine, theirs in zip(kept, incoming)))

    for bit in range(depth_bits - 1, -1, -1):
        grams = halve(grams, bit)
    shaped = tuple((piece.reshape(n_task, tile_rows // n_task, column_band) for piece in grams))
    grams = lax.psum_scatter(shaped, "task", scatter_dimension=0, tiled=True)
    factor = 1.0 / (tok_dev * n_tok)
    final_attn = grams[0] * factor
    final_mlp = grams[1] * factor
    return (final_attn, final_mlp)


def solution(mesh):
    return jax.shard_map(
        per_device,
        mesh=mesh,
        in_specs=(P("task", "tok", None), P("task", "tok", None), P(), P(), P("task", None)),
        out_specs=(P("tok", "task", None), P("tok", "task", None)),
        check_vma=False,
    )
```
